32 devices in a mesh: section: 4 (over y, x), seq: 2 (over core), exp: 4 (over z).
Axes of the slice: x: 2, y: 2, z: 4, core: 2. Of those that a mesh axis runs over, the one named last changes fastest.
Arguments:
- latent: bfloat16 [8, 8, 64, 384], P('section', 'seq', 'exp'), may hold values from -6 to 6
- cotangent: bfloat16 [8, 8, 64, 384], P('section', 'seq', 'exp'), may hold values from -6 to 6
- gain_one: float32 [384], replicated, may hold values from 0.5 to 2
- gain_two: float32 [384], replicated, may hold values from 0.5 to 2
- kernel_one: bfloat16 [3, 3, 3, 384, 384], P(None, None, None, 'exp'), may hold values from -0.0625 to 0.0625
- kernel_two: bfloat16 [3, 3, 3, 384, 384], P(None, None, None, 'exp'), may hold values from -0.0625 to 0.0625
Outputs:
- block_out: bfloat16 [8, 8, 64, 384], P('section', 'seq', 'exp')
- latent_grad: bfloat16 [8, 8, 64, 384], P('section', 'seq', 'exp')
The draws below stay inside these ranges and needn't reach their ends.
All inputs are finite; a program needn't handle non-finite values.
Results may differ from the reference program's by a relative error of at most 0.015.
Values may be sent and summed in bfloat16 or wider, within the bound.
A program may use at most 64 MiB of HBM per device.

```python
import math
import jax
import jax.numpy as jnp
from jax import lax

C = 384
NT = 8
NH = 8
NW = 64


def block_levels(rng, shape, pieces, least, top_value):
    loudness, own = 1.0, jax.random.fold_in(rng, 6)
    for position, parts in pieces:
        draws = jnp.exp(jax.random.uniform(jax.random.fold_in(own, position), (parts,), jnp.float32, least / len(pieces), top_value / len(pieces)))
        loudness = loudness * jnp.repeat(draws, shape[position] // parts).reshape([-1 if axis == position else 1 for axis in range(len(shape))])
    return loudness


def bell_draw(rng, shape, spread, limit, pieces=(), kind=jnp.bfloat16):
    loudness = block_levels(rng, shape, pieces, -0.22, 0.18) if pieces else 1.0
    array = jax.random.normal(rng, shape, jnp.float32) * spread * loudness
    return jnp.minimum(jnp.maximum(array, -limit), limit).astype(kind)


def setup_inputs(seed: int = 0) -> dict:
    keys = jax.random.split(jax.random.key(seed), 7)
    return {
        "latent": bell_draw(keys[0], (NT, NH, NW, C), 1.0, 6.0, ((0, 4), (1, 2), (2, 4))),
        "cotangent": bell_draw(keys[1], (NT, NH, NW, C), 1.0, 6.0, ((0, 4), (1, 2), (2, 4))),
        "gain_one": jnp.clip(jnp.exp(jax.random.uniform(keys[2], (C,), jnp.float32, math.log(0.5), math.log(2.0))), 0.5, 2.0),
        "gain_two": jnp.clip(jnp.exp(jax.random.uniform(keys[3], (C,), jnp.float32, math.log(0.5), math.log(2.0))), 0.5, 2.0),
        "kernel_one": bell_draw(keys[4], (3, 3, 3, C, C), (27 * C) ** -0.5, 0.0625, ((3, 4),)),
        "kernel_two": bell_draw(keys[5], (3, 3, 3, C, C), (27 * C) ** -0.5, 0.0625, ((3, 4),)),
    }


epsilon = 1e-06

def normalize(values, gain):
    inverse = lax.rsqrt(lax.optimization_barrier(jnp.mean(values * values, axis=-1, keepdims=True)) + epsilon)
    return (values * inverse * gain, inverse)

def norm_backward(values, inverse, gain, upstream):
    scaled = upstream * gain
    return inverse * scaled - values * inverse ** 3 * lax.optimization_barrier(jnp.mean(values * scaled, axis=-1, keepdims=True))

def silu_slope(normed):
    sigma = jax.nn.sigmoid(normed)
    return sigma * (1.0 + normed * (1.0 - sigma))

def forward_kernel(weight):
    swapped = jnp.swapaxes(weight, 3, 4)
    return swapped.reshape(3, 3, 3 * swapped.shape[3], swapped.shape[4])

def backward_kernel(weight):
    flipped = weight[::-1, ::-1, ::-1]
    return flipped.reshape(3, 3, 3 * flipped.shape[3], flipped.shape[4])

def conv_taps(padded, kernel, frame_count, row_count, col_count):
    summed = jnp.zeros((frame_count * row_count * col_count, kernel.shape[3]), jnp.float32)
    for time_tap in range(3):
        for row_tap in range(3):
            columns = jnp.concatenate([padded[time_tap:time_tap + frame_count, row_tap:row_tap + row_count, col_tap:col_tap + col_count] for col_tap in range(3)], axis=-1)
            columns = columns.reshape(frame_count * row_count * col_count, columns.shape[-1])
            summed = summed + jnp.dot(columns, kernel[time_tap, row_tap], preferred_element_type=jnp.float32)
    return summed.reshape(frame_count, row_count, col_count, kernel.shape[3])

def conv_whole(padded, kernel):

    def one_frame(index):
        window = lax.dynamic_slice_in_dim(padded, index, 3, 0)
        return conv_taps(window, kernel, 1, NH, NW)[0]
    return lax.map(one_frame, jnp.arange(NT, dtype=jnp.int32))

def reference(latent, cotangent, gain_one, gain_two, kernel_one, kernel_two):
    ahead = ((2, 0), (1, 1), (1, 1), (0, 0))
    behind = ((0, 2), (1, 1), (1, 1), (0, 0))
    source = latent.astype(jnp.float32)
    normed_one, inverse_one = normalize(source, gain_one)
    active_one = jax.nn.silu(normed_one).astype(jnp.bfloat16)
    inner = conv_whole(jnp.pad(active_one, ahead), forward_kernel(kernel_one))
    normed_two, inverse_two = normalize(inner, gain_two)
    active_two = jax.nn.silu(normed_two).astype(jnp.bfloat16)
    branch = conv_whole(jnp.pad(active_two, ahead), forward_kernel(kernel_two))
    block_out = (source + branch).astype(jnp.bfloat16)
    grad_two = conv_whole(jnp.pad(cotangent, behind), backward_kernel(kernel_two))
    grad_inner = norm_backward(inner, inverse_two, gain_two, grad_two * silu_slope(normed_two)).astype(jnp.bfloat16)
    grad_one = conv_whole(jnp.pad(grad_inner, behind), backward_kernel(kernel_one))
    latent_grad = cotangent.astype(jnp.float32) + norm_backward(source, inverse_one, gain_one, grad_one * silu_slope(normed_one))
    return (block_out, latent_grad.astype(jnp.bfloat16))
```

```python
import functools

import jax
import jax.numpy as jnp
from jax import lax
from jax.experimental import pallas as pl
from jax.experimental.pallas import tpu as pltpu
from jax.sharding import PartitionSpec as P

epsilon = 1e-06
MESH = pl.DeviceIdType.MESH
bf16, f32 = jnp.bfloat16, jnp.float32
EXACT = lax.Precision.HIGHEST


def normalize(values, gain):
    inverse = lax.rsqrt(jnp.mean(values * values, axis=-1, keepdims=True) + epsilon)
    return values * inverse * gain, inverse


def norm_backward(values, inverse, gain, upstream):
    scaled = upstream * gain
    mean = jnp.mean(values * scaled, axis=-1, keepdims=True)
    return inverse * scaled - values * (inverse * inverse * inverse) * mean


def silu(normed):
    return normed / (1.0 + jnp.exp(-normed))


def silu_slope(normed):
    sigma = 1.0 / (1.0 + jnp.exp(-normed))
    return sigma * (1.0 + normed * (1.0 - sigma))


def shift_sum(taps, width, size):
    rows = taps.shape[0]
    column = lax.rem(lax.broadcasted_iota(jnp.int32, (rows, size), 0), width)
    low = pltpu.roll(taps[:, :size], 1, axis=0)
    high = pltpu.roll(taps[:, 2 * size :], rows - 1, axis=0)
    return (
        taps[:, size : 2 * size]
        + jnp.where(column == 0, 0.0, low)
        + jnp.where(column == width - 1, 0.0, high)
    )


def pad_to(value, axis, size):
    shape = list(value.shape)
    if shape[axis] == size:
        return value
    shape[axis] = size - shape[axis]
    return jnp.concatenate([value, jnp.zeros(shape, value.dtype)], axis=axis)


class Links:
    def __init__(self, send, recv):
        self.send, self.recv, self.all = send, recv, []

    def copy(self, src, dst, device, sends=True, receives=True):
        made = Copy(self, len(self.all), src, dst, device, sends, receives)
        self.all.append(made)
        return made

    def drain(self):
        for made in self.all:
            made.drain()


class Copy:
    def __init__(self, links, slot, src, dst, device, sends, receives):
        self.made = lambda: pltpu.make_async_remote_copy(
            src_ref=src,
            dst_ref=dst,
            send_sem=links.send.at[slot],
            recv_sem=links.recv.at[slot],
            device_id=device,
            device_id_type=MESH,
        )
        self.sends, self.receives = sends, receives

    def start(self):
        when(self.sends, lambda: self.made().start())

    def wait(self):
        when(self.receives, lambda: self.made().wait_recv())

    def drain(self):
        when(self.sends, lambda: self.made().wait_send())


def when(condition, action):
    if condition is True:
        action()
    else:
        pl.when(condition)(action)


def kernel(sizes, latent, cotangent, gain_one, gain_two, kernel_one, kernel_two, out, latent_grad, *scratch):
    S, Q, Z = sizes
    (
        w_one, w_two, w_gap, act, xp, qs, qp, gs, gr, fs, fr, vall, st, gains,
        xq, gi, gh, gu, gd, qq, yf, rf, rp, yb, rb, g_sum, send, recv, w_sem,
    ) = scratch
    F, R, W, C = latent.shape
    O = kernel_one.shape[3]
    WW = W * Z
    OP = -(-O // 128) * 128
    rows = F * R * W
    s, q, z = lax.axis_index("section"), lax.axis_index("seq"), lax.axis_index("exp")
    has_next, has_prev = s < S - 1, s > 0
    has_high, has_low = q < Q - 1, q > 0
    both = jnp.logical_and
    nxt, prv = jnp.minimum(s + 1, S - 1), jnp.maximum(s - 1, 0)
    upper, lower = jnp.minimum(q + 1, Q - 1), jnp.maximum(q - 1, 0)
    body, own, halo = pl.ds(1, R), pl.ds(0, F), pl.ds(F, 2)
    two = pl.ds(0, 2)
    links = Links(send, recv)

    load_one = pltpu.make_async_copy(kernel_one, w_one, w_sem.at[0])
    load_two = pltpu.make_async_copy(kernel_two, w_two, w_sem.at[1])
    load_two.start()
    load_one.start()

    barrier = pltpu.get_barrier_semaphore()

    def greet(device):
        pl.semaphore_signal(barrier, inc=1, device_id=device, device_id_type=MESH)

    for d in range(1, Z):
        greet((s, q, lax.rem(z + d, Z)))
    for near, step in ((has_next, 1), (has_prev, -1)):

        @pl.when(near)
        def _():
            for d in range(Z):
                greet((s + step, q, lax.rem(z + d, Z)))

        for side, move in ((has_high, 1), (has_low, -1)):

            @pl.when(both(near, side))
            def _():
                greet((s + step, q + move, z))

    for side, move in ((has_high, 1), (has_low, -1)):

        @pl.when(side)
        def _():
            greet((s, q + move, z))

    def peer(d):
        return lax.rem(z + d + Z, Z)

    def block(index):
        return pl.ds(pl.multiple_of(index * W, W), W)

    def gather(source, at):
        arrive = []
        for d in range(1, Z):
            for sign in (1, -1):
                if d <= 2:
                    target, sends = z + sign * d, (z + d < Z) if sign > 0 else (z >= d)
                    src, dst = source, at(z)
                else:
                    target = z + sign
                    held = z - sign * (d - 1)
                    sends = both(z < Z - 1, z >= d - 1) if sign > 0 else both(z > 0, z <= Z - d)
                    src = dst = at(jnp.clip(held, 0, Z - 1))
                receives = (z >= d) if sign > 0 else (z + d < Z)
                target = jnp.clip(target, 0, Z - 1)
                arrive.append((d, z - sign * d, links.copy(src, dst, (s, q, target), sends, receives)))
        return arrive

    def gather_start(arrive):
        for d in (2, 1):
            for distance, _, made in arrive:
                if distance == d:
                    made.start()

    def gather_wait(arrive, d, use=None):
        for distance, owner, made in arrive:
            if distance == d:
                made.wait()
        for distance, owner, made in arrive:
            if distance == d + 1 and d >= 2:
                made.start()
        if use is not None:
            for distance, owner, made in arrive:
                if distance == d:
                    when(made.receives, functools.partial(use, owner))

    q_own = {d: links.copy(qs.at[peer(d)], qp.at[own, body, block(z)], (s, q, peer(d))) for d in range(1, Z)}
    q_next = {
        d: links.copy(
            qp.at[two, body, block(peer(-d))], qp.at[halo, body, block(peer(-d))], (prv, q, z), has_prev, has_next
        )
        for d in range(Z)
    }

    def rows_out(src, dst, device, towards):
        sides = (has_high, has_low) if towards > 0 else (has_low, has_high)
        return links.copy(src, dst, device, *sides)

    q_rows = [
        rows_out(qp.at[own, R], qp.at[own, 0], (s, upper, z), 1),
        rows_out(qp.at[own, 1], qp.at[own, R + 1], (s, lower, z), -1),
    ]
    q_corner = [
        links.copy(qp.at[two, R], qp.at[halo, 0], (prv, upper, z), both(has_prev, has_high), both(has_next, has_low)),
        links.copy(qp.at[two, 1], qp.at[halo, R + 1], (prv, lower, z), both(has_prev, has_low), both(has_next, has_high)),
    ]
    x_rows = [
        rows_out(xp.at[:, R], xp.at[:, 0], (s, upper, z), 1),
        rows_out(xp.at[:, 1], xp.at[:, R + 1], (s, lower, z), -1),
    ]
    x_all = gather(act, lambda owner: xp.at[:, body, block(owner)])
    g_out = {
        (d, f): links.copy(gs.at[peer(d), f], gr.at[d, f], (s, q, peer(d))) for d in range(1, Z) for f in range(F)
    }
    f_out = [links.copy(fs.at[t], fr.at[t], (nxt, q, z), has_next, has_prev) for t in range(2)]
    v_all = gather(vall.at[z], lambda owner: vall.at[owner])
    sums = [{d: links.copy(st.at[k, 0], st.at[k, d], (s, q, peer(d))) for d in range(1, Z)} for k in range(2)]
    xq_rows = [
        rows_out(xq.at[:, :, R], xq.at[:, :, 0], (s, upper, z), 1),
        rows_out(xq.at[:, :, 1], xq.at[:, :, R + 1], (s, lower, z), -1),
    ]
    gi_next = links.copy(gi.at[two], gh, (prv, q, z), has_prev, has_next)
    gi_rows = [
        rows_out(gi.at[:, R - 1], gd.at[own], (s, upper, z), 1),
        rows_out(gi.at[:, 0], gu.at[own], (s, lower, z), -1),
    ]
    gi_corner = [
        links.copy(gi.at[two, R - 1], gd.at[halo], (prv, upper, z), both(has_prev, has_high), both(has_next, has_low)),
        links.copy(gi.at[two, 0], gu.at[halo], (prv, lower, z), both(has_prev, has_low), both(has_next, has_high)),
    ]
    b_out = {
        (d, f): links.copy(yb.at[f, :, block(peer(d))], rb.at[d, f], (s, q, peer(d)))
        for d in range(1, Z)
        for f in range(F)
    }
    y_own = {d: links.copy(yf.at[own, :, block(peer(d))], rf.at[z], (s, q, peer(d))) for d in range(1, Z)}
    y_next = {
        d: links.copy(yf.at[halo, :, block(peer(d))], rp.at[z], (nxt, q, peer(d)), has_next, has_prev)
        for d in range(Z)
    }

    lane = lax.broadcasted_iota(jnp.int32, (8, C), 1)
    group = lax.broadcasted_iota(jnp.int32, (8, C), 0)
    segments = jnp.where(both(lane >= group * O, lane < group * O + O), 1.0, 0.0).astype(f32)

    def pack(value, offset=0):
        count = value.shape[0] // WW
        grouped = value.reshape(count, Z, W, value.shape[1])
        return jnp.concatenate(
            [grouped[:, m].reshape(count * W, value.shape[1])[:, offset : offset + O] for m in range(Z)], axis=1
        )

    def unpack(packed, m):
        return pad_to(packed[:, m * O : (m + 1) * O], 1, OP)

    def segment_sums(value):
        return lax.dot_general(segments, value, (((1,), (1,)), ((), ())), precision=EXACT, preferred_element_type=f32)

    def spread(tile):
        return lax.dot_general(tile, segments, (((0,), (0,)), ((), ())), precision=EXACT, preferred_element_type=f32)

    def rhs_forward(w, i, K):
        return jnp.concatenate(
            [jnp.concatenate([pad_to(w[i, j, l], 0, OP) for l in range(3)], axis=0) for j in range(3)], axis=1
        )

    def rhs_backward(w, i):
        return jnp.concatenate(
            [jnp.concatenate([pad_to(w[2 - i, 2 - j, 2 - l], 0, OP) for l in range(3)], axis=1) for j in range(3)],
            axis=0,
        )

    def forward(lhs_of, w, t):
        total = None
        for i in range(3):
            f = t + i - 2
            if not 0 <= f < F:
                continue
            part = lax.dot_general(
                lhs_of(f), rhs_forward(w, i, None), (((1,), (1,)), ((), ())), preferred_element_type=f32
            )
            total = part if total is None else total + part
        return shift_sum(total, WW, OP)[:, :O]

    def backward(qbuf, w, f, taps):
        total = None
        for i in taps:
            lhs = jnp.concatenate(
                [pad_to(qbuf[f + i, pl.ds(j, R)].reshape(R * WW, qbuf.shape[3]), 1, OP) for j in range(3)], axis=1
            )
            part = jnp.dot(lhs, rhs_backward(w, i), preferred_element_type=f32)
            total = part if total is None else total + part
        return total

    source = latent[...].reshape(rows, C).astype(f32)
    g_one, g_two = gain_one[...].reshape(1, C), gain_two[...].reshape(1, C)
    normed_one, _ = normalize(source, g_one)
    act[...] = silu(normed_one).astype(bf16).reshape(F, R, W, C)
    for m in range(Z):
        qs[m] = cotangent[:, :, :, m * O : (m + 1) * O]

    near = has_next.astype(jnp.int32) + has_prev.astype(jnp.int32)
    sides = has_high.astype(jnp.int32) + has_low.astype(jnp.int32)
    pl.semaphore_wait(barrier, Z - 1 + Z * near + sides + near * sides)

    for d in sorted(range(1, Z), key=lambda d: -abs(2 * d - Z)):
        q_own[d].start()
    gather_start(x_all)
    qp[own, body, block(z)] = qs[z]
    xp[:, body, block(z)] = act[...]
    q_next[0].start()

    def zero(ref, index):
        ref[index] = jnp.zeros_like(ref[index])

    full = slice(None)

    @pl.when(jnp.logical_not(has_next))
    def _():
        zero(qp, (halo,))
        zero(qq, (halo,))

    for missing, row in ((jnp.logical_not(has_low), 0), (jnp.logical_not(has_high), R + 1)):

        @pl.when(missing)
        def _():
            zero(qp, (full, row))
            zero(qq, (full, row))
            zero(xp, (full, row))
            zero(xq, (full, full, row))

    @pl.when(jnp.logical_not(has_prev))
    def _():
        zero(fr, (full,))
        zero(rp, (full,))

    for m in range(Z):
        gains[m] = jnp.broadcast_to(jnp.concatenate([g_two[:, m * O : (m + 1) * O]] * Z, axis=1), (8, C))

    for d in range(1, Z):
        q_own[d].wait()
        q_next[d].start()
    for made in q_rows + q_corner:
        made.start()
    gather_wait(x_all, 2)
    load_two.wait()
    for i in range(3):
        for j in range(3):
            for l in range(3):
                w = w_two[i, j, l].astype(f32)
                w_gap[i, j, l] = jnp.concatenate(
                    [pad_to(w[:, m * O : (m + 1) * O], 1, OP) for m in range(Z)], axis=1
                ).astype(bf16)
    for made in q_rows:
        made.wait()
    for d in range(Z):
        q_next[d].wait()
    for made in q_corner:
        made.wait()
    for f in range(F):
        total = shift_sum(backward(qp, w_two, f, range(3)), WW, C)
        for m in range(Z):
            gs[m, f] = pack(total, m * O).astype(bf16).reshape(R, W, C)
        for d in sorted(range(1, Z), key=lambda d: -abs(2 * d - Z)):
            g_out[d, f].start()

    gather_wait(x_all, 1)
    for d in range(3, Z):
        gather_wait(x_all, d)
    for made in x_rows:
        made.start()
    load_one.wait()
    for made in x_rows:
        made.wait()

    def lhs_one(f):
        return jnp.concatenate([xp[f, pl.ds(j, R)].reshape(R * WW, C) for j in range(3)], axis=1)

    for t in (F + 1, F):
        fs[t - F] = pack(forward(lhs_one, w_one, t)).astype(bf16).reshape(R, W, C)
        f_out[t - F].start()
    inner = [pack(forward(lhs_one, w_one, t)) for t in range(F)]
    for made in f_out:
        made.wait()
    for t in range(2):
        inner[t] = inner[t] + fr[t].reshape(R * W, C).astype(f32)
    inner = jnp.concatenate(inner, axis=0)
    vall[z] = inner.astype(bf16).reshape(F, R, W, C)
    st[0, 0] = segment_sums(inner * inner)
    for d in range(1, Z):
        sums[0][d].start()
    gather_start(v_all)

    grad_two = gs[z].astype(f32)
    for d in range(1, Z):
        for f in range(F):
            g_out[d, f].wait()
        grad_two = grad_two + gr[d].astype(f32)
    grad_two = grad_two.reshape(rows, C)
    squares = st[0, 0]
    for d in range(1, Z):
        sums[0][d].wait()
        squares = squares + st[0, d]
    inverse = lax.rsqrt(squares / C + epsilon)
    inverse_wide = spread(inverse)
    gain = gains[z][0:1]
    scaled = grad_two * silu_slope(inner * inverse_wide * gain) * gain
    st[1, 0] = segment_sums(inner * scaled)
    for d in range(1, Z):
        sums[1][d].start()

    def activate(owner):
        value = vall[owner].reshape(rows, C).astype(f32)
        active = silu(value * spread(inverse) * gains[owner][0:1])
        for m in range(Z):
            xq[owner, :, body, m * W : (m + 1) * W] = unpack(active, m).astype(bf16).reshape(F, R, W, OP)

    activate(z)
    gather_wait(v_all, 2, activate)
    gather_wait(v_all, 1, activate)

    means = st[1, 0]
    for d in range(1, Z):
        sums[1][d].wait()
        means = means + st[1, d]
    factor = spread(inverse * inverse * inverse * means / C)
    grad_inner = (inverse_wide * scaled - inner * factor).astype(bf16)
    gi[...] = grad_inner.reshape(F, R, W, C)
    gi_next.start()
    for made in gi_rows + gi_corner:
        made.start()

    def place(ref, frames, band, count):
        value = ref.reshape(count, C).astype(f32)
        for m in range(Z):
            piece = unpack(value, m).astype(bf16)
            qq[frames, band, m * W : (m + 1) * W] = piece.reshape(
                qq.at[frames, band, m * W : (m + 1) * W].shape
            )

    for d in range(3, Z):
        gather_wait(v_all, d, activate)
    for made in xq_rows:
        made.start()
    place(gi[...], own, body, rows)
    for made in xq_rows:
        made.wait()

    def lhs_two(f):
        return jnp.concatenate(
            [xq[m, f, pl.ds(j, R)].reshape(R * WW, OP) for j in range(3) for m in range(Z)], axis=1
        )

    for t in (F, F + 1):
        yf[t] = forward(lhs_two, w_gap, t).astype(bf16).reshape(R, WW, O)
    for d in range(Z):
        y_next[d].start()
    for t in range(F):
        yf[t] = forward(lhs_two, w_gap, t).astype(bf16).reshape(R, WW, O)
    for d in range(1, Z):
        y_own[d].start()
    rf[z] = yf[own, :, block(z)]

    for made in gi_rows + gi_corner + [gi_next]:
        made.wait()

    @pl.when(has_next)
    def _():
        place(gh[...], halo, body, 2 * R * W)

    for side, ref, row in ((has_low, gd, 0), (has_high, gu, R + 1)):

        @pl.when(side)
        def _():
            place(ref[own], own, row, F * W)

        @pl.when(both(side, has_next))
        def _():
            place(ref[halo], halo, row, 2 * W)

    for f in range(F):
        yb[f] = shift_sum(backward(qq, w_one, f, range(3)), WW, C).astype(bf16).reshape(R, WW, C)
        for d in sorted(range(1, Z), key=lambda d: -abs(2 * d - Z)):
            b_out[d, f].start()

    for d in range(1, Z):
        y_own[d].wait()
    for d in range(Z):
        y_next[d].wait()
    chunks = []
    for m in range(Z):
        head = rf[m, two].astype(f32) + rp[m].astype(f32)
        if F > 2:
            head = jnp.concatenate([head, rf[m, pl.ds(2, F - 2)].astype(f32)], axis=0)
        chunks.append(head.reshape(rows, O))
    branch = jnp.concatenate(chunks, axis=1)
    source = latent[...].reshape(rows, C).astype(f32)
    out[...] = (source + branch).astype(bf16).reshape(F, R, W, C)

    grad_one = yb[:, :, block(z)].astype(f32)
    for d in range(1, Z):
        for f in range(F):
            b_out[d, f].wait()
        grad_one = grad_one + rb[d].astype(f32)
    grad_one = grad_one.reshape(rows, C)
    normed_one, inverse_one = normalize(source, g_one)
    grad = norm_backward(source, inverse_one, g_one, grad_one * silu_slope(normed_one))
    upstream = cotangent[...].reshape(rows, C).astype(f32)
    latent_grad[...] = (upstream + grad).astype(bf16).reshape(F, R, W, C)
    links.drain()


def local(sizes, latent, cotangent, gain_one, gain_two, kernel_one, kernel_two):
    S, Q, Z = sizes
    F, R, W, C = latent.shape
    O = kernel_one.shape[3]
    WW = W * Z
    OP = -(-O // 128) * 128
    rows = F * R * W
    taps = kernel_one.shape[:3]
    packed = (F, R, W, C)
    slots = 128
    shapes = [
        kernel_one.shape,
        kernel_two.shape,
        taps + (O, Z * OP),
        packed,
        (F, R + 2, WW, C),
        (Z, F, R, W, O),
        (F + 2, R + 2, WW, O),
        (Z,) + packed,
        (Z,) + packed,
        (2, R, W, C),
        (2, R, W, C),
        (Z,) + packed,
        None,
        None,
        (Z, F, R + 2, WW, OP),
        packed,
        (2, R, W, C),
        (F + 2, W, C),
        (F + 2, W, C),
        (F + 2, R + 2, WW, OP),
        (F + 2, R, WW, O),
        (Z, F, R, W, O),
        (Z, 2, R, W, O),
        (F, R, WW, C),
        (Z,) + packed,
        None,
    ]
    scratch = [pltpu.VMEM(shape, bf16) if shape else None for shape in shapes]
    scratch[12] = pltpu.VMEM((2, Z, 8, rows), f32)
    scratch[13] = pltpu.VMEM((Z, 8, C), f32)
    scratch[25] = pltpu.VMEM((8, 128), f32)
    vmem = pl.BlockSpec(memory_space=pltpu.VMEM)
    hbm = pl.BlockSpec(memory_space=pl.ANY)
    return pl.pallas_call(
        functools.partial(kernel, sizes),
        out_shape=[jax.ShapeDtypeStruct((F, R, W, C), bf16)] * 2,
        in_specs=[vmem, vmem, vmem, vmem, hbm, hbm],
        out_specs=[vmem, vmem],
        scratch_shapes=[
            *scratch,
            pltpu.SemaphoreType.DMA((slots,)),
            pltpu.SemaphoreType.DMA((slots,)),
            pltpu.SemaphoreType.DMA((2,)),
        ],
        compiler_params=pltpu.CompilerParams(
            collective_id=0, has_side_effects=True, vmem_limit_bytes=60 * 1024 * 1024
        ),
    )(latent, cotangent, gain_one, gain_two, kernel_one, kernel_two)


def solution(mesh):
    sizes = (mesh.shape["section"], mesh.shape["seq"], mesh.shape["exp"])
    spread = P("section", "seq", "exp", None)
    split = P(None, None, None, "exp", None)
    return jax.shard_map(
        functools.partial(local, sizes),
        mesh=mesh,
        in_specs=(spread, spread, P(), P(), split, split),
        out_specs=(spread, spread),
        check_vma=False,
    )
```

```python
import functools

import jax
import jax.numpy as jnp
from jax import lax
from jax.experimental import pallas as pl
from jax.experimental.pallas import tpu as pltpu
from jax.sharding import PartitionSpec as P

epsilon = 1e-06
MESH = pl.DeviceIdType.MESH
bf16, f32 = jnp.bfloat16, jnp.float32
EXACT = lax.Precision.HIGHEST


def normalize(values, gain):
    inverse = lax.rsqrt(jnp.mean(values * values, axis=-1, keepdims=True) + epsilon)
    return values * inverse * gain, inverse


def norm_backward(values, inverse, gain, upstream):
    scaled = upstream * gain
    mean = jnp.mean(values * scaled, axis=-1, keepdims=True)
    return inverse * scaled - values * (inverse * inverse * inverse) * mean


def silu(normed):
    return normed / (1.0 + jnp.exp(-normed))


def silu_slope(normed):
    sigma = 1.0 / (1.0 + jnp.exp(-normed))
    return sigma * (1.0 + normed * (1.0 - sigma))


def shift_sum(taps, width, size):
    rows = taps.shape[0]
    column = lax.rem(lax.broadcasted_iota(jnp.int32, (rows, size), 0), width)
    low = pltpu.roll(taps[:, :size], 1, axis=0)
    high = pltpu.roll(taps[:, 2 * size :], rows - 1, axis=0)
    return (
        taps[:, size : 2 * size]
        + jnp.where(column == 0, 0.0, low)
        + jnp.where(column == width - 1, 0.0, high)
    )


def fold_of(rows, width):
    return next((n for n in (4, 2) if rows % n == 0 and n * width % 128 == 0), 1)


def pad_to(value, axis, size):
    shape = list(value.shape)
    if shape[axis] == size:
        return value
    shape[axis] = size - shape[axis]
    return jnp.concatenate([value, jnp.zeros(shape, value.dtype)], axis=axis)


class Links:
    def __init__(self, send, recv):
        self.send, self.recv, self.all = send, recv, []

    def copy(self, src, dst, device, sends=True, receives=True):
        made = Copy(self, len(self.all), src, dst, device, sends, receives)
        self.all.append(made)
        return made

    def drain(self):
        for made in self.all:
            made.drain()


class Copy:
    def __init__(self, links, slot, src, dst, device, sends, receives):
        self.made = lambda: pltpu.make_async_remote_copy(
            src_ref=src,
            dst_ref=dst,
            send_sem=links.send.at[slot],
            recv_sem=links.recv.at[slot],
            device_id=device,
            device_id_type=MESH,
        )
        self.sends, self.receives = sends, receives

    def start(self):
        when(self.sends, lambda: self.made().start())

    def wait(self):
        when(self.receives, lambda: self.made().wait_recv())

    def drain(self):
        when(self.sends, lambda: self.made().wait_send())


def when(condition, action):
    if condition is True:
        action()
    else:
        pl.when(condition)(action)


def kernel(sizes, latent_hbm, cotangent_hbm, gain_one_hbm, gain_two_hbm, kernel_one, kernel_two, out_hbm, latent_grad_hbm, *scratch):
    S, Q, Z = sizes
    (
        w_one, w_two, w_gap, act, xp, qs, qp, gs, gr, fs, fr, vall, st, gains,
        xq, gi, gh, gu, gd, qq, yf, rf, ys, yr, yb, rb, g_hop, b_hop,
        latent, cotangent, gain_one, gain_two, out, latent_grad, send, recv, w_sem,
    ) = scratch
    F, R, W, C = latent_hbm.shape
    O = kernel_one.shape[3]
    WW = W * Z
    OP = -(-O // 128) * 128
    rows = F * R * W
    s, q, z = lax.axis_index("section"), lax.axis_index("seq"), lax.axis_index("exp")
    has_next, has_prev = s < S - 1, s > 0
    has_high, has_low = q < Q - 1, q > 0
    both = jnp.logical_and
    nxt, prv = jnp.minimum(s + 1, S - 1), jnp.maximum(s - 1, 0)
    upper, lower = jnp.minimum(q + 1, Q - 1), jnp.maximum(q - 1, 0)
    fold = fold_of(R, O)
    body, own, halo = pl.ds(1, R), pl.ds(0, F), pl.ds(F, 2)
    two = pl.ds(0, 2)
    links = Links(send, recv)

    barrier = pltpu.get_barrier_semaphore()
    loads = [
        pltpu.make_async_copy(src, dst, w_sem.at[k])
        for k, (src, dst) in enumerate(
            [
                (cotangent_hbm, cotangent),
                (latent_hbm, latent),
                (gain_one_hbm, gain_one),
                (gain_two_hbm, gain_two),
                (kernel_two, w_two),
                (kernel_one, w_one),
            ]
        )
    ]
    load_two, load_one = loads[4:]
    stores = [
        pltpu.make_async_copy(out, out_hbm, w_sem.at[6]),
        pltpu.make_async_copy(latent_grad, latent_grad_hbm, w_sem.at[7]),
    ]
    for load in loads[:4]:
        load.start()

    def greet(device):
        pl.semaphore_signal(barrier, inc=1, device_id=device, device_id_type=MESH)

    for d in range(1, Z):
        greet((s, q, lax.rem(z + d, Z)))
    for near, step in ((has_next, 1), (has_prev, -1)):

        @pl.when(near)
        def _():
            for d in range(Z):
                greet((s + step, q, lax.rem(z + d, Z)))

        for side, move in ((has_high, 1), (has_low, -1)):

            @pl.when(both(near, side))
            def _():
                greet((s + step, q + move, z))

    for side, move in ((has_high, 1), (has_low, -1)):

        @pl.when(side)
        def _():
            greet((s, q + move, z))

    for load in loads[4:]:
        load.start()

    def peer(d):
        return lax.rem(z + d + Z, Z)

    def block(index):
        return pl.ds(pl.multiple_of(index * W, W), W)

    def gather(source, at):
        arrive = []
        for d in range(1, Z):
            for sign in (1, -1):
                if d <= 2:
                    target, sends = z + sign * d, (z + d < Z) if sign > 0 else (z >= d)
                    src, dst = source, at(z)
                else:
                    target = z + sign
                    held = z - sign * (d - 1)
                    sends = both(z < Z - 1, z >= d - 1) if sign > 0 else both(z > 0, z <= Z - d)
                    src = dst = at(jnp.clip(held, 0, Z - 1))
                receives = (z >= d) if sign > 0 else (z + d < Z)
                target = jnp.clip(target, 0, Z - 1)
                arrive.append((d, z - sign * d, links.copy(src, dst, (s, q, target), sends, receives)))
        return arrive

    def gather_start(arrive):
        for d in (2, 1):
            for distance, _, made in arrive:
                if distance == d:
                    made.start()

    def gather_wait(arrive, d, use=None):
        for distance, owner, made in arrive:
            if distance == d:
                made.wait()
        for distance, owner, made in arrive:
            if distance == d + 1 and d >= 2:
                made.start()
        if use is not None:
            for distance, owner, made in arrive:
                if distance == d:
                    when(made.receives, functools.partial(use, owner))

    class Scatter:
        def __init__(self, at, landing, hop):
            self.at, self.landing, self.hop, self.far, self.near = at, landing, hop, {}, {}
            for sign in (1, -1):
                for D in range(Z - 1, 0, -1):
                    for f in range(F):
                        target, origin = z + sign * D, z - sign * D
                        sends = (z + D < Z) if sign > 0 else (z >= D)
                        src = at(jnp.clip(target, 0, Z - 1), f)
                        if D >= 3:
                            before = (z >= 1) if sign > 0 else (z < Z - 1)
                            further = (z + D <= Z) if sign > 0 else (z >= D - 1)
                            self.far[sign, D, f] = links.copy(
                                src, hop.at[int(sign > 0), D - 3, f], (s, q, jnp.clip(z + sign, 0, Z - 1)), sends, both(before, further)
                            )
                        else:
                            receives = (z >= D) if sign > 0 else (z + D < Z)
                            slot = 2 * (sign > 0) + D - 1
                            self.near[sign, D, f] = links.copy(
                                src, landing.at[slot, f], (s, q, jnp.clip(target, 0, Z - 1)), sends, receives
                            )

        def start(self, f):
            for D in range(Z - 1, 0, -1):
                for sign in (1, -1):
                    made = self.far.get((sign, D, f)) or self.near[sign, D, f]
                    joined = self.far.get((sign, D + 1, f))
                    if joined is None:
                        made.start()
                    else:
                        when(both(made.sends, jnp.logical_not(joined.receives)), lambda: made.made().start())

        def join(self, f):
            for D in range(Z - 1, 2, -1):
                for sign in (1, -1):
                    arrived = self.far[sign, D, f]
                    onward = self.far.get((sign, D - 1, f)) or self.near[sign, D - 1, f]

                    @pl.when(arrived.receives)
                    def _():
                        arrived.made().wait_recv()
                        held = self.at(jnp.clip(z + sign * (D - 1), 0, Z - 1), f)
                        total = held[...].astype(f32) + self.hop[int(sign > 0), D - 3, f].astype(f32)
                        held[...] = total.astype(bf16)
                        onward.made().start()

        def total(self, own):
            for D in (1, 2):
                for sign in (1, -1):
                    for f in range(F):
                        if (sign, D, f) in self.near:
                            self.near[sign, D, f].wait()
            for D in (1, 2):
                for sign in (1, -1):
                    if (sign, D, 0) in self.near:
                        made = self.near[sign, D, 0]
                        term = self.landing[2 * (sign > 0) + D - 1].astype(f32)
                        own = own + jnp.where(made.receives, term, 0.0)
            return own

    q_own = {d: links.copy(qs.at[peer(d)], qp.at[own, body, block(z)], (s, q, peer(d))) for d in range(1, Z)}
    q_next = {
        d: links.copy(
            qp.at[two, body, block(peer(-d))], qp.at[halo, body, block(peer(-d))], (prv, q, z), has_prev, has_next
        )
        for d in range(Z)
    }

    def rows_out(src, dst, device, towards):
        sides = (has_high, has_low) if towards > 0 else (has_low, has_high)
        return links.copy(src, dst, device, *sides)

    q_rows = [
        rows_out(qp.at[own, R], qp.at[own, 0], (s, upper, z), 1),
        rows_out(qp.at[own, 1], qp.at[own, R + 1], (s, lower, z), -1),
    ]
    q_corner = [
        links.copy(qp.at[two, R], qp.at[halo, 0], (prv, upper, z), both(has_prev, has_high), both(has_next, has_low)),
        links.copy(qp.at[two, 1], qp.at[halo, R + 1], (prv, lower, z), both(has_prev, has_low), both(has_next, has_high)),
    ]
    x_rows = [
        rows_out(xp.at[:, R], xp.at[:, 0], (s, upper, z), 1),
        rows_out(xp.at[:, 1], xp.at[:, R + 1], (s, lower, z), -1),
    ]
    x_all = gather(act, lambda owner: xp.at[:, body, block(owner)])
    g_out = Scatter(lambda owner, f: gs.at[owner, f], gr, g_hop)
    f_out = [links.copy(fs.at[t], fr.at[t], (nxt, q, z), has_next, has_prev) for t in range(2)]
    v_all = gather(vall.at[z], lambda owner: vall.at[owner])
    sums = [{d: links.copy(st.at[k, 0], st.at[k, d], (s, q, peer(d))) for d in range(1, Z)} for k in range(2)]
    xq_rows = [
        rows_out(xq.at[:, :, R], xq.at[:, :, 0], (s, upper, z), 1),
        rows_out(xq.at[:, :, 1], xq.at[:, :, R + 1], (s, lower, z), -1),
    ]
    gi_next = links.copy(gi.at[two], gh, (prv, q, z), has_prev, has_next)
    gi_rows = [
        rows_out(gi.at[:, R - 1], gd.at[own], (s, upper, z), 1),
        rows_out(gi.at[:, 0], gu.at[own], (s, lower, z), -1),
    ]
    gi_corner = [
        links.copy(gi.at[two, R - 1], gd.at[halo], (prv, upper, z), both(has_prev, has_high), both(has_next, has_low)),
        links.copy(gi.at[two, 0], gu.at[halo], (prv, lower, z), both(has_prev, has_low), both(has_next, has_high)),
    ]
    b_out = Scatter(lambda owner, f: yb.at[f, :, block(owner)], rb, b_hop)
    y_own = {d: links.copy(yf.at[peer(d)], rf.at[z], (s, q, peer(d))) for d in range(1, Z)}
    y_next = [links.copy(ys.at[t], yr.at[t], (nxt, q, z), has_next, has_prev) for t in range(2)]

    lane = lax.broadcasted_iota(jnp.int32, (8, C), 1)
    group = lax.broadcasted_iota(jnp.int32, (8, C), 0)
    segments = jnp.where(both(lane >= group * O, lane < group * O + O), 1.0, 0.0).astype(f32)

    def pack(value, offset=0):
        count = value.shape[0] // WW
        grouped = value.reshape(count, Z, W, value.shape[1])
        return jnp.concatenate(
            [grouped[:, m].reshape(count * W, value.shape[1])[:, offset : offset + O] for m in range(Z)], axis=1
        )

    def unpack(packed, m):
        return pad_to(packed[:, m * O : (m + 1) * O], 1, OP)

    def segment_sums(value):
        return lax.dot_general(segments, value, (((1,), (1,)), ((), ())), precision=EXACT, preferred_element_type=f32)

    def spread(tile):
        return lax.dot_general(tile, segments, (((0,), (0,)), ((), ())), precision=EXACT, preferred_element_type=f32)

    def rhs_forward(w, i, K):
        return jnp.concatenate(
            [jnp.concatenate([pad_to(w[i, j, l], 0, OP) for l in range(3)], axis=0) for j in range(3)], axis=1
        )

    def rhs_backward(w, i):
        return jnp.concatenate(
            [jnp.concatenate([pad_to(w[2 - i, 2 - j, 2 - l], 0, OP) for l in range(3)], axis=1) for j in range(3)],
            axis=0,
        )

    def forward(lhs_of, w, t):
        total = None
        for i in range(3):
            f = t + i - 2
            if not 0 <= f < F:
                continue
            part = lax.dot_general(
                lhs_of(f), rhs_forward(w, i, None), (((1,), (1,)), ((), ())), preferred_element_type=f32
            )
            total = part if total is None else total + part
        return shift_sum(total, WW, OP)[:, :O]

    def backward(qbuf, w, f, taps):
        total = None
        for i in taps:
            lhs = jnp.concatenate(
                [pad_to(qbuf[f + i, pl.ds(j, R)].reshape(R * WW, qbuf.shape[3]), 1, OP) for j in range(3)], axis=1
            )
            part = jnp.dot(lhs, rhs_backward(w, i), preferred_element_type=f32)
            total = part if total is None else total + part
        return total

    loads[0].wait()
    for m in range(Z):
        qs[m] = cotangent[:, :, :, m * O : (m + 1) * O]
    for load in loads[1:4]:
        load.wait()
    source = latent[...].reshape(rows, C).astype(f32)
    g_one, g_two = gain_one[...].reshape(1, C), gain_two[...].reshape(1, C)
    normed_one, _ = normalize(source, g_one)
    act[...] = silu(normed_one).astype(bf16).reshape(F, R, W, C)

    near = has_next.astype(jnp.int32) + has_prev.astype(jnp.int32)
    sides = has_high.astype(jnp.int32) + has_low.astype(jnp.int32)
    pl.semaphore_wait(barrier, Z - 1 + Z * near + sides + near * sides)

    for d in sorted(range(1, Z), key=lambda d: -abs(2 * d - Z)):
        q_own[d].start()
    gather_start(x_all)
    qp[own, body, block(z)] = qs[z]
    xp[:, body, block(z)] = act[...]
    q_next[0].start()

    def zero(ref, index):
        ref[index] = jnp.zeros_like(ref[index])

    full = slice(None)

    @pl.when(jnp.logical_not(has_next))
    def _():
        zero(qp, (halo,))
        zero(qq, (halo,))

    for missing, row in ((jnp.logical_not(has_low), 0), (jnp.logical_not(has_high), R + 1)):

        @pl.when(missing)
        def _():
            zero(qp, (full, row))
            zero(qq, (full, row))
            zero(xp, (full, row))
            zero(xq, (full, full, row))

    @pl.when(jnp.logical_not(has_prev))
    def _():
        zero(fr, (full,))
        zero(yr, (full,))

    for m in range(Z):
        gains[m] = jnp.broadcast_to(jnp.concatenate([g_two[:, m * O : (m + 1) * O]] * Z, axis=1), (8, C))

    load_two.wait()
    for i in range(3):
        for j in range(3):
            for l in range(3):
                w = w_two[i, j, l].astype(f32)
                w_gap[i, j, l] = jnp.concatenate(
                    [pad_to(w[:, m * O : (m + 1) * O], 1, OP) for m in range(Z)], axis=1
                ).astype(bf16)
    for d in range(1, Z):
        q_own[d].wait()
        q_next[d].start()
    for made in q_rows + q_corner:
        made.start()
    for made in q_rows:
        made.wait()
    early = [backward(qp, w_two, f, range(F - f)) for f in range(F)]
    gather_wait(x_all, 2)
    for d in range(Z):
        q_next[d].wait()
    for made in q_corner:
        made.wait()
    for f in range(F):
        total = early[f] + backward(qp, w_two, f, range(F - f, 3))
        total = shift_sum(total, WW, C)
        for m in range(Z):
            gs[m, f] = pack(total, m * O).astype(bf16).reshape(R, W, C)
        g_out.start(f)

    gather_wait(x_all, 1)
    for d in range(3, Z):
        gather_wait(x_all, d)
    for made in x_rows:
        made.start()
    load_one.wait()
    for made in x_rows:
        made.wait()

    def lhs_one(f):
        return jnp.concatenate([xp[f, pl.ds(j, R)].reshape(R * WW, C) for j in range(3)], axis=1)

    for t in (F + 1, F):
        fs[t - F] = pack(forward(lhs_one, w_one, t)).astype(bf16).reshape(R, W, C)
        f_out[t - F].start()
    inner = [pack(forward(lhs_one, w_one, t)) for t in range(F)]
    for f in range(F):
        g_out.join(f)
    for made in f_out:
        made.wait()
    for t in range(2):
        inner[t] = inner[t] + fr[t].reshape(R * W, C).astype(f32)
    inner = jnp.concatenate(inner, axis=0)
    vall[z] = inner.astype(bf16).reshape(F, R, W, C)
    st[0, 0] = segment_sums(inner * inner)
    for d in range(1, Z):
        sums[0][d].start()

    grad_two = g_out.total(gs[z].astype(f32)).reshape(rows, C)
    gather_start(v_all)
    squares = st[0, 0]
    for d in range(1, Z):
        sums[0][d].wait()
        squares = squares + st[0, d]
    inverse = lax.rsqrt(squares / C + epsilon)
    inverse_wide = spread(inverse)
    gain = gains[z][0:1]
    scaled = grad_two * silu_slope(inner * inverse_wide * gain) * gain
    st[1, 0] = segment_sums(inner * scaled)
    for d in range(1, Z):
        sums[1][d].start()

    def activate(owner):
        value = vall[owner].reshape(rows, C).astype(f32)
        active = silu(value * spread(inverse) * gains[owner][0:1])
        for m in range(Z):
            xq[owner, :, body, m * W : (m + 1) * W] = unpack(active, m).astype(bf16).reshape(F, R, W, OP)

    activate(z)
    gather_wait(v_all, 2, activate)
    gather_wait(v_all, 1, activate)

    means = st[1, 0]
    for d in range(1, Z):
        sums[1][d].wait()
        means = means + st[1, d]
    factor = spread(inverse * inverse * inverse * means / C)
    grad_inner = (inverse_wide * scaled - inner * factor).astype(bf16)
    gi[...] = grad_inner.reshape(F, R, W, C)
    gi_next.start()
    for made in gi_rows + gi_corner:
        made.start()

    def place(ref, frames, band, count):
        value = ref.reshape(count, C).astype(f32)
        for m in range(Z):
            piece = unpack(value, m).astype(bf16)
            qq[frames, band, m * W : (m + 1) * W] = piece.reshape(
                qq.at[frames, band, m * W : (m + 1) * W].shape
            )

    place(gi[...], own, body, rows)
    for d in range(3, Z):
        gather_wait(v_all, d, activate)
    for made in xq_rows:
        made.start()

    def place_rows(frames, count, among):
        for side, ref, row in ((has_low, gd, 0), (has_high, gu, R + 1)):

            @pl.when(side if among is None else both(side, among))
            def _():
                place(ref[frames], frames, row, count * W)

    for made in gi_rows:
        made.wait()
    place_rows(own, F, None)

    early = [backward(qq, w_one, f, range(F - f)) for f in range(F)]

    def lhs_two(f):
        return jnp.concatenate(
            [xq[m, f, pl.ds(j, R)].reshape(R * WW, OP) for j in range(3) for m in range(Z)], axis=1
        )

    for made in xq_rows:
        made.wait()
    for t in (F + 1, F):
        ys[t - F] = pack(forward(lhs_two, w_gap, t)).astype(bf16).reshape(R, W, C)
        y_next[t - F].start()
    for made in gi_corner + [gi_next]:
        made.wait()

    @pl.when(has_next)
    def _():
        place(gh[...], halo, body, 2 * R * W)

    place_rows(halo, 2, has_next)
    for f in range(F):
        total = early[f] + backward(qq, w_one, f, range(F - f, 3))
        yb[f] = shift_sum(total, WW, C).astype(bf16).reshape(R, WW, C)
        b_out.start(f)
    branch = [forward(lhs_two, w_gap, t).reshape(R, Z, W, O) for t in range(F)]
    for made in y_next:
        made.wait()
    for t in range(F):
        for m in range(Z):
            term = branch[t][:, m].reshape(R // fold, fold, W, O)
            if t < 2:
                carried = yr[t].reshape(R * W, C).astype(f32)[:, m * O : (m + 1) * O]
                term = term + carried.reshape(R // fold, fold, W, O)
            yf[m, t] = jnp.concatenate(
                [term[:, k].reshape(R // fold * W, O) for k in range(fold)], axis=1
            ).astype(bf16).reshape(R // fold, W, fold * O)
    for d in sorted(range(1, Z), key=lambda d: -abs(2 * d - Z)):
        y_own[d].start()
    rf[z] = yf[z]
    for f in range(F):
        b_out.join(f)

    for d in range(1, Z):
        y_own[d].wait()
    chunks = []
    for m in range(Z):
        value = rf[m].reshape(F * R // fold, W, fold * O).astype(f32)
        parts = [value[:, :, k * O : (k + 1) * O] for k in range(fold)]
        chunks.append(jnp.stack(parts, axis=1).reshape(rows, O))
    branch = jnp.concatenate(chunks, axis=1)
    source = latent[...].reshape(rows, C).astype(f32)
    out[...] = (source + branch).astype(bf16).reshape(F, R, W, C)
    stores[0].start()

    grad_one = b_out.total(yb[:, :, block(z)].astype(f32)).reshape(rows, C)
    normed_one, inverse_one = normalize(source, g_one)
    grad = norm_backward(source, inverse_one, g_one, grad_one * silu_slope(normed_one))
    upstream = cotangent[...].reshape(rows, C).astype(f32)
    latent_grad[...] = (upstream + grad).astype(bf16).reshape(F, R, W, C)
    stores[1].start()
    links.drain()
    for store in stores:
        store.wait()


def hand_over(first, second, first_out, second_out, sem):
    copies = [
        pltpu.make_async_copy(first, first_out, sem.at[0]),
        pltpu.make_async_copy(second, second_out, sem.at[1]),
    ]
    for made in copies:
        made.start()
    for made in copies:
        made.wait()


def local(sizes, latent, cotangent, gain_one, gain_two, kernel_one, kernel_two):
    S, Q, Z = sizes
    F, R, W, C = latent.shape
    O = kernel_one.shape[3]
    WW = W * Z
    OP = -(-O // 128) * 128
    rows = F * R * W
    taps = kernel_one.shape[:3]
    fold = fold_of(R, O)
    packed = (F, R, W, C)
    slots = 128
    shapes = [
        kernel_one.shape,
        kernel_two.shape,
        taps + (O, Z * OP),
        packed,
        (F, R + 2, WW, C),
        (Z, F, R, W, O),
        (F + 2, R + 2, WW, O),
        (Z,) + packed,
        (4,) + packed,
        (2, R, W, C),
        (2, R, W, C),
        (Z,) + packed,
        None,
        None,
        (Z, F, R + 2, WW, OP),
        packed,
        (2, R, W, C),
        (F + 2, W, C),
        (F + 2, W, C),
        (F + 2, R + 2, WW, OP),
        (Z, F, R // fold, W, fold * O),
        (Z, F, R // fold, W, fold * O),
        (2, R, W, C),
        (2, R, W, C),
        (F, R, WW, C),
        (4,) + packed,
        (2, max(Z - 3, 1)) + packed,
        (2, max(Z - 3, 1)) + packed,
        packed,
        packed,
        None,
        None,
        packed,
        packed,
    ]
    scratch = [pltpu.VMEM(shape, bf16) if shape else None for shape in shapes]
    scratch[12] = pltpu.VMEM((2, Z, 8, rows), f32)
    scratch[13] = pltpu.VMEM((Z, 8, C), f32)
    scratch[30] = scratch[31] = pltpu.VMEM((C,), f32)
    hbm = pl.BlockSpec(memory_space=pltpu.HBM)
    results = pl.pallas_call(
        functools.partial(kernel, sizes),
        out_shape=[jax.ShapeDtypeStruct((F, R, W, C), bf16)] * 2,
        in_specs=[hbm] * 6,
        out_specs=[hbm] * 2,
        scratch_shapes=[
            *scratch,
            pltpu.SemaphoreType.DMA((slots,)),
            pltpu.SemaphoreType.DMA((slots,)),
            pltpu.SemaphoreType.DMA((8,)),
        ],
        compiler_params=pltpu.CompilerParams(
            collective_id=0, has_side_effects=True, vmem_limit_bytes=60 * 1024 * 1024
        ),
    )(latent, cotangent, gain_one, gain_two, kernel_one, kernel_two)
    vmem = pl.BlockSpec(memory_space=pltpu.VMEM)

    def pass_on(first, second, first_out, second_out):
        first_out[...] = first[...]
        second_out[...] = second[...]

    return pl.pallas_call(
        pass_on,
        out_shape=[jax.ShapeDtypeStruct((F, R, W, C), bf16)] * 2,
        in_specs=[vmem] * 2,
        out_specs=[vmem] * 2,
    )(*results)

def solution(mesh):
    sizes = (mesh.shape["section"], mesh.shape["seq"], mesh.shape["exp"])
    spread = P("section", "seq", "exp", None)
    split = P(None, None, None, "exp", None)
    return jax.shard_map(
        functools.partial(local, sizes),
        mesh=mesh,
        in_specs=(spread, spread, P(), P(), split, split),
        out_specs=(spread, spread),
        check_vma=False,
    )
```

```python
import functools

import jax
import jax.numpy as jnp
from jax import lax
from jax.experimental import pallas as pl
from jax.experimental.pallas import tpu as pltpu
from jax.sharding import PartitionSpec as P

epsilon = 1e-06
MESH = pl.DeviceIdType.MESH
bf16, f32 = jnp.bfloat16, jnp.float32
EXACT = lax.Precision.HIGHEST


def normalize(values, gain):
    inverse = lax.rsqrt(jnp.mean(values * values, axis=-1, keepdims=True) + epsilon)
    return values * inverse * gain, inverse


def norm_backward(values, inverse, gain, upstream):
    scaled = upstream * gain
    mean = jnp.mean(values * scaled, axis=-1, keepdims=True)
    return inverse * scaled - values * (inverse * inverse * inverse) * mean


def silu(normed):
    return normed / (1.0 + jnp.exp(-normed))


def silu_slope(normed):
    sigma = 1.0 / (1.0 + jnp.exp(-normed))
    return sigma * (1.0 + normed * (1.0 - sigma))


def shift_sum(taps, width, size):
    rows = taps.shape[0]
    column = lax.rem(lax.broadcasted_iota(jnp.int32, (rows, size), 0), width)
    low = pltpu.roll(taps[:, :size], 1, axis=0)
    high = pltpu.roll(taps[:, 2 * size :], rows - 1, axis=0)
    return (
        taps[:, size : 2 * size]
        + jnp.where(column == 0, 0.0, low)
        + jnp.where(column == width - 1, 0.0, high)
    )


def fold_of(rows, width):
    return next((n for n in (4, 2) if rows % n == 0 and n * width % 128 == 0), 1)


def pad_to(value, axis, size):
    shape = list(value.shape)
    if shape[axis] == size:
        return value
    shape[axis] = size - shape[axis]
    return jnp.concatenate([value, jnp.zeros(shape, value.dtype)], axis=axis)


class Links:
    def __init__(self, send, recv):
        self.send, self.recv, self.all = send, recv, []

    def copy(self, src, dst, device, sends=True, receives=True):
        made = Copy(self, len(self.all), src, dst, device, sends, receives)
        self.all.append(made)
        return made

    def drain(self):
        for made in self.all:
            made.drain()
        assert len(self.all) == self.send.shape[0], len(self.all)


class Copy:
    def __init__(self, links, slot, src, dst, device, sends, receives):
        self.made = lambda: pltpu.make_async_remote_copy(
            src_ref=src,
            dst_ref=dst,
            send_sem=links.send.at[slot],
            recv_sem=links.recv.at[slot],
            device_id=device,
            device_id_type=MESH,
        )
        self.sends, self.receives = sends, receives

    def start(self):
        when(self.sends, lambda: self.made().start())

    def wait(self):
        when(self.receives, lambda: self.made().wait_recv())

    def drain(self):
        when(self.sends, lambda: self.made().wait_send())


def when(condition, action):
    if condition is True:
        action()
    else:
        pl.when(condition)(action)


def kernel(sizes, latent_hbm, cotangent_hbm, gain_one_hbm, gain_two_hbm, kernel_one, kernel_two, out_hbm, latent_grad_hbm, *scratch):
    S, Q, Z = sizes
    (
        w_one, w_two, w_gap, act, xp, qs, qr, qn, qp, gs, gr, fs, fr, vall, st, gains,
        xq, gi, gh, gu, gd, qq, yf, rf, ys, yr, yb, rb, g_hop, b_hop, vh, gt, sq, sh, early,
        latent, cotangent, gain_one, gain_two, out, latent_grad, send, recv, w_sem, seen,
    ) = scratch
    F, R, W, C = latent_hbm.shape
    O = kernel_one.shape[3]
    WW = W * Z
    OP = -(-O // 128) * 128
    rows = F * R * W
    s, q, z = lax.axis_index("section"), lax.axis_index("seq"), lax.axis_index("exp")
    has_next, has_prev = s < S - 1, s > 0
    has_high, has_low = q < Q - 1, q > 0
    both = jnp.logical_and
    nxt, prv = jnp.minimum(s + 1, S - 1), jnp.maximum(s - 1, 0)
    upper, lower = jnp.minimum(q + 1, Q - 1), jnp.maximum(q - 1, 0)
    fold = fold_of(R, O)
    body, own, halo = pl.ds(1, R), pl.ds(0, F), pl.ds(F, 2)
    two = pl.ds(0, 2)
    links = Links(send, recv)

    barrier = pltpu.get_barrier_semaphore()
    loads = [
        pltpu.make_async_copy(src, dst, w_sem.at[k])
        for k, (src, dst) in enumerate(
            [
                (cotangent_hbm, cotangent),
                (latent_hbm, latent),
                (gain_one_hbm, gain_one),
                (gain_two_hbm, gain_two),
                (kernel_two, w_two),
                (kernel_one, w_one),
            ]
        )
    ]
    load_two, load_one = loads[4:]
    stores = [
        pltpu.make_async_copy(out, out_hbm, w_sem.at[6]),
        pltpu.make_async_copy(latent_grad, latent_grad_hbm, w_sem.at[7]),
    ]
    for load in loads[:4]:
        load.start()

    def greet(device):
        pl.semaphore_signal(barrier, inc=1, device_id=device, device_id_type=MESH)

    has_right, has_left = z < Z - 1, z > 0
    for beside, step in ((has_right, 1), (has_left, -1)):

        @pl.when(beside)
        def _():
            greet((s, q, z + step))

    for near, step in ((has_next, 1), (has_prev, -1)):

        @pl.when(near)
        def _():
            greet((s + step, q, z))

        for side, move in ((has_high, 1), (has_low, -1)):

            @pl.when(both(near, side))
            def _():
                greet((s + step, q + move, z))

    for side, move in ((has_high, 1), (has_low, -1)):

        @pl.when(side)
        def _():
            greet((s, q + move, z))

    for load in loads[4:]:
        load.start()

    def peer(d):
        return lax.rem(z + d + Z, Z)

    def block(index):
        return pl.ds(pl.multiple_of(index * W, W), W)

    def gather(source, at, reach):
        arrive = []
        for d in range(1, Z):
            for sign in (1, -1):
                if d <= reach:
                    target, sends = z + sign * d, (z + d < Z) if sign > 0 else (z >= d)
                    src, dst = source, at(z)
                else:
                    target = z + sign
                    held = z - sign * (d - 1)
                    sends = both(z < Z - 1, z >= d - 1) if sign > 0 else both(z > 0, z <= Z - d)
                    src = dst = at(jnp.clip(held, 0, Z - 1))
                receives = (z >= d) if sign > 0 else (z + d < Z)
                target = jnp.clip(target, 0, Z - 1)
                arrive.append((d, z - sign * d, links.copy(src, dst, (s, q, target), sends, receives)))
        return arrive

    def gather_start(arrive, distances):
        for d in distances:
            for distance, _, made in arrive:
                if distance == d:
                    made.start()

    def gather_wait(arrive, d, reach, use=None):
        for distance, owner, made in arrive:
            if distance == d:
                made.wait()
        for distance, owner, made in arrive:
            if distance == d + 1 and d >= reach:
                made.start()
        if use is not None:
            for distance, owner, made in arrive:
                if distance == d:
                    when(made.receives, functools.partial(use, owner))

    class Scatter:
        def __init__(self, at, landing, hop):
            self.at, self.landing, self.hop, self.far, self.near = at, landing, hop, {}, {}
            for sign in (1, -1):
                for D in range(Z - 1, 0, -1):
                    for f in range(F):
                        target, origin = z + sign * D, z - sign * D
                        sends = (z + D < Z) if sign > 0 else (z >= D)
                        src = at(jnp.clip(target, 0, Z - 1), f)
                        if D >= 3:
                            before = (z >= 1) if sign > 0 else (z < Z - 1)
                            further = (z + D <= Z) if sign > 0 else (z >= D - 1)
                            self.far[sign, D, f] = links.copy(
                                src, hop.at[int(sign > 0), D - 3, f], (s, q, jnp.clip(z + sign, 0, Z - 1)), sends, both(before, further)
                            )
                        else:
                            receives = (z >= D) if sign > 0 else (z + D < Z)
                            slot = 2 * (sign > 0) + D - 1
                            self.near[sign, D, f] = links.copy(
                                src, landing.at[slot, f], (s, q, jnp.clip(target, 0, Z - 1)), sends, receives
                            )

        def start(self, f, distances):
            for D in distances:
                for sign in (1, -1):
                    made = self.far.get((sign, D, f)) or self.near[sign, D, f]
                    joined = self.far.get((sign, D + 1, f))
                    if joined is None:
                        made.start()
                    else:
                        when(both(made.sends, jnp.logical_not(joined.receives)), lambda: made.made().start())

        def join(self, f):
            for D in range(Z - 1, 2, -1):
                for sign in (1, -1):
                    arrived = self.far[sign, D, f]
                    onward = self.far.get((sign, D - 1, f)) or self.near[sign, D - 1, f]

                    @pl.when(arrived.receives)
                    def _():
                        arrived.made().wait_recv()
                        held = self.at(jnp.clip(z + sign * (D - 1), 0, Z - 1), f)
                        total = held[...].astype(f32) + self.hop[int(sign > 0), D - 3, f].astype(f32)
                        held[...] = total.astype(bf16)
                        onward.made().start()

        def total(self, own):
            for D in (1, 2):
                for sign in (1, -1):
                    for f in range(F):
                        if (sign, D, f) in self.near:
                            self.near[sign, D, f].wait()
            for D in (1, 2):
                for sign in (1, -1):
                    if (sign, D, 0) in self.near:
                        made = self.near[sign, D, 0]
                        term = self.landing[2 * (sign > 0) + D - 1].astype(f32)
                        own = own + jnp.where(made.receives, term, 0.0)
            return own

    q_own = {}
    for d in range(1, Z):
        for sign in (1, -1):
            target = jnp.clip(z + sign * d, 0, Z - 1)
            ends = (z + d < Z, z >= d)
            q_own[sign, d] = links.copy(qs.at[target], qr.at[z], (s, q, target), *ends[::sign])
    q_next = {
        d: links.copy((qr if d else qs).at[peer(-d), two], qn.at[peer(-d)], (prv, q, z), has_prev, has_next)
        for d in range(Z)
    }

    def q_pass_on(sign, d):
        made = q_own[sign, d]
        made.wait()

        @pl.when(made.receives)
        def _():
            q_next[(sign * d) % Z].start()

    def rows_out(src, dst, device, towards):
        sides = (has_high, has_low) if towards > 0 else (has_low, has_high)
        return links.copy(src, dst, device, *sides)

    q_rows = [
        rows_out(qp.at[own, R], qp.at[own, 0], (s, upper, z), 1),
        rows_out(qp.at[own, 1], qp.at[own, R + 1], (s, lower, z), -1),
    ]
    q_corner = [
        links.copy(qp.at[two, R], qp.at[halo, 0], (prv, upper, z), both(has_prev, has_high), both(has_next, has_low)),
        links.copy(qp.at[two, 1], qp.at[halo, R + 1], (prv, lower, z), both(has_prev, has_low), both(has_next, has_high)),
    ]
    x_rows = [
        rows_out(xp.at[:, R], xp.at[:, 0], (s, upper, z), 1),
        rows_out(xp.at[:, 1], xp.at[:, R + 1], (s, lower, z), -1),
    ]
    x_all = gather(act, lambda owner: xp.at[:, body, block(owner)], Z)
    g_out = Scatter(lambda owner, f: gs.at[owner, f], gr, g_hop)
    f_out = [links.copy(fs.at[t], fr.at[t], (nxt, q, z), has_next, has_prev) for t in range(2)]
    v_all = gather(vall.at[z], lambda owner: vall.at[owner], 2)
    sums = [{d: links.copy(st.at[k, 0], st.at[k, d], (s, q, peer(d))) for d in range(1, Z)} for k in range(2)]
    xq_rows = [
        rows_out(xq.at[:, :, R], xq.at[:, :, 0], (s, upper, z), 1),
        rows_out(xq.at[:, :, 1], xq.at[:, :, R + 1], (s, lower, z), -1),
    ]
    v_next = links.copy(vall.at[z, two], vh, (prv, q, z), has_prev, has_next)
    g_next = links.copy(gt, gh, (prv, q, z), has_prev, has_next)
    squares_next = links.copy(sq, sh.at[Z], (prv, q, z), has_prev, has_next)
    sums_next = {d: links.copy(st.at[1, 0], sh.at[d], (prv, q, peer(d)), has_prev, has_next) for d in range(Z)}

    def gi_out(frames):
        return [
            rows_out(gi.at[frames, R - 1], gd.at[frames], (s, upper, z), 1),
            rows_out(gi.at[frames, 0], gu.at[frames], (s, lower, z), -1),
        ]

    gi_rows, gi_corner = gi_out(own), gi_out(halo)
    b_out = Scatter(lambda owner, f: yb.at[f, :, block(owner)], rb, b_hop)
    y_own = {d: links.copy(yf.at[peer(d)], rf.at[z], (s, q, peer(d))) for d in range(1, Z)}
    y_next = [links.copy(ys.at[t], yr.at[t], (nxt, q, z), has_next, has_prev) for t in range(2)]

    lane = lax.broadcasted_iota(jnp.int32, (8, C), 1)
    group = lax.broadcasted_iota(jnp.int32, (8, C), 0)
    segments = jnp.where(both(lane >= group * O, lane < group * O + O), 1.0, 0.0).astype(f32)

    def pack(value, offset=0):
        count = value.shape[0] // WW
        grouped = value.reshape(count, Z, W, value.shape[1])
        return jnp.concatenate(
            [grouped[:, m].reshape(count * W, value.shape[1])[:, offset : offset + O] for m in range(Z)], axis=1
        )

    def unpack(packed, m):
        return pad_to(packed[:, m * O : (m + 1) * O], 1, OP)

    def segment_sums(value):
        return lax.dot_general(segments, value, (((1,), (1,)), ((), ())), precision=EXACT, preferred_element_type=f32)

    def spread(tile):
        return lax.dot_general(tile, segments, (((0,), (0,)), ((), ())), precision=EXACT, preferred_element_type=f32)

    def rhs_forward(w, taps):
        return jnp.concatenate(
            [
                jnp.concatenate([pad_to(w[i, j, l], 0, OP) for l in range(3) for i in taps], axis=0)
                for j in range(3)
            ],
            axis=1,
        )

    def rhs_backward(w, i):
        return jnp.concatenate(
            [jnp.concatenate([pad_to(w[2 - i, 2 - j, 2 - l], 0, OP) for l in range(3)], axis=1) for j in range(3)],
            axis=0,
        )

    def forward(lhs_of, w):
        parts = {}

        def run(f, taps):
            product = lax.dot_general(
                lhs_of(f), rhs_forward(w, taps), (((1,), (1,)), ((), ())), preferred_element_type=f32
            )
            joined = shift_sum(product, WW, len(taps) * OP)
            for n, i in enumerate(taps):
                parts.setdefault(f + 2 - i, []).append(joined[:, n * OP : n * OP + O])

        def finish(t):
            return functools.reduce(lambda a, b: a + b, parts[t])

        def ahead(t):
            if not parts:
                for f in range(F - 1, max(F - 3, -1), -1):
                    run(f, (0, 1))
            return finish(t)

        def rest(t):
            for f in range(F):
                if f + 2 - 2 == t:
                    run(f, (2,) if f >= F - 2 else (0, 1, 2))
            return finish(t)

        return ahead, rest

    def backward(qbuf, w, f, taps):
        lhs = jnp.concatenate(
            [
                pad_to(qbuf[f + i, pl.ds(j, R)].reshape(R * WW, qbuf.shape[3]), 1, OP)
                for i in taps
                for j in range(3)
            ],
            axis=1,
        )
        rhs = jnp.concatenate([rhs_backward(w, i) for i in taps], axis=0)
        return jnp.dot(lhs, rhs, preferred_element_type=f32)

    def fold_rows(pieces):
        return jnp.concatenate([p.reshape(p.shape[0] * W, O) for p in pieces], axis=1).astype(bf16)

    def unfold_rows(value, width):
        value = value.reshape(value.shape[0] * value.shape[1], W, fold * O).astype(f32)
        parts = [pad_to(value[:, :, k * O : (k + 1) * O], 2, width) for k in range(fold)]
        return jnp.stack(parts, axis=1).reshape(-1, R, W, width)

    loads[0].wait()
    folded = cotangent[...].astype(f32).reshape(F * R // fold, fold, W, C)
    for m in range(Z):
        qs[m] = fold_rows([folded[:, k, :, m * O : (m + 1) * O] for k in range(fold)]).reshape(qs.shape[1:])
    for load in loads[1:4]:
        load.wait()
    source = latent[...].reshape(rows, C).astype(f32)
    g_one, g_two = gain_one[...].reshape(1, C), gain_two[...].reshape(1, C)
    normed_one, _ = normalize(source, g_one)
    act[...] = silu(normed_one).astype(bf16).reshape(F, R, W, C)

    near = has_next.astype(jnp.int32) + has_prev.astype(jnp.int32)
    sides = has_high.astype(jnp.int32) + has_low.astype(jnp.int32)
    beside = has_right.astype(jnp.int32) + has_left.astype(jnp.int32)
    pl.semaphore_wait(barrier, beside + near + sides + near * sides)

    def announce(d):
        for k, known, teller in (
            (0, z + d - 1 < Z, has_left),
            (1, z >= d - 1, has_right),
        ):

            @pl.when(both(known, teller))
            def _():
                pl.semaphore_signal(
                    seen.at[k, d - 2],
                    inc=1,
                    device_id=(s, q, jnp.clip(z - 1 if k == 0 else z + 1, 0, Z - 1)),
                    device_id_type=MESH,
                )

    def await_seen(d):
        for k, known in ((0, z + d < Z), (1, z >= d)):

            @pl.when(known)
            def _():
                pl.semaphore_wait(seen.at[k, d - 2], 1)

    for d in range(1, Z):
        if d > 1:
            await_seen(d)
        if d < Z - 1:
            announce(d + 1)
        for sign in (1, -1):
            q_own[sign, d].start()
    qr[z] = qs[z]
    xp[:, body, block(z)] = act[...]
    q_next[0].start()

    def zero(ref, index):
        ref[index] = jnp.zeros_like(ref[index])

    full = slice(None)

    @pl.when(jnp.logical_not(has_next))
    def _():
        zero(qp, (halo,))
        zero(qq, (halo,))

    for missing, row in ((jnp.logical_not(has_low), 0), (jnp.logical_not(has_high), R + 1)):

        @pl.when(missing)
        def _():
            zero(qp, (full, row))
            zero(qq, (full, row))
            zero(xp, (full, row))
            zero(xq, (full, full, row))

    @pl.when(jnp.logical_not(has_prev))
    def _():
        zero(fr, (full,))
        zero(yr, (full,))

    for m in range(Z):
        gains[m] = jnp.broadcast_to(jnp.concatenate([g_two[:, m * O : (m + 1) * O]] * Z, axis=1), (8, C))

    load_two.wait()
    for i in range(3):
        for j in range(3):
            for l in range(3):
                w = w_two[i, j, l].astype(f32)
                w_gap[i, j, l] = jnp.concatenate(
                    [pad_to(w[:, m * O : (m + 1) * O], 1, OP) for m in range(Z)], axis=1
                ).astype(bf16)
    gather_start(x_all, range(Z - 1, 0, -1))
    for d in range(1, Z):
        for sign in (1, -1):
            q_pass_on(sign, d)
    for m in range(Z):
        qp[own, body, m * W : (m + 1) * W] = unfold_rows(qr[m], OP).astype(bf16)
    for made in q_rows + q_corner:
        made.start()
    for made in q_rows:
        made.wait()
    for f in range(F):
        early[f] = backward(qp, w_two, f, range(F - f))
    for d in range(Z):
        q_next[d].wait()

    @pl.when(has_next)
    def _():
        for m in range(Z):
            qp[halo, body, m * W : (m + 1) * W] = unfold_rows(qn[m], OP).astype(bf16)

    for made in q_corner:
        made.wait()
    for f in range(F):
        total = early[f] + backward(qp, w_two, f, range(F - f, 3))
        total = shift_sum(total, WW, C)
        for m in range(Z):
            gs[m, f] = pack(total, m * O).astype(bf16).reshape(R, W, C)
        g_out.start(f, range(Z - 1, 1, -1))
    for f in range(F):
        g_out.start(f, (1,))

    for d in range(1, Z):
        gather_wait(x_all, d, Z)
    for made in x_rows:
        made.start()
    load_one.wait()
    for made in x_rows:
        made.wait()

    def lhs_one(f):
        return jnp.concatenate([xp[f, pl.ds(j, R)].reshape(R * WW, C) for j in range(3)], axis=1)

    ahead, inner = forward(lhs_one, w_one)
    for t in (F + 1, F):
        fs[t - F] = pack(ahead(t)).astype(bf16).reshape(R, W, C)
        f_out[t - F].start()
    rest, inner = inner, []
    for t in range(F):
        g_out.join(t)
        inner.append(pack(rest(t)))
    for made in f_out:
        made.wait()
    for t in range(2):
        inner[t] = inner[t] + fr[t].reshape(R * W, C).astype(f32)
    inner = jnp.concatenate(inner, axis=0)
    vall[z] = inner.astype(bf16).reshape(F, R, W, C)
    st[0, 0] = segment_sums(inner * inner)
    for d in range(1, Z):
        sums[0][d].start()

    gather_start(v_all, (2,))
    v_next.start()
    grad_two = g_out.total(gs[z].astype(f32)).reshape(rows, C)
    gt[...] = grad_two[: 2 * R * W].astype(bf16).reshape(2, R, W, C)
    g_next.start()
    squares = st[0, 0]
    for d in range(1, Z):
        sums[0][d].wait()
        squares = squares + st[0, d]
    sq[...] = squares
    squares_next.start()
    inverse = lax.rsqrt(squares / C + epsilon)
    inverse_wide = spread(inverse)
    gain = gains[z][0:1]
    scaled = grad_two * silu_slope(inner * inverse_wide * gain) * gain
    st[1, 0] = segment_sums(inner * scaled)
    for d in range(1, Z):
        sums[1][d].start()
    for d in range(Z):
        sums_next[d].start()

    def activate(owner):
        value = vall[owner].reshape(rows, C).astype(f32)
        active = silu(value * spread(inverse) * gains[owner][0:1])
        for m in range(Z):
            xq[owner, :, body, m * W : (m + 1) * W] = unpack(active, m).astype(bf16).reshape(F, R, W, OP)

    gather_start(v_all, (1,))
    activate(z)
    gather_wait(v_all, 2, 2, activate)

    means = st[1, 0]
    for d in range(1, Z):
        sums[1][d].wait()
        means = means + st[1, d]
    factor = spread(inverse * inverse * inverse * means / C)
    grad_inner = (inverse_wide * scaled - inner * factor).astype(bf16)
    gi[own] = grad_inner.reshape(F, R, W, C)
    for made in gi_rows:
        made.start()

    def place(ref, frames, band, count):
        value = ref.reshape(count, C).astype(f32)
        for m in range(Z):
            piece = unpack(value, m).astype(bf16)
            qq[frames, band, m * W : (m + 1) * W] = piece.reshape(
                qq.at[frames, band, m * W : (m + 1) * W].shape
            )

    place(gi[own], own, body, rows)

    def place_rows(frames, count, among):
        for side, ref, row in ((has_low, gd, 0), (has_high, gu, R + 1)):

            @pl.when(side if among is None else both(side, among))
            def _():
                place(ref[frames], frames, row, count * W)

    for made in (v_next, g_next, squares_next):
        made.wait()
    for d in range(Z):
        sums_next[d].wait()

    @pl.when(has_next)
    def _():
        taken = slice(0, 2 * R * W)
        inverse = lax.rsqrt(sh[Z] / C + epsilon)
        mean = sh[0]
        for d in range(1, Z):
            mean = mean + sh[d]
        value = vh[...].reshape(2 * R * W, C).astype(f32)
        inverse_wide = spread(inverse)[taken]
        upstream = gh[...].reshape(2 * R * W, C).astype(f32)
        upstream = upstream * silu_slope(value * inverse_wide * gain) * gain
        factor = spread(inverse * inverse * inverse * mean / C)[taken]
        gi[halo] = (inverse_wide * upstream - value * factor).astype(bf16).reshape(2, R, W, C)
        place(gi[halo], halo, body, 2 * R * W)

    @pl.when(jnp.logical_not(has_next))
    def _():
        zero(gi, (halo,))

    for made in gi_corner:
        made.start()
    gather_wait(v_all, 1, 2, activate)
    for d in range(3, Z):
        gather_wait(v_all, d, 2, activate)
    for made in xq_rows:
        made.start()
    for made in gi_rows:
        made.wait()
    place_rows(own, F, None)
    for f in range(F):
        early[f] = backward(qq, w_one, f, range(F - f))
    for made in gi_corner:
        made.wait()
    place_rows(halo, 2, has_next)
    for f in range(F):
        total = early[f] + backward(qq, w_one, f, range(F - f, 3))
        yb[f] = shift_sum(total, WW, C).astype(bf16).reshape(R, WW, C)
        b_out.start(f, range(Z - 1, 1, -1))
    for f in range(F):
        b_out.start(f, (1,))

    def lhs_two(f):
        return jnp.concatenate(
            [xq[m, f, pl.ds(j, R)].reshape(R * WW, OP) for j in range(3) for m in range(Z)], axis=1
        )

    for made in xq_rows:
        made.wait()
    ahead, branch = forward(lhs_two, w_gap)
    for t in (F + 1, F):
        ys[t - F] = pack(ahead(t)).astype(bf16).reshape(R, W, C)
        y_next[t - F].start()
    rest, branch = branch, []
    for t in range(F):
        b_out.join(t)
        branch.append(rest(t).reshape(R, Z, W, O))
    for made in y_next:
        made.wait()
    for t in range(F):
        for m in range(Z):
            term = branch[t][:, m].reshape(R // fold, fold, W, O)
            if t < 2:
                carried = yr[t].reshape(R * W, C).astype(f32)[:, m * O : (m + 1) * O]
                term = term + carried.reshape(R // fold, fold, W, O)
            yf[m, t] = fold_rows([term[:, k] for k in range(fold)]).reshape(R // fold, W, fold * O)
    for d in sorted(range(1, Z), key=lambda d: -abs(2 * d - Z)):
        y_own[d].start()
    rf[z] = yf[z]

    for d in range(1, Z):
        y_own[d].wait()
    chunks = []
    for m in range(Z):
        chunks.append(unfold_rows(rf[m], O).reshape(rows, O))
    branch = jnp.concatenate(chunks, axis=1)
    source = latent[...].reshape(rows, C).astype(f32)
    out[...] = (source + branch).astype(bf16).reshape(F, R, W, C)
    stores[0].start()

    grad_one = b_out.total(yb[:, :, block(z)].astype(f32)).reshape(rows, C)
    normed_one, inverse_one = normalize(source, g_one)
    grad = norm_backward(source, inverse_one, g_one, grad_one * silu_slope(normed_one))
    upstream = cotangent[...].reshape(rows, C).astype(f32)
    latent_grad[...] = (upstream + grad).astype(bf16).reshape(F, R, W, C)
    stores[1].start()
    links.drain()
    for store in stores:
        store.wait()


def hand_over(first, second, first_out, second_out, sem):
    copies = [
        pltpu.make_async_copy(first, first_out, sem.at[0]),
        pltpu.make_async_copy(second, second_out, sem.at[1]),
    ]
    for made in copies:
        made.start()
    for made in copies:
        made.wait()


def local(sizes, latent, cotangent, gain_one, gain_two, kernel_one, kernel_two):
    S, Q, Z = sizes
    F, R, W, C = latent.shape
    O = kernel_one.shape[3]
    WW = W * Z
    OP = -(-O // 128) * 128
    rows = F * R * W
    taps = kernel_one.shape[:3]
    fold = fold_of(R, O)
    packed = (F, R, W, C)
    slots = (Z - 1) * (9 + 4 * F) + 2 * Z + 19
    shapes = [
        kernel_one.shape,
        kernel_two.shape,
        taps + (O, Z * OP),
        packed,
        (F, R + 2, WW, C),
        (Z, F, R // fold, W, fold * O),
        (Z, F, R // fold, W, fold * O),
        (Z, 2, R // fold, W, fold * O),
        (F + 2, R + 2, WW, OP),
        (Z,) + packed,
        (4,) + packed,
        (2, R, W, C),
        (2, R, W, C),
        (Z,) + packed,
        None,
        None,
        (Z, F, R + 2, WW, OP),
        (F + 2, R, W, C),
        (2, R, W, C),
        (F + 2, W, C),
        (F + 2, W, C),
        (F + 2, R + 2, WW, OP),
        (Z, F, R // fold, W, fold * O),
        (Z, F, R // fold, W, fold * O),
        (2, R, W, C),
        (2, R, W, C),
        (F, R, WW, C),
        (4,) + packed,
        (2, max(Z - 3, 1)) + packed,
        (2, max(Z - 3, 1)) + packed,
        (2, R, W, C),
        (2, R, W, C),
        None,
        None,
        None,
        packed,
        packed,
        None,
        None,
        packed,
        packed,
    ]
    scratch = [pltpu.VMEM(shape, bf16) if shape else None for shape in shapes]
    scratch[14] = pltpu.VMEM((2, Z, 8, rows), f32)
    scratch[15] = pltpu.VMEM((Z, 8, C), f32)
    scratch[32] = pltpu.VMEM((8, rows), f32)
    scratch[33] = pltpu.VMEM((Z + 1, 8, rows), f32)
    scratch[34] = pltpu.VMEM((F, R * WW, 3 * C), f32)
    scratch[37] = scratch[38] = pltpu.VMEM((C,), f32)
    hbm = pl.BlockSpec(memory_space=pltpu.HBM)
    results = pl.pallas_call(
        functools.partial(kernel, sizes),
        out_shape=[jax.ShapeDtypeStruct((F, R, W, C), bf16)] * 2,
        in_specs=[hbm] * 6,
        out_specs=[hbm] * 2,
        scratch_shapes=[
            *scratch,
            pltpu.SemaphoreType.DMA((slots,)),
            pltpu.SemaphoreType.DMA((slots,)),
            pltpu.SemaphoreType.DMA((8,)),
            pltpu.SemaphoreType.REGULAR((2, max(Z - 2, 1))),
        ],
        compiler_params=pltpu.CompilerParams(
            collective_id=0, has_side_effects=True, vmem_limit_bytes=60 * 1024 * 1024
        ),
    )(latent, cotangent, gain_one, gain_two, kernel_one, kernel_two)
    vmem = pl.BlockSpec(memory_space=pltpu.VMEM)

    def pass_on(first, second, first_out, second_out):
        first_out[...] = first[...]
        second_out[...] = second[...]

    return pl.pallas_call(
        pass_on,
        out_shape=[jax.ShapeDtypeStruct((F, R, W, C), bf16)] * 2,
        in_specs=[vmem] * 2,
        out_specs=[vmem] * 2,
    )(*results)

def solution(mesh):
    sizes = (mesh.shape["section"], mesh.shape["seq"], mesh.shape["exp"])
    spread = P("section", "seq", "exp", None)
    split = P(None, None, None, "exp", None)
    return jax.shard_map(
        functools.partial(local, sizes),
        mesh=mesh,
        in_specs=(spread, spread, P(), P(), split, split),
        out_specs=(spread, spread),
        check_vma=False,
    )
```

```python
import functools

import jax
import jax.numpy as jnp
from jax import lax
from jax.experimental import pallas as pl
from jax.experimental.pallas import tpu as pltpu
from jax.sharding import PartitionSpec as P

epsilon = 1e-06
MESH = pl.DeviceIdType.MESH
bf16, f32 = jnp.bfloat16, jnp.float32


def normalize(values, gain):
    inverse = lax.rsqrt(jnp.mean(values * values, axis=-1, keepdims=True) + epsilon)
    return values * inverse * gain, inverse


def norm_backward(values, inverse, gain, upstream):
    scaled = upstream * gain
    mean = jnp.mean(values * scaled, axis=-1, keepdims=True)
    return inverse * scaled - values * (inverse * inverse * inverse) * mean


def silu(normed):
    return normed / (1.0 + jnp.exp(-normed))


def silu_slope(normed):
    sigma = 1.0 / (1.0 + jnp.exp(-normed))
    return sigma * (1.0 + normed * (1.0 - sigma))


def shift_sum(taps, width, size):
    rows = taps.shape[0]
    column = lax.rem(lax.broadcasted_iota(jnp.int32, (rows, size), 0), width)
    low = pltpu.roll(taps[:, :size], 1, axis=0)
    high = pltpu.roll(taps[:, 2 * size :], rows - 1, axis=0)
    return (
        taps[:, size : 2 * size]
        + jnp.where(column == 0, 0.0, low)
        + jnp.where(column == width - 1, 0.0, high)
    )


def fold_of(rows, width):
    return next((n for n in (4, 2) if rows % n == 0 and n * width % 128 == 0), 1)


def pad_to(value, axis, size):
    shape = list(value.shape)
    if shape[axis] == size:
        return value
    shape[axis] = size - shape[axis]
    return jnp.concatenate([value, jnp.zeros(shape, value.dtype)], axis=axis)


class Links:
    def __init__(self, send, recv):
        self.send, self.recv, self.slots, self.open = send, recv, 0, []

    def copy(self, src, dst, device, sends=True, receives=True, after=None):
        slot = self.slots if after is None else after.slot
        self.slots += after is None
        made = Copy(self, slot, src, dst, device, sends, receives)
        self.open.append(made)
        return made

    def retire(self, copies):
        for made in copies:
            made.drain()
            self.open.remove(made)

    def drain(self):
        for made in self.open:
            made.drain()
        assert self.slots == self.send.shape[0], self.slots


class Copy:
    def __init__(self, links, slot, src, dst, device, sends, receives):
        self.made = lambda: pltpu.make_async_remote_copy(
            src_ref=src,
            dst_ref=dst,
            send_sem=links.send.at[slot],
            recv_sem=links.recv.at[slot],
            device_id=device,
            device_id_type=MESH,
        )
        self.slot, self.sends, self.receives = slot, sends, receives

    def start(self):
        when(self.sends, lambda: self.made().start())

    def wait(self):
        when(self.receives, lambda: self.made().wait_recv())

    def drain(self):
        when(self.sends, lambda: self.made().wait_send())


def when(condition, action):
    if condition is True:
        action()
    else:
        pl.when(condition)(action)


def kernel(sizes, latent_hbm, cotangent_hbm, gain_one_hbm, gain_two_hbm, kernel_one, kernel_two, out_hbm, latent_grad_hbm, *scratch):
    S, Q, Z = sizes
    (
        w_one, w_two, w_gap, act, xp, qs, qr, qn, qp, gs, gr, fs, fr, vall, st, gains,
        xq, gi, gh, gu, gd, qq, yf, rf, ys, yr, yb, rb, g_hop, b_hop, vh, gt, sq, sh, early,
        latent, cotangent, gain_one, gain_two, out, latent_grad, send, recv, w_sem, seen,
    ) = scratch
    F, R, W, C = latent_hbm.shape
    O = kernel_one.shape[3]
    WW = W * Z
    OP = -(-O // 128) * 128
    rows = F * R * W
    s, q, z = lax.axis_index("section"), lax.axis_index("seq"), lax.axis_index("exp")
    has_next, has_prev = s < S - 1, s > 0
    has_high, has_low = q < Q - 1, q > 0
    both = jnp.logical_and
    nxt, prv = jnp.minimum(s + 1, S - 1), jnp.maximum(s - 1, 0)
    upper, lower = jnp.minimum(q + 1, Q - 1), jnp.maximum(q - 1, 0)
    fold = fold_of(R, O)
    body, own, halo = pl.ds(1, R), pl.ds(0, F), pl.ds(F, 2)
    two = pl.ds(0, 2)
    links = Links(send, recv)

    barrier = pltpu.get_barrier_semaphore()
    loads = [
        pltpu.make_async_copy(src, dst, w_sem.at[k])
        for k, (src, dst) in enumerate(
            [
                (cotangent_hbm, cotangent),
                (latent_hbm, latent),
                (gain_one_hbm, gain_one),
                (gain_two_hbm, gain_two),
                (kernel_two, w_two),
                (kernel_one, w_one),
            ]
        )
    ]
    load_two, load_one = loads[4:]
    stores = [
        pltpu.make_async_copy(out, out_hbm, w_sem.at[6]),
        pltpu.make_async_copy(latent_grad, latent_grad_hbm, w_sem.at[7]),
    ]
    for load in loads[:4]:
        load.start()

    def greet(device):
        pl.semaphore_signal(barrier, inc=1, device_id=device, device_id_type=MESH)

    has_right, has_left = z < Z - 1, z > 0
    for beside, step in ((has_right, 1), (has_left, -1)):

        @pl.when(beside)
        def _():
            greet((s, q, z + step))

    for near, step in ((has_next, 1), (has_prev, -1)):

        @pl.when(near)
        def _():
            greet((s + step, q, z))

        for side, move in ((has_high, 1), (has_low, -1)):

            @pl.when(both(near, side))
            def _():
                greet((s + step, q + move, z))

    for side, move in ((has_high, 1), (has_low, -1)):

        @pl.when(side)
        def _():
            greet((s, q + move, z))

    for load in loads[4:]:
        load.start()

    def peer(d):
        return lax.rem(z + d + Z, Z)

    def block(index):
        return pl.ds(pl.multiple_of(index * W, W), W)

    def gather(source, at, reach, after=None):
        arrive = []
        for d in range(1, Z):
            for sign in (1, -1):
                if d <= reach:
                    target, sends = z + sign * d, (z + d < Z) if sign > 0 else (z >= d)
                    src, dst = source, at(z)
                else:
                    target = z + sign
                    held = z - sign * (d - 1)
                    sends = both(z < Z - 1, z >= d - 1) if sign > 0 else both(z > 0, z <= Z - d)
                    src = dst = at(jnp.clip(held, 0, Z - 1))
                receives = (z >= d) if sign > 0 else (z + d < Z)
                target = jnp.clip(target, 0, Z - 1)
                earlier = None if after is None else after[len(arrive)][2]
                arrive.append((d, z - sign * d, links.copy(src, dst, (s, q, target), sends, receives, earlier)))
        return arrive

    def gather_start(arrive, distances):
        for d in distances:
            for distance, _, made in arrive:
                if distance == d:
                    made.start()

    def gather_wait(arrive, d, reach, use=None):
        for distance, owner, made in arrive:
            if distance == d:
                made.wait()
        for distance, owner, made in arrive:
            if distance == d + 1 and d >= reach:
                made.start()
        if use is not None:
            for distance, owner, made in arrive:
                if distance == d:
                    when(made.receives, functools.partial(use, owner))

    class Scatter:
        def __init__(self, at, landing, hop, after=None):
            self.at, self.landing, self.hop, self.far, self.near = at, landing, hop, {}, {}
            for sign in (1, -1):
                for D in range(Z - 1, 0, -1):
                    for f in range(F):
                        target, origin = z + sign * D, z - sign * D
                        sends = (z + D < Z) if sign > 0 else (z >= D)
                        src = at(jnp.clip(target, 0, Z - 1), f)
                        if D >= 3:
                            before = (z >= 1) if sign > 0 else (z < Z - 1)
                            further = (z + D <= Z) if sign > 0 else (z >= D - 1)
                            self.far[sign, D, f] = links.copy(
                                src,
                                hop.at[int(sign > 0), D - 3, f],
                                (s, q, jnp.clip(z + sign, 0, Z - 1)),
                                sends,
                                both(before, further),
                                after and after.far[sign, D, f],
                            )
                        else:
                            receives = (z >= D) if sign > 0 else (z + D < Z)
                            slot = 2 * (sign > 0) + D - 1
                            self.near[sign, D, f] = links.copy(
                                src,
                                landing.at[slot, f],
                                (s, q, jnp.clip(target, 0, Z - 1)),
                                sends,
                                receives,
                                after and after.near[sign, D, f],
                            )

        def copies(self):
            return [*self.far.values(), *self.near.values()]

        def start(self, f, distances):
            for D in distances:
                for sign in (1, -1):
                    made = self.far.get((sign, D, f)) or self.near[sign, D, f]
                    joined = self.far.get((sign, D + 1, f))
                    if joined is None:
                        made.start()
                    else:
                        when(both(made.sends, jnp.logical_not(joined.receives)), lambda: made.made().start())

        def join(self, f):
            for D in range(Z - 1, 2, -1):
                for sign in (1, -1):
                    arrived = self.far[sign, D, f]
                    onward = self.far.get((sign, D - 1, f)) or self.near[sign, D - 1, f]

                    @pl.when(arrived.receives)
                    def _():
                        arrived.made().wait_recv()
                        held = self.at(jnp.clip(z + sign * (D - 1), 0, Z - 1), f)
                        total = held[...].astype(f32) + self.hop[int(sign > 0), D - 3, f].astype(f32)
                        held[...] = total.astype(bf16)
                        onward.made().start()

        def total(self, own):
            for D in (1, 2):
                for sign in (1, -1):
                    for f in range(F):
                        if (sign, D, f) in self.near:
                            self.near[sign, D, f].wait()
            for D in (1, 2):
                for sign in (1, -1):
                    if (sign, D, 0) in self.near:
                        made = self.near[sign, D, 0]
                        term = self.landing[2 * (sign > 0) + D - 1].astype(f32)
                        own = own + jnp.where(made.receives, term, 0.0)
            return own

    q_own = {}
    for d in range(1, Z):
        for sign in (1, -1):
            target = jnp.clip(z + sign * d, 0, Z - 1)
            ends = (z + d < Z, z >= d)
            q_own[sign, d] = links.copy(qs.at[target], qr.at[z], (s, q, target), *ends[::sign])
    q_next = {
        d: links.copy((qr if d else qs).at[peer(-d), two], qn.at[peer(-d)], (prv, q, z), has_prev, has_next)
        for d in range(Z)
    }

    def q_pass_on(sign, d):
        made = q_own[sign, d]
        made.wait()

        @pl.when(made.receives)
        def _():
            q_next[(sign * d) % Z].start()

    def rows_out(src, dst, device, towards, after=None):
        sides = (has_high, has_low) if towards > 0 else (has_low, has_high)
        return links.copy(src, dst, device, *sides, after)

    q_rows = [
        rows_out(qp.at[own, R], qp.at[own, 0], (s, upper, z), 1),
        rows_out(qp.at[own, 1], qp.at[own, R + 1], (s, lower, z), -1),
    ]
    q_corner = [
        links.copy(qp.at[two, R], qp.at[halo, 0], (prv, upper, z), both(has_prev, has_high), both(has_next, has_low)),
        links.copy(qp.at[two, 1], qp.at[halo, R + 1], (prv, lower, z), both(has_prev, has_low), both(has_next, has_high)),
    ]
    x_rows = [
        rows_out(xp.at[:, R], xp.at[:, 0], (s, upper, z), 1),
        rows_out(xp.at[:, 1], xp.at[:, R + 1], (s, lower, z), -1),
    ]
    x_all = gather(act, lambda owner: xp.at[:, body, block(owner)], 2)
    g_out = Scatter(lambda owner, f: gs.at[owner, f], gr, g_hop)
    f_out = [links.copy(fs.at[t], fr.at[t], (nxt, q, z), has_next, has_prev) for t in range(2)]
    v_all = gather(vall.at[z], lambda owner: vall.at[owner], 2, x_all)
    sums = [{d: links.copy(st.at[k, 0], st.at[k, d], (s, q, peer(d))) for d in range(1, Z)} for k in range(2)]
    xq_rows = [
        rows_out(xq.at[:, :, R], xq.at[:, :, 0], (s, upper, z), 1),
        rows_out(xq.at[:, :, 1], xq.at[:, :, R + 1], (s, lower, z), -1),
    ]
    v_next = links.copy(vall.at[z, two], vh, (prv, q, z), has_prev, has_next)
    g_next = links.copy(gt, gh, (prv, q, z), has_prev, has_next)
    squares_next = links.copy(sq, sh.at[Z], (prv, q, z), has_prev, has_next)
    sums_next = {d: links.copy(st.at[1, 0], sh.at[d], (prv, q, peer(d)), has_prev, has_next) for d in range(Z)}

    def gi_out(frames, after):
        return [
            rows_out(gi.at[frames, R - 1], gd.at[frames], (s, upper, z), 1, after[0]),
            rows_out(gi.at[frames, 0], gu.at[frames], (s, lower, z), -1, after[1]),
        ]

    gi_rows, gi_corner = gi_out(own, q_rows), gi_out(halo, (None, None))
    b_out = Scatter(lambda owner, f: yb.at[f, :, block(owner)], rb, b_hop, g_out)
    y_own = {
        d: links.copy(yf.at[peer(d)], rf.at[z], (s, q, peer(d)), True, True, q_own[1, d]) for d in range(1, Z)
    }
    y_next = [
        links.copy(ys.at[t], yr.at[t], (nxt, q, z), has_next, has_prev, f_out[t]) for t in range(2)
    ]

    lane = lax.broadcasted_iota(jnp.int32, (8, C), 1)
    group = lax.broadcasted_iota(jnp.int32, (8, C), 0)
    segments = jnp.where(both(lane >= group * O, lane < group * O + O), 1.0, 0.0).astype(f32)

    def pack(value, offset=0):
        count = value.shape[0] // WW
        grouped = value.reshape(count, Z, W, value.shape[1])
        return jnp.concatenate(
            [grouped[:, m].reshape(count * W, value.shape[1])[:, offset : offset + O] for m in range(Z)], axis=1
        )

    def unpack(packed, m):
        return pad_to(packed[:, m * O : (m + 1) * O], 1, OP)

    segments_three = jnp.concatenate([segments] * 3, axis=1).astype(bf16)
    segments_down = jnp.concatenate([segments] * 3, axis=0).astype(bf16)

    def thirds(value, axis):
        high = value.astype(bf16).astype(f32)
        middle = (value - high).astype(bf16).astype(f32)
        return jnp.concatenate([high, middle, value - high - middle], axis=axis).astype(bf16)

    def segment_sums(value):
        return lax.dot_general(
            segments_three, thirds(value, 1), (((1,), (1,)), ((), ())), preferred_element_type=f32
        )

    def spread(tile):
        return lax.dot_general(
            thirds(tile, 0), segments_down, (((0,), (0,)), ((), ())), preferred_element_type=f32
        )

    def rhs_forward(w, taps):
        return jnp.concatenate(
            [
                jnp.concatenate([pad_to(w[i, j, l], 0, OP) for l in range(3) for i in taps], axis=0)
                for j in range(3)
            ],
            axis=1,
        )

    def rhs_backward(w, i):
        return jnp.concatenate(
            [jnp.concatenate([pad_to(w[2 - i, 2 - j, 2 - l], 0, OP) for l in range(3)], axis=1) for j in range(3)],
            axis=0,
        )

    def forward(lhs_of, w):
        parts = {}

        def run(f, taps):
            product = lax.dot_general(
                lhs_of(f), rhs_forward(w, taps), (((1,), (1,)), ((), ())), preferred_element_type=f32
            )
            joined = shift_sum(product, WW, len(taps) * OP)
            for n, i in enumerate(taps):
                parts.setdefault(f + 2 - i, []).append(joined[:, n * OP : n * OP + O])

        def finish(t):
            return functools.reduce(lambda a, b: a + b, parts[t])

        def ahead(t):
            if not parts:
                for f in range(F - 1, max(F - 3, -1), -1):
                    run(f, (0, 1))
            return finish(t)

        def rest(t):
            for f in range(F):
                if f + 2 - 2 == t:
                    run(f, (2,) if f >= F - 2 else (0, 1, 2))
            return finish(t)

        return ahead, rest

    def backward(qbuf, w, f, taps):
        lhs = jnp.concatenate(
            [
                pad_to(qbuf[f + i, pl.ds(j, R)].reshape(R * WW, qbuf.shape[3]), 1, OP)
                for i in taps
                for j in range(3)
            ],
            axis=1,
        )
        rhs = jnp.concatenate([rhs_backward(w, i) for i in taps], axis=0)
        return jnp.dot(lhs, rhs, preferred_element_type=f32)

    def fold_rows(pieces):
        return jnp.concatenate([p.reshape(p.shape[0] * W, O) for p in pieces], axis=1).astype(bf16)

    def unfold_rows(value, width):
        value = value.reshape(value.shape[0] * value.shape[1], W, fold * O).astype(f32)
        parts = [pad_to(value[:, :, k * O : (k + 1) * O], 2, width) for k in range(fold)]
        return jnp.stack(parts, axis=1).reshape(-1, R, W, width)

    loads[0].wait()
    folded = cotangent[...].astype(f32).reshape(F * R // fold, fold, W, C)
    for m in range(Z):
        qs[m] = fold_rows([folded[:, k, :, m * O : (m + 1) * O] for k in range(fold)]).reshape(qs.shape[1:])
    for load in loads[1:4]:
        load.wait()
    source = latent[...].reshape(rows, C).astype(f32)
    g_one, g_two = gain_one[...].reshape(1, C), gain_two[...].reshape(1, C)
    normed_one, _ = normalize(source, g_one)
    act[...] = silu(normed_one).astype(bf16).reshape(F, R, W, C)

    near = has_next.astype(jnp.int32) + has_prev.astype(jnp.int32)
    sides = has_high.astype(jnp.int32) + has_low.astype(jnp.int32)
    beside = has_right.astype(jnp.int32) + has_left.astype(jnp.int32)
    pl.semaphore_wait(barrier, beside + near + sides + near * sides)

    def announce(d):
        for k, known, teller in (
            (0, z + d - 1 < Z, has_left),
            (1, z >= d - 1, has_right),
        ):

            @pl.when(both(known, teller))
            def _():
                pl.semaphore_signal(
                    seen.at[k, d - 2],
                    inc=1,
                    device_id=(s, q, jnp.clip(z - 1 if k == 0 else z + 1, 0, Z - 1)),
                    device_id_type=MESH,
                )

    def await_seen(d):
        for k, known in ((0, z + d < Z), (1, z >= d)):

            @pl.when(known)
            def _():
                pl.semaphore_wait(seen.at[k, d - 2], 1)

    for d in range(1, Z):
        if d > 1:
            await_seen(d)
        if d < Z - 1:
            announce(d + 1)
        for sign in (1, -1):
            q_own[sign, d].start()
    qr[z] = qs[z]
    xp[:, body, block(z)] = act[...]
    q_next[0].start()

    def zero(ref, index):
        ref[index] = jnp.zeros_like(ref[index])

    full = slice(None)

    @pl.when(jnp.logical_not(has_next))
    def _():
        zero(qp, (halo,))
        zero(qq, (halo,))

    for missing, row in ((jnp.logical_not(has_low), 0), (jnp.logical_not(has_high), R + 1)):

        @pl.when(missing)
        def _():
            zero(qp, (full, row))
            zero(qq, (full, row))
            zero(xp, (full, row))
            zero(xq, (full, full, row))

    @pl.when(jnp.logical_not(has_prev))
    def _():
        zero(fr, (full,))
        zero(yr, (full,))

    for m in range(Z):
        gains[m] = jnp.broadcast_to(jnp.concatenate([g_two[:, m * O : (m + 1) * O]] * Z, axis=1), (8, C))

    load_two.wait()
    for i in range(3):
        for j in range(3):
            for l in range(3):
                w = w_two[i, j, l].astype(f32)
                w_gap[i, j, l] = jnp.concatenate(
                    [pad_to(w[:, m * O : (m + 1) * O], 1, OP) for m in range(Z)], axis=1
                ).astype(bf16)
    gather_start(x_all, (2, 1))
    for d in range(1, Z):
        for sign in (1, -1):
            q_pass_on(sign, d)
    for m in range(Z):
        qp[own, body, m * W : (m + 1) * W] = unfold_rows(qr[m], OP).astype(bf16)
    for made in q_rows + q_corner:
        made.start()
    for made in q_rows:
        made.wait()
    for f in range(F):
        early[f] = backward(qp, w_two, f, range(F - f))
    for d in range(Z):
        q_next[d].wait()

    @pl.when(has_next)
    def _():
        for m in range(Z):
            qp[halo, body, m * W : (m + 1) * W] = unfold_rows(qn[m], OP).astype(bf16)

    for made in q_corner:
        made.wait()
    for f in range(F):
        total = early[f] + backward(qp, w_two, f, range(F - f, 3))
        total = shift_sum(total, WW, C)
        if f == 0:
            gather_wait(x_all, 2, 2)
        for m in range(Z):
            gs[m, f] = pack(total, m * O).astype(bf16).reshape(R, W, C)
        g_out.start(f, range(Z - 1, 1, -1))
    for f in range(F):
        g_out.start(f, (1,))

    gather_wait(x_all, 1, 2)
    for d in range(3, Z):
        gather_wait(x_all, d, 2)
    for made in x_rows:
        made.start()
    load_one.wait()
    for made in x_rows:
        made.wait()

    def lhs_one(f):
        return jnp.concatenate([xp[f, pl.ds(j, R)].reshape(R * WW, C) for j in range(3)], axis=1)

    ahead, inner = forward(lhs_one, w_one)
    for t in (F + 1, F):
        fs[t - F] = pack(ahead(t)).astype(bf16).reshape(R, W, C)
        f_out[t - F].start()
    rest, inner = inner, []
    for t in range(F):
        g_out.join(t)
        inner.append(pack(rest(t)))
    for made in f_out:
        made.wait()
    for t in range(2):
        inner[t] = inner[t] + fr[t].reshape(R * W, C).astype(f32)
    inner = jnp.concatenate(inner, axis=0)
    vall[z] = inner.astype(bf16).reshape(F, R, W, C)
    st[0, 0] = segment_sums(inner * inner)
    for d in range(1, Z):
        sums[0][d].start()

    v_next.start()
    grad_two = g_out.total(gs[z].astype(f32)).reshape(rows, C)
    gt[...] = grad_two[: 2 * R * W].astype(bf16).reshape(2, R, W, C)
    g_next.start()
    links.retire([made for _, _, made in x_all])
    gather_start(v_all, (2,))
    squares = st[0, 0]
    for d in range(1, Z):
        sums[0][d].wait()
        squares = squares + st[0, d]
    sq[...] = squares
    squares_next.start()
    inverse = lax.rsqrt(squares / C + epsilon)
    inverse_wide = spread(inverse)
    gain = gains[z][0:1]
    scaled = grad_two * silu_slope(inner * inverse_wide * gain) * gain
    st[1, 0] = segment_sums(inner * scaled)
    for d in range(1, Z):
        sums[1][d].start()
    for d in range(Z):
        sums_next[d].start()

    def activate(owner):
        value = vall[owner].reshape(rows, C).astype(f32)
        active = silu(value * inverse_wide * gains[owner][0:1])
        for m in range(Z):
            xq[owner, :, body, m * W : (m + 1) * W] = unpack(active, m).astype(bf16).reshape(F, R, W, OP)

    gather_start(v_all, (1,))
    activate(z)
    gather_wait(v_all, 2, 2, activate)

    links.retire([*(q_own[1, d] for d in range(1, Z)), *f_out, *q_rows, *g_out.copies()])
    means = st[1, 0]
    for d in range(1, Z):
        sums[1][d].wait()
        means = means + st[1, d]
    factor = spread(inverse * inverse * inverse * means / C)
    grad_inner = (inverse_wide * scaled - inner * factor).astype(bf16)
    gi[own] = grad_inner.reshape(F, R, W, C)
    for made in gi_rows:
        made.start()

    def place(ref, frames, band, count):
        value = ref.reshape(count, C).astype(f32)
        for m in range(Z):
            piece = unpack(value, m).astype(bf16)
            qq[frames, band, m * W : (m + 1) * W] = piece.reshape(
                qq.at[frames, band, m * W : (m + 1) * W].shape
            )

    place(gi[own], own, body, rows)

    def place_rows(frames, count, among):
        for side, ref, row in ((has_low, gd, 0), (has_high, gu, R + 1)):

            @pl.when(side if among is None else both(side, among))
            def _():
                place(ref[frames], frames, row, count * W)

    for made in (v_next, g_next, squares_next):
        made.wait()
    for d in range(Z):
        sums_next[d].wait()

    @pl.when(has_next)
    def _():
        taken = slice(0, 2 * R * W)
        inverse = lax.rsqrt(sh[Z] / C + epsilon)
        mean = sh[0]
        for d in range(1, Z):
            mean = mean + sh[d]
        value = vh[...].reshape(2 * R * W, C).astype(f32)
        inverse_wide = spread(inverse)[taken]
        upstream = gh[...].reshape(2 * R * W, C).astype(f32)
        upstream = upstream * silu_slope(value * inverse_wide * gain) * gain
        factor = spread(inverse * inverse * inverse * mean / C)[taken]
        gi[halo] = (inverse_wide * upstream - value * factor).astype(bf16).reshape(2, R, W, C)
        place(gi[halo], halo, body, 2 * R * W)

    @pl.when(jnp.logical_not(has_next))
    def _():
        zero(gi, (halo,))

    for made in gi_corner:
        made.start()
    gather_wait(v_all, 1, 2, activate)
    for d in range(3, Z):
        gather_wait(v_all, d, 2, activate)
    for made in xq_rows:
        made.start()
    for made in gi_rows:
        made.wait()
    place_rows(own, F, None)
    for f in range(F):
        early[f] = backward(qq, w_one, f, range(F - f))
    for made in gi_corner:
        made.wait()
    place_rows(halo, 2, has_next)
    for f in range(F):
        total = early[f] + backward(qq, w_one, f, range(F - f, 3))
        yb[f] = shift_sum(total, WW, C).astype(bf16).reshape(R, WW, C)
        b_out.start(f, range(Z - 1, 1, -1))
    for f in range(F):
        b_out.start(f, (1,))

    def lhs_two(f):
        return jnp.concatenate(
            [xq[m, f, pl.ds(j, R)].reshape(R * WW, OP) for j in range(3) for m in range(Z)], axis=1
        )

    for made in xq_rows:
        made.wait()
    ahead, branch = forward(lhs_two, w_gap)
    for t in (F + 1, F):
        ys[t - F] = pack(ahead(t)).astype(bf16).reshape(R, W, C)
        y_next[t - F].start()
    rest, branch = branch, []
    for t in range(F):
        b_out.join(t)
        branch.append(rest(t).reshape(R, Z, W, O))
    for made in y_next:
        made.wait()
    for t in range(F):
        for m in range(Z):
            term = branch[t][:, m].reshape(R // fold, fold, W, O)
            if t < 2:
                carried = yr[t].reshape(R * W, C).astype(f32)[:, m * O : (m + 1) * O]
                term = term + carried.reshape(R // fold, fold, W, O)
            yf[m, t] = fold_rows([term[:, k] for k in range(fold)]).reshape(R // fold, W, fold * O)
    for d in sorted(range(1, Z), key=lambda d: -abs(2 * d - Z)):
        y_own[d].start()
    rf[z] = yf[z]

    for d in range(1, Z):
        y_own[d].wait()
    chunks = []
    for m in range(Z):
        chunks.append(unfold_rows(rf[m], O).reshape(rows, O))
    branch = jnp.concatenate(chunks, axis=1)
    source = latent[...].reshape(rows, C).astype(f32)
    out[...] = (source + branch).astype(bf16).reshape(F, R, W, C)
    stores[0].start()

    grad_one = b_out.total(yb[:, :, block(z)].astype(f32)).reshape(rows, C)
    normed_one, inverse_one = normalize(source, g_one)
    grad = norm_backward(source, inverse_one, g_one, grad_one * silu_slope(normed_one))
    upstream = cotangent[...].reshape(rows, C).astype(f32)
    latent_grad[...] = (upstream + grad).astype(bf16).reshape(F, R, W, C)
    stores[1].start()
    links.drain()
    for store in stores:
        store.wait()


def hand_over(first, second, first_out, second_out, sem):
    copies = [
        pltpu.make_async_copy(first, first_out, sem.at[0]),
        pltpu.make_async_copy(second, second_out, sem.at[1]),
    ]
    for made in copies:
        made.start()
    for made in copies:
        made.wait()


def local(sizes, latent, cotangent, gain_one, gain_two, kernel_one, kernel_two):
    S, Q, Z = sizes
    F, R, W, C = latent.shape
    O = kernel_one.shape[3]
    WW = W * Z
    OP = -(-O // 128) * 128
    rows = F * R * W
    taps = kernel_one.shape[:3]
    fold = fold_of(R, O)
    packed = (F, R, W, C)
    slots = (Z - 1) * (6 + 2 * F) + 2 * Z + 15
    shapes = [
        kernel_one.shape,
        kernel_two.shape,
        taps + (O, Z * OP),
        packed,
        (F, R + 2, WW, C),
        (Z, F, R // fold, W, fold * O),
        (Z, F, R // fold, W, fold * O),
        (Z, 2, R // fold, W, fold * O),
        (F + 2, R + 2, WW, OP),
        (Z,) + packed,
        (4,) + packed,
        (2, R, W, C),
        (2, R, W, C),
        (Z,) + packed,
        None,
        None,
        (Z, F, R + 2, WW, OP),
        (F + 2, R, W, C),
        (2, R, W, C),
        (F + 2, W, C),
        (F + 2, W, C),
        (F + 2, R + 2, WW, OP),
        (Z, F, R // fold, W, fold * O),
        (Z, F, R // fold, W, fold * O),
        (2, R, W, C),
        (2, R, W, C),
        (F, R, WW, C),
        (4,) + packed,
        (2, max(Z - 3, 1)) + packed,
        (2, max(Z - 3, 1)) + packed,
        (2, R, W, C),
        (2, R, W, C),
        None,
        None,
        None,
        packed,
        packed,
        None,
        None,
        packed,
        packed,
    ]
    scratch = [pltpu.VMEM(shape, bf16) if shape else None for shape in shapes]
    scratch[14] = pltpu.VMEM((2, Z, 8, rows), f32)
    scratch[15] = pltpu.VMEM((Z, 8, C), f32)
    scratch[32] = pltpu.VMEM((8, rows), f32)
    scratch[33] = pltpu.VMEM((Z + 1, 8, rows), f32)
    scratch[34] = pltpu.VMEM((F, R * WW, 3 * C), f32)
    scratch[37] = scratch[38] = pltpu.VMEM((C,), f32)
    hbm = pl.BlockSpec(memory_space=pltpu.HBM)
    results = pl.pallas_call(
        functools.partial(kernel, sizes),
        out_shape=[jax.ShapeDtypeStruct((F, R, W, C), bf16)] * 2,
        in_specs=[hbm] * 6,
        out_specs=[hbm] * 2,
        scratch_shapes=[
            *scratch,
            pltpu.SemaphoreType.DMA((slots,)),
            pltpu.SemaphoreType.DMA((slots,)),
            pltpu.SemaphoreType.DMA((8,)),
            pltpu.SemaphoreType.REGULAR((2, max(Z - 2, 1))),
        ],
        compiler_params=pltpu.CompilerParams(
            collective_id=0, has_side_effects=True, vmem_limit_bytes=60 * 1024 * 1024
        ),
    )(latent, cotangent, gain_one, gain_two, kernel_one, kernel_two)
    vmem = pl.BlockSpec(memory_space=pltpu.VMEM)

    def pass_on(first, second, first_out, second_out):
        first_out[...] = first[...]
        second_out[...] = second[...]

    return pl.pallas_call(
        pass_on,
        out_shape=[jax.ShapeDtypeStruct((F, R, W, C), bf16)] * 2,
        in_specs=[vmem] * 2,
        out_specs=[vmem] * 2,
    )(*results)

def solution(mesh):
    sizes = (mesh.shape["section"], mesh.shape["seq"], mesh.shape["exp"])
    spread = P("section", "seq", "exp", None)
    split = P(None, None, None, "exp", None)
    return jax.shard_map(
        functools.partial(local, sizes),
        mesh=mesh,
        in_specs=(spread, spread, P(), P(), split, split),
        out_specs=(spread, spread),
        check_vma=False,
    )
```

```python
import functools

import jax
import jax.numpy as jnp
from jax import lax
from jax.experimental import pallas as pl
from jax.experimental.pallas import tpu as pltpu
from jax.sharding import PartitionSpec as P

epsilon = 1e-06
MESH = pl.DeviceIdType.MESH
bf16, f32 = jnp.bfloat16, jnp.float32


def normalize(values, gain):
    inverse = lax.rsqrt(jnp.mean(values * values, axis=-1, keepdims=True) + epsilon)
    return values * inverse * gain, inverse


def norm_backward(values, inverse, gain, upstream):
    scaled = upstream * gain
    mean = jnp.mean(values * scaled, axis=-1, keepdims=True)
    return inverse * scaled - values * (inverse * inverse * inverse) * mean


def silu(normed):
    return normed / (1.0 + jnp.exp(-normed))


def silu_slope(normed):
    sigma = 1.0 / (1.0 + jnp.exp(-normed))
    return sigma * (1.0 + normed * (1.0 - sigma))


def shift_sum(taps, width, size):
    rows = taps.shape[0]
    column = lax.rem(lax.broadcasted_iota(jnp.int32, (rows, size), 0), width)
    low = pltpu.roll(taps[:, :size], 1, axis=0)
    high = pltpu.roll(taps[:, 2 * size :], rows - 1, axis=0)
    return (
        taps[:, size : 2 * size]
        + jnp.where(column == 0, 0.0, low)
        + jnp.where(column == width - 1, 0.0, high)
    )


def fold_of(rows, width):
    return next((n for n in (4, 2) if rows % n == 0 and n * width % 128 == 0), 1)


def pad_to(value, axis, size):
    shape = list(value.shape)
    if shape[axis] == size:
        return value
    shape[axis] = size - shape[axis]
    return jnp.concatenate([value, jnp.zeros(shape, value.dtype)], axis=axis)


class Links:
    def __init__(self, send, recv):
        self.send, self.recv, self.slots, self.open = send, recv, 0, []

    def copy(self, src, dst, device, sends=True, receives=True, after=None):
        slot = self.slots if after is None else after.slot
        self.slots += after is None
        made = Copy(self, slot, src, dst, device, sends, receives)
        self.open.append(made)
        return made

    def retire(self, copies):
        for made in copies:
            made.drain()
            self.open.remove(made)

    def drain(self):
        for made in self.open:
            made.drain()
        assert self.slots == self.send.shape[0], self.slots


class Copy:
    def __init__(self, links, slot, src, dst, device, sends, receives):
        self.made = lambda: pltpu.make_async_remote_copy(
            src_ref=src,
            dst_ref=dst,
            send_sem=links.send.at[slot],
            recv_sem=links.recv.at[slot],
            device_id=device,
            device_id_type=MESH,
        )
        self.slot, self.sends, self.receives = slot, sends, receives

    def start(self):
        when(self.sends, lambda: self.made().start())

    def wait(self):
        when(self.receives, lambda: self.made().wait_recv())

    def drain(self):
        when(self.sends, lambda: self.made().wait_send())


def when(condition, action):
    if condition is True:
        action()
    else:
        pl.when(condition)(action)


def kernel(sizes, latent_hbm, cotangent_hbm, gain_one_hbm, gain_two_hbm, kernel_one, kernel_two, out, latent_grad, *scratch):
    S, Q, Z = sizes
    (
        w_one, w_two, w_gap, act, xp, qs, qr, qn, qp, gs, gr, fs, fr, vall, st, gains,
        xq, gi, gh, gu, gd, qq, yf, rf, ys, yr, yb, rb, g_hop, b_hop, vh, gt, sq, sh, early,
        latent, cotangent, gain_one, gain_two, send, recv, w_sem, seen,
    ) = scratch
    F, R, W, C = latent_hbm.shape
    O = kernel_one.shape[3]
    WW = W * Z
    OP = -(-O // 128) * 128
    rows = F * R * W
    s, q, z = lax.axis_index("section"), lax.axis_index("seq"), lax.axis_index("exp")
    has_next, has_prev = s < S - 1, s > 0
    has_high, has_low = q < Q - 1, q > 0
    both = jnp.logical_and
    nxt, prv = jnp.minimum(s + 1, S - 1), jnp.maximum(s - 1, 0)
    upper, lower = jnp.minimum(q + 1, Q - 1), jnp.maximum(q - 1, 0)
    fold = fold_of(R, O)
    body, own, halo = pl.ds(1, R), pl.ds(0, F), pl.ds(F, 2)
    two = pl.ds(0, 2)
    links = Links(send, recv)

    barrier = pltpu.get_barrier_semaphore()
    loads = [
        pltpu.make_async_copy(src, dst, w_sem.at[k])
        for k, (src, dst) in enumerate(
            [
                (cotangent_hbm, cotangent),
                (latent_hbm, latent),
                (gain_one_hbm, gain_one),
                (gain_two_hbm, gain_two),
                (kernel_two, w_two),
                (kernel_one, w_one),
            ]
        )
    ]
    load_two, load_one = loads[4:]
    for load in loads[:4]:
        load.start()

    def greet(device):
        pl.semaphore_signal(barrier, inc=1, device_id=device, device_id_type=MESH)

    has_right, has_left = z < Z - 1, z > 0
    for beside, step in ((has_right, 1), (has_left, -1)):

        @pl.when(beside)
        def _():
            greet((s, q, z + step))

    for near, step in ((has_next, 1), (has_prev, -1)):

        @pl.when(near)
        def _():
            greet((s + step, q, z))

        for side, move in ((has_high, 1), (has_low, -1)):

            @pl.when(both(near, side))
            def _():
                greet((s + step, q + move, z))

    for side, move in ((has_high, 1), (has_low, -1)):

        @pl.when(side)
        def _():
            greet((s, q + move, z))

    for load in loads[4:]:
        load.start()

    def peer(d):
        return lax.rem(z + d + Z, Z)

    def block(index):
        return pl.ds(pl.multiple_of(index * W, W), W)

    def gather(source, at, reach, after=None):
        arrive = []
        for d in range(1, Z):
            for sign in (1, -1):
                if d <= reach:
                    target, sends = z + sign * d, (z + d < Z) if sign > 0 else (z >= d)
                    src, dst = source, at(z)
                else:
                    target = z + sign
                    held = z - sign * (d - 1)
                    sends = both(z < Z - 1, z >= d - 1) if sign > 0 else both(z > 0, z <= Z - d)
                    src = dst = at(jnp.clip(held, 0, Z - 1))
                receives = (z >= d) if sign > 0 else (z + d < Z)
                target = jnp.clip(target, 0, Z - 1)
                earlier = None if after is None else after[len(arrive)][2]
                arrive.append((d, z - sign * d, links.copy(src, dst, (s, q, target), sends, receives, earlier)))
        return arrive

    def gather_start(arrive, distances):
        for d in distances:
            for distance, _, made in arrive:
                if distance == d:
                    made.start()

    def gather_wait(arrive, d, reach, use=None):
        for distance, owner, made in arrive:
            if distance == d:
                made.wait()
        for distance, owner, made in arrive:
            if distance == d + 1 and d >= reach:
                made.start()
        if use is not None:
            for distance, owner, made in arrive:
                if distance == d:
                    when(made.receives, functools.partial(use, owner))

    class Scatter:
        def __init__(self, at, landing, hop, after=None):
            self.at, self.landing, self.hop, self.far, self.near = at, landing, hop, {}, {}
            for sign in (1, -1):
                for D in range(Z - 1, 0, -1):
                    for f in range(F):
                        target, origin = z + sign * D, z - sign * D
                        sends = (z + D < Z) if sign > 0 else (z >= D)
                        src = at(jnp.clip(target, 0, Z - 1), f)
                        if D >= 3:
                            before = (z >= 1) if sign > 0 else (z < Z - 1)
                            further = (z + D <= Z) if sign > 0 else (z >= D - 1)
                            self.far[sign, D, f] = links.copy(
                                src,
                                hop.at[int(sign > 0), D - 3, f],
                                (s, q, jnp.clip(z + sign, 0, Z - 1)),
                                sends,
                                both(before, further),
                                after and after.far[sign, D, f],
                            )
                        else:
                            receives = (z >= D) if sign > 0 else (z + D < Z)
                            slot = 2 * (sign > 0) + D - 1
                            self.near[sign, D, f] = links.copy(
                                src,
                                landing.at[slot, f],
                                (s, q, jnp.clip(target, 0, Z - 1)),
                                sends,
                                receives,
                                after and after.near[sign, D, f],
                            )

        def copies(self):
            return [*self.far.values(), *self.near.values()]

        def start(self, f, distances):
            for D in distances:
                for sign in (1, -1):
                    made = self.far.get((sign, D, f)) or self.near[sign, D, f]
                    joined = self.far.get((sign, D + 1, f))
                    if joined is None:
                        made.start()
                    else:
                        when(both(made.sends, jnp.logical_not(joined.receives)), lambda: made.made().start())

        def join(self, f):
            for D in range(Z - 1, 2, -1):
                for sign in (1, -1):
                    arrived = self.far[sign, D, f]
                    onward = self.far.get((sign, D - 1, f)) or self.near[sign, D - 1, f]

                    @pl.when(arrived.receives)
                    def _():
                        arrived.made().wait_recv()
                        held = self.at(jnp.clip(z + sign * (D - 1), 0, Z - 1), f)
                        total = held[...].astype(f32) + self.hop[int(sign > 0), D - 3, f].astype(f32)
                        held[...] = total.astype(bf16)
                        onward.made().start()

        def total(self, own):
            for D in (1, 2):
                for sign in (1, -1):
                    for f in range(F):
                        if (sign, D, f) in self.near:
                            self.near[sign, D, f].wait()
            for D in (1, 2):
                for sign in (1, -1):
                    if (sign, D, 0) in self.near:
                        made = self.near[sign, D, 0]
                        term = self.landing[2 * (sign > 0) + D - 1].astype(f32)
                        own = own + jnp.where(made.receives, term, 0.0)
            return own

    q_own = {}
    for d in range(1, Z):
        for sign in (1, -1):
            target = jnp.clip(z + sign * d, 0, Z - 1)
            ends = (z + d < Z, z >= d)
            q_own[sign, d] = links.copy(qs.at[target], qr.at[z], (s, q, target), *ends[::sign])
    q_next = {
        d: links.copy((qr if d else qs).at[peer(-d), two], qn.at[peer(-d)], (prv, q, z), has_prev, has_next)
        for d in range(Z)
    }

    def q_pass_on(sign, d):
        made = q_own[sign, d]
        made.wait()

        @pl.when(made.receives)
        def _():
            q_next[(sign * d) % Z].start()

    def rows_out(src, dst, device, towards, after=None):
        sides = (has_high, has_low) if towards > 0 else (has_low, has_high)
        return links.copy(src, dst, device, *sides, after)

    q_rows = [
        rows_out(qp.at[own, R], qp.at[own, 0], (s, upper, z), 1),
        rows_out(qp.at[own, 1], qp.at[own, R + 1], (s, lower, z), -1),
    ]
    q_corner = [
        links.copy(qp.at[two, R], qp.at[halo, 0], (prv, upper, z), both(has_prev, has_high), both(has_next, has_low)),
        links.copy(qp.at[two, 1], qp.at[halo, R + 1], (prv, lower, z), both(has_prev, has_low), both(has_next, has_high)),
    ]
    x_rows = [
        rows_out(xp.at[:, R], xp.at[:, 0], (s, upper, z), 1),
        rows_out(xp.at[:, 1], xp.at[:, R + 1], (s, lower, z), -1),
    ]
    x_all = gather(act, lambda owner: xp.at[:, body, block(owner)], 2)
    g_out = Scatter(lambda owner, f: gs.at[owner, f], gr, g_hop)
    f_out = [links.copy(fs.at[t], fr.at[t], (nxt, q, z), has_next, has_prev) for t in range(2)]
    v_all = gather(vall.at[z], lambda owner: vall.at[owner], 2, x_all)
    sums = [
        {
            d: links.copy(st.at[k, 0], st.at[k, d], (s, q, peer(d)), True, True, q_own[-1, d] if k else None)
            for d in range(1, Z)
        }
        for k in range(2)
    ]
    xq_rows = [
        rows_out(xq.at[:, :, R], xq.at[:, :, 0], (s, upper, z), 1),
        rows_out(xq.at[:, :, 1], xq.at[:, :, R + 1], (s, lower, z), -1),
    ]
    v_next = links.copy(vall.at[z, two], vh, (prv, q, z), has_prev, has_next, q_corner[0])
    g_next = links.copy(gt, gh, (prv, q, z), has_prev, has_next, q_corner[1])
    squares_next = links.copy(sq, sh.at[Z], (prv, q, z), has_prev, has_next)
    sums_next = {
        d: links.copy(st.at[1, 0], sh.at[d], (prv, q, peer(d)), has_prev, has_next, q_next[d]) for d in range(Z)
    }

    def gi_out(frames, after):
        return [
            rows_out(gi.at[frames, R - 1], gd.at[frames], (s, upper, z), 1, after[0]),
            rows_out(gi.at[frames, 0], gu.at[frames], (s, lower, z), -1, after[1]),
        ]

    gi_rows, gi_corner = gi_out(own, q_rows), gi_out(halo, (None, None))
    b_out = Scatter(lambda owner, f: yb.at[f, :, block(owner)], rb, b_hop, g_out)
    y_own = {
        d: links.copy(yf.at[peer(d)], rf.at[z], (s, q, peer(d)), True, True, q_own[1, d]) for d in range(1, Z)
    }
    y_next = [
        links.copy(ys.at[t], yr.at[t], (nxt, q, z), has_next, has_prev, f_out[t]) for t in range(2)
    ]

    lane = lax.broadcasted_iota(jnp.int32, (8, C), 1)
    group = lax.broadcasted_iota(jnp.int32, (8, C), 0)
    segments = jnp.where(both(lane >= group * O, lane < group * O + O), 1.0, 0.0).astype(f32)

    def pack(value, offset=0):
        count = value.shape[0] // WW
        grouped = value.reshape(count, Z, W, value.shape[1])
        return jnp.concatenate(
            [grouped[:, m].reshape(count * W, value.shape[1])[:, offset : offset + O] for m in range(Z)], axis=1
        )

    def unpack(packed, m):
        return pad_to(packed[:, m * O : (m + 1) * O], 1, OP)

    segments_three = jnp.concatenate([segments] * 3, axis=1).astype(bf16)
    segments_down = jnp.concatenate([segments] * 3, axis=0).astype(bf16)

    def thirds(value, axis):
        high = value.astype(bf16).astype(f32)
        middle = (value - high).astype(bf16).astype(f32)
        return jnp.concatenate([high, middle, value - high - middle], axis=axis).astype(bf16)

    def segment_sums(value):
        return lax.dot_general(
            segments_three, thirds(value, 1), (((1,), (1,)), ((), ())), preferred_element_type=f32
        )

    def spread(tile):
        return lax.dot_general(
            thirds(tile, 0), segments_down, (((0,), (0,)), ((), ())), preferred_element_type=f32
        )

    def rhs_forward(w, taps):
        return jnp.concatenate(
            [
                jnp.concatenate([pad_to(w[i, j, l], 0, OP) for l in range(3) for i in taps], axis=0)
                for j in range(3)
            ],
            axis=1,
        )

    def rhs_backward(w, i):
        return jnp.concatenate(
            [jnp.concatenate([pad_to(w[2 - i, 2 - j, 2 - l], 0, OP) for l in range(3)], axis=1) for j in range(3)],
            axis=0,
        )

    def forward(lhs_of, w):
        parts = {}

        def run(f, taps):
            product = lax.dot_general(
                lhs_of(f), rhs_forward(w, taps), (((1,), (1,)), ((), ())), preferred_element_type=f32
            )
            joined = shift_sum(product, WW, len(taps) * OP)
            for n, i in enumerate(taps):
                parts.setdefault(f + 2 - i, []).append(joined[:, n * OP : n * OP + O])

        def finish(t):
            return functools.reduce(lambda a, b: a + b, parts[t])

        def ahead(t):
            if not parts:
                for f in range(F - 1, max(F - 3, -1), -1):
                    run(f, (0, 1))
            return finish(t)

        def rest(t):
            for f in range(F):
                if f + 2 - 2 == t:
                    run(f, (2,) if f >= F - 2 else (0, 1, 2))
            return finish(t)

        return ahead, rest

    def backward(qbuf, w, f, taps):
        lhs = jnp.concatenate(
            [
                pad_to(qbuf[f + i, pl.ds(j, R)].reshape(R * WW, qbuf.shape[3]), 1, OP)
                for i in taps
                for j in range(3)
            ],
            axis=1,
        )
        rhs = jnp.concatenate([rhs_backward(w, i) for i in taps], axis=0)
        return jnp.dot(lhs, rhs, preferred_element_type=f32)

    def fold_rows(pieces):
        return jnp.concatenate([p.reshape(p.shape[0] * W, O) for p in pieces], axis=1).astype(bf16)

    def unfold_rows(value, width):
        value = value.reshape(value.shape[0] * value.shape[1], W, fold * O).astype(f32)
        parts = [pad_to(value[:, :, k * O : (k + 1) * O], 2, width) for k in range(fold)]
        return jnp.stack(parts, axis=1).reshape(-1, R, W, width)

    loads[0].wait()
    folded = cotangent[...].astype(f32).reshape(F * R // fold, fold, W, C)
    for m in range(Z):
        qs[m] = fold_rows([folded[:, k, :, m * O : (m + 1) * O] for k in range(fold)]).reshape(qs.shape[1:])
    for load in loads[1:4]:
        load.wait()
    source = latent[...].reshape(rows, C).astype(f32)
    g_one, g_two = gain_one[...].reshape(1, C), gain_two[...].reshape(1, C)
    normed_one, _ = normalize(source, g_one)
    act[...] = silu(normed_one).astype(bf16).reshape(F, R, W, C)

    near = has_next.astype(jnp.int32) + has_prev.astype(jnp.int32)
    sides = has_high.astype(jnp.int32) + has_low.astype(jnp.int32)
    beside = has_right.astype(jnp.int32) + has_left.astype(jnp.int32)
    pl.semaphore_wait(barrier, beside + near + sides + near * sides)

    def announce(d):
        for k, known, teller in (
            (0, z + d - 1 < Z, has_left),
            (1, z >= d - 1, has_right),
        ):

            @pl.when(both(known, teller))
            def _():
                pl.semaphore_signal(
                    seen.at[k, d - 2],
                    inc=1,
                    device_id=(s, q, jnp.clip(z - 1 if k == 0 else z + 1, 0, Z - 1)),
                    device_id_type=MESH,
                )

    def await_seen(d):
        for k, known in ((0, z + d < Z), (1, z >= d)):

            @pl.when(known)
            def _():
                pl.semaphore_wait(seen.at[k, d - 2], 1)

    for d in range(1, Z):
        if d > 1:
            await_seen(d)
        if d < Z - 1:
            announce(d + 1)
        for sign in (1, -1):
            q_own[sign, d].start()
    qr[z] = qs[z]
    xp[:, body, block(z)] = act[...]
    q_next[0].start()

    def zero(ref, index):
        ref[index] = jnp.zeros_like(ref[index])

    full = slice(None)

    @pl.when(jnp.logical_not(has_next))
    def _():
        zero(qp, (halo,))
        zero(qq, (halo,))

    for missing, row in ((jnp.logical_not(has_low), 0), (jnp.logical_not(has_high), R + 1)):

        @pl.when(missing)
        def _():
            zero(qp, (full, row))
            zero(qq, (full, row))
            zero(xp, (full, row))
            zero(xq, (full, full, row))

    @pl.when(jnp.logical_not(has_prev))
    def _():
        zero(fr, (full,))
        zero(yr, (full,))

    for m in range(Z):
        gains[m] = jnp.broadcast_to(jnp.concatenate([g_two[:, m * O : (m + 1) * O]] * Z, axis=1), (8, C))

    load_two.wait()
    for i in range(3):
        for j in range(3):
            for l in range(3):
                w = w_two[i, j, l].astype(f32)
                w_gap[i, j, l] = jnp.concatenate(
                    [pad_to(w[:, m * O : (m + 1) * O], 1, OP) for m in range(Z)], axis=1
                ).astype(bf16)
    gather_start(x_all, (2, 1))
    for d in range(1, Z):
        for sign in (1, -1):
            q_pass_on(sign, d)
    for m in range(Z):
        qp[own, body, m * W : (m + 1) * W] = unfold_rows(qr[m], OP).astype(bf16)
    for made in q_rows + q_corner:
        made.start()
    for made in q_rows:
        made.wait()
    for f in range(F):
        early[f] = backward(qp, w_two, f, range(F - f))
    for d in range(Z):
        q_next[d].wait()

    @pl.when(has_next)
    def _():
        for m in range(Z):
            qp[halo, body, m * W : (m + 1) * W] = unfold_rows(qn[m], OP).astype(bf16)

    for made in q_corner:
        made.wait()
    for f in range(F):
        total = early[f] + backward(qp, w_two, f, range(F - f, 3))
        total = shift_sum(total, WW, C)
        if f == 0:
            gather_wait(x_all, 2, 2)
        for m in range(Z):
            gs[m, f] = pack(total, m * O).astype(bf16).reshape(R, W, C)
        g_out.start(f, range(Z - 1, 1, -1))
    for f in range(F):
        g_out.start(f, (1,))

    gather_wait(x_all, 1, 2)
    for d in range(3, Z):
        gather_wait(x_all, d, 2)
    for made in x_rows:
        made.start()
    load_one.wait()
    for made in x_rows:
        made.wait()

    def lhs_one(f):
        return jnp.concatenate([xp[f, pl.ds(j, R)].reshape(R * WW, C) for j in range(3)], axis=1)

    ahead, inner = forward(lhs_one, w_one)
    for t in (F + 1, F):
        fs[t - F] = pack(ahead(t)).astype(bf16).reshape(R, W, C)
        f_out[t - F].start()
    rest, inner = inner, []
    for t in range(F):
        g_out.join(t)
        inner.append(pack(rest(t)))
    for made in f_out:
        made.wait()
    for t in range(2):
        inner[t] = inner[t] + fr[t].reshape(R * W, C).astype(f32)
    inner = jnp.concatenate(inner, axis=0)
    vall[z] = inner.astype(bf16).reshape(F, R, W, C)
    st[0, 0] = segment_sums(inner * inner)
    for d in range(1, Z):
        sums[0][d].start()

    links.retire([*q_own.values(), *q_next.values(), *q_corner])
    v_next.start()
    grad_two = g_out.total(gs[z].astype(f32)).reshape(rows, C)
    gt[...] = grad_two[: 2 * R * W].astype(bf16).reshape(2, R, W, C)
    g_next.start()
    links.retire([made for _, _, made in x_all])
    gather_start(v_all, (2,))
    squares = st[0, 0]
    for d in range(1, Z):
        sums[0][d].wait()
        squares = squares + st[0, d]
    sq[...] = squares
    squares_next.start()
    inverse = lax.rsqrt(squares / C + epsilon)
    inverse_wide = spread(inverse)
    gain = gains[z][0:1]
    scaled = grad_two * silu_slope(inner * inverse_wide * gain) * gain
    st[1, 0] = segment_sums(inner * scaled)
    for d in range(1, Z):
        sums[1][d].start()
    for d in range(Z):
        sums_next[d].start()

    def activate(owner):
        value = vall[owner].reshape(rows, C).astype(f32)
        active = silu(value * inverse_wide * gains[owner][0:1])
        for m in range(Z):
            xq[owner, :, body, m * W : (m + 1) * W] = unpack(active, m).astype(bf16).reshape(F, R, W, OP)

    gather_start(v_all, (1,))
    activate(z)
    gather_wait(v_all, 2, 2, activate)

    links.retire([*f_out, *q_rows, *g_out.copies()])
    means = st[1, 0]
    for d in range(1, Z):
        sums[1][d].wait()
        means = means + st[1, d]
    factor = spread(inverse * inverse * inverse * means / C)
    grad_inner = (inverse_wide * scaled - inner * factor).astype(bf16)
    gi[own] = grad_inner.reshape(F, R, W, C)
    for made in gi_rows:
        made.start()

    def place(ref, frames, band, count):
        value = ref.reshape(count, C).astype(f32)
        for m in range(Z):
            piece = unpack(value, m).astype(bf16)
            qq[frames, band, m * W : (m + 1) * W] = piece.reshape(
                qq.at[frames, band, m * W : (m + 1) * W].shape
            )

    place(gi[own], own, body, rows)

    def place_rows(frames, count, among):
        for side, ref, row in ((has_low, gd, 0), (has_high, gu, R + 1)):

            @pl.when(side if among is None else both(side, among))
            def _():
                place(ref[frames], frames, row, count * W)

    gather_wait(v_all, 1, 2, activate)
    for made in (v_next, g_next, squares_next):
        made.wait()
    for d in range(Z):
        sums_next[d].wait()

    @pl.when(has_next)
    def _():
        taken = slice(0, 2 * R * W)
        inverse = lax.rsqrt(sh[Z] / C + epsilon)
        mean = sh[0]
        for d in range(1, Z):
            mean = mean + sh[d]
        value = vh[...].reshape(2 * R * W, C).astype(f32)
        inverse_wide = spread(inverse)[taken]
        upstream = gh[...].reshape(2 * R * W, C).astype(f32)
        upstream = upstream * silu_slope(value * inverse_wide * gain) * gain
        factor = spread(inverse * inverse * inverse * mean / C)[taken]
        gi[halo] = (inverse_wide * upstream - value * factor).astype(bf16).reshape(2, R, W, C)
        place(gi[halo], halo, body, 2 * R * W)

    @pl.when(jnp.logical_not(has_next))
    def _():
        zero(gi, (halo,))

    for made in gi_corner:
        made.start()
    for d in range(3, Z):
        gather_wait(v_all, d, 2, activate)
    for made in xq_rows:
        made.start()
    for made in gi_rows:
        made.wait()
    place_rows(own, F, None)
    for f in range(F):
        early[f] = backward(qq, w_one, f, range(F - f))
    for made in gi_corner:
        made.wait()
    place_rows(halo, 2, has_next)
    for f in range(F):
        total = early[f] + backward(qq, w_one, f, range(F - f, 3))
        yb[f] = shift_sum(total, WW, C).astype(bf16).reshape(R, WW, C)
        b_out.start(f, range(Z - 1, 2, -1))
    for d in (2, 1):
        for f in range(F):
            b_out.start(f, (d,))

    def lhs_two(f):
        return jnp.concatenate(
            [xq[m, f, pl.ds(j, R)].reshape(R * WW, OP) for j in range(3) for m in range(Z)], axis=1
        )

    for made in xq_rows:
        made.wait()
    ahead, branch = forward(lhs_two, w_gap)
    for t in (F + 1, F):
        ys[t - F] = pack(ahead(t)).astype(bf16).reshape(R, W, C)
        y_next[t - F].start()
    rest, branch = branch, []
    for t in range(F):
        b_out.join(t)
        branch.append(rest(t).reshape(R, Z, W, O))
    for made in y_next:
        made.wait()
    for t in range(F):
        for m in range(Z):
            term = branch[t][:, m].reshape(R // fold, fold, W, O)
            if t < 2:
                carried = yr[t].reshape(R * W, C).astype(f32)[:, m * O : (m + 1) * O]
                term = term + carried.reshape(R // fold, fold, W, O)
            yf[m, t] = fold_rows([term[:, k] for k in range(fold)]).reshape(R // fold, W, fold * O)
    for d in sorted(range(1, Z), key=lambda d: -abs(2 * d - Z)):
        y_own[d].start()
    rf[z] = yf[z]

    source = latent[...].reshape(rows, C).astype(f32)
    normed_one, inverse_one = normalize(source, g_one)
    slope_one = silu_slope(normed_one)
    upstream = cotangent[...].reshape(rows, C).astype(f32)
    grad_one = b_out.total(yb[:, :, block(z)].astype(f32)).reshape(rows, C)
    grad = norm_backward(source, inverse_one, g_one, grad_one * slope_one)
    latent_grad[...] = (upstream + grad).astype(bf16).reshape(F, R, W, C)
    for d in range(1, Z):
        y_own[d].wait()
    branch = jnp.concatenate([unfold_rows(rf[m], O).reshape(rows, O) for m in range(Z)], axis=1)
    out[...] = (source + branch).astype(bf16).reshape(F, R, W, C)
    links.drain()


def hand_over(first, second, first_out, second_out, sem):
    copies = [
        pltpu.make_async_copy(first, first_out, sem.at[0]),
        pltpu.make_async_copy(second, second_out, sem.at[1]),
    ]
    for made in copies:
        made.start()
    for made in copies:
        made.wait()


def local(sizes, latent, cotangent, gain_one, gain_two, kernel_one, kernel_two):
    S, Q, Z = sizes
    F, R, W, C = latent.shape
    O = kernel_one.shape[3]
    WW = W * Z
    OP = -(-O // 128) * 128
    rows = F * R * W
    taps = kernel_one.shape[:3]
    fold = fold_of(R, O)
    packed = (F, R, W, C)
    slots = (Z - 1) * (5 + 2 * F) + Z + 13
    shapes = [
        kernel_one.shape,
        kernel_two.shape,
        taps + (O, Z * OP),
        packed,
        (F, R + 2, WW, C),
        (Z, F, R // fold, W, fold * O),
        (Z, F, R // fold, W, fold * O),
        (Z, 2, R // fold, W, fold * O),
        (F + 2, R + 2, WW, OP),
        (Z,) + packed,
        (4,) + packed,
        (2, R, W, C),
        (2, R, W, C),
        (Z,) + packed,
        None,
        None,
        (Z, F, R + 2, WW, OP),
        (F + 2, R, W, C),
        (2, R, W, C),
        (F + 2, W, C),
        (F + 2, W, C),
        (F + 2, R + 2, WW, OP),
        (Z, F, R // fold, W, fold * O),
        (Z, F, R // fold, W, fold * O),
        (2, R, W, C),
        (2, R, W, C),
        (F, R, WW, C),
        (4,) + packed,
        (2, max(Z - 3, 1)) + packed,
        (2, max(Z - 3, 1)) + packed,
        (2, R, W, C),
        (2, R, W, C),
        None,
        None,
        None,
        packed,
        packed,
        None,
        None,
    ]
    scratch = [pltpu.VMEM(shape, bf16) if shape else None for shape in shapes]
    scratch[14] = pltpu.VMEM((2, Z, 8, rows), f32)
    scratch[15] = pltpu.VMEM((Z, 8, C), f32)
    scratch[32] = pltpu.VMEM((8, rows), f32)
    scratch[33] = pltpu.VMEM((Z + 1, 8, rows), f32)
    scratch[34] = pltpu.VMEM((F, R * WW, 3 * C), f32)
    scratch[37] = scratch[38] = pltpu.VMEM((C,), f32)
    hbm = pl.BlockSpec(memory_space=pltpu.HBM)
    results = pl.pallas_call(
        functools.partial(kernel, sizes),
        out_shape=[jax.ShapeDtypeStruct((F, R, W, C), bf16)] * 2,
        in_specs=[hbm] * 6,
        out_specs=[pl.BlockSpec(memory_space=pltpu.VMEM)] * 2,
        scratch_shapes=[
            *scratch,
            pltpu.SemaphoreType.DMA((slots,)),
            pltpu.SemaphoreType.DMA((slots,)),
            pltpu.SemaphoreType.DMA((6,)),
            pltpu.SemaphoreType.REGULAR((2, max(Z - 2, 1))),
        ],
        compiler_params=pltpu.CompilerParams(
            collective_id=0, has_side_effects=True, vmem_limit_bytes=28 * 1024 * 1024
        ),
    )(*[pltpu.with_memory_space_constraint(a, pltpu.HBM) for a in (latent, cotangent, gain_one, gain_two, kernel_one, kernel_two)])
    vmem = pl.BlockSpec(memory_space=pltpu.VMEM)
    return pl.pallas_call(
        hand_over,
        out_shape=[jax.ShapeDtypeStruct((F, R, W, C), bf16)] * 2,
        in_specs=[vmem] * 2,
        out_specs=[hbm] * 2,
        scratch_shapes=[pltpu.SemaphoreType.DMA((2,))],
    )(*[pltpu.with_memory_space_constraint(a, pltpu.VMEM) for a in results])

def solution(mesh):
    sizes = (mesh.shape["section"], mesh.shape["seq"], mesh.shape["exp"])
    spread = P("section", "seq", "exp", None)
    split = P(None, None, None, "exp", None)
    return jax.shard_map(
        functools.partial(local, sizes),
        mesh=mesh,
        in_specs=(spread, spread, P(), P(), split, split),
        out_specs=(spread, spread),
        check_vma=False,
    )
```

```python
import functools

import jax
import jax.numpy as jnp
from jax import lax
from jax.experimental import pallas as pl
from jax.experimental.pallas import tpu as pltpu
from jax.sharding import PartitionSpec as P

epsilon = 1e-06
MESH = pl.DeviceIdType.MESH
bf16, f32 = jnp.bfloat16, jnp.float32


def normalize(values, gain):
    inverse = lax.rsqrt(jnp.mean(values * values, axis=-1, keepdims=True) + epsilon)
    return values * inverse * gain, inverse


def norm_backward(values, inverse, gain, upstream):
    scaled = upstream * gain
    mean = jnp.mean(values * scaled, axis=-1, keepdims=True)
    return inverse * scaled - values * (inverse * inverse * inverse) * mean


def silu(normed):
    return normed / (1.0 + jnp.exp(-normed))


def silu_slope(normed):
    sigma = 1.0 / (1.0 + jnp.exp(-normed))
    return sigma * (1.0 + normed * (1.0 - sigma))


def shift_sum(taps, width, size):
    rows = taps.shape[0]
    column = lax.rem(lax.broadcasted_iota(jnp.int32, (rows, size), 0), width)
    low = pltpu.roll(taps[:, :size], 1, axis=0)
    high = pltpu.roll(taps[:, 2 * size :], rows - 1, axis=0)
    return (
        taps[:, size : 2 * size]
        + jnp.where(column == 0, 0.0, low)
        + jnp.where(column == width - 1, 0.0, high)
    )


def fold_of(rows, width):
    return next((n for n in (4, 2) if rows % n == 0 and n * width % 128 == 0), 1)


def pad_to(value, axis, size):
    shape = list(value.shape)
    if shape[axis] == size:
        return value
    shape[axis] = size - shape[axis]
    return jnp.concatenate([value, jnp.zeros(shape, value.dtype)], axis=axis)


class Links:
    def __init__(self, send, recv):
        self.send, self.recv, self.slots, self.open = send, recv, 0, []

    def copy(self, src, dst, device, sends=True, receives=True, after=None):
        slot = self.slots if after is None else after.slot
        self.slots += after is None
        made = Copy(self, slot, src, dst, device, sends, receives)
        self.open.append(made)
        return made

    def retire(self, copies):
        for made in copies:
            made.drain()
            self.open.remove(made)

    def drain(self):
        for made in self.open:
            made.drain()
        assert self.slots == self.send.shape[0], self.slots


class Copy:
    def __init__(self, links, slot, src, dst, device, sends, receives):
        self.made = lambda: pltpu.make_async_remote_copy(
            src_ref=src,
            dst_ref=dst,
            send_sem=links.send.at[slot],
            recv_sem=links.recv.at[slot],
            device_id=device,
            device_id_type=MESH,
        )
        self.slot, self.sends, self.receives = slot, sends, receives

    def start(self):
        when(self.sends, lambda: self.made().start())

    def wait(self):
        when(self.receives, lambda: self.made().wait_recv())

    def drain(self):
        when(self.sends, lambda: self.made().wait_send())


def when(condition, action):
    if condition is True:
        action()
    else:
        pl.when(condition)(action)


def kernel(sizes, latent_hbm, cotangent_hbm, gain_one_hbm, gain_two_hbm, kernel_one, kernel_two, out, latent_grad, *scratch):
    S, Q, Z = sizes
    (
        w_one, w_two, w_gap, act, xp, qs, qr, qn, qp, gs, gr, fs, fr, vall, st, gains,
        xq, gi, gh, gu, gd, qq, yf, rf, ys, yr, yb, rb, g_hop, b_hop, vh, gt, sq, sh, early,
        latent, cotangent, gain_one, gain_two, send, recv, w_sem, seen,
    ) = scratch
    F, R, W, C = latent_hbm.shape
    O = kernel_one.shape[3]
    WW = W * Z
    OP = -(-O // 128) * 128
    rows = F * R * W
    s, q, z = lax.axis_index("section"), lax.axis_index("seq"), lax.axis_index("exp")
    has_next, has_prev = s < S - 1, s > 0
    has_high, has_low = q < Q - 1, q > 0
    both = jnp.logical_and
    nxt, prv = jnp.minimum(s + 1, S - 1), jnp.maximum(s - 1, 0)
    upper, lower = jnp.minimum(q + 1, Q - 1), jnp.maximum(q - 1, 0)
    fold = fold_of(R, O)
    body, own, halo = pl.ds(1, R), pl.ds(0, F), pl.ds(F, 2)
    two = pl.ds(0, 2)
    links = Links(send, recv)

    barrier = pltpu.get_barrier_semaphore()
    loads = [
        pltpu.make_async_copy(src, dst, w_sem.at[k])
        for k, (src, dst) in enumerate(
            [
                (cotangent_hbm, cotangent),
                (latent_hbm, latent),
                (gain_one_hbm, gain_one),
                (gain_two_hbm, gain_two),
                (kernel_two, w_two),
                (kernel_one, w_one),
            ]
        )
    ]
    load_two, load_one = loads[4:]
    for load in loads[:4]:
        load.start()

    def greet(device):
        pl.semaphore_signal(barrier, inc=1, device_id=device, device_id_type=MESH)

    has_right, has_left = z < Z - 1, z > 0
    for beside, step in ((has_right, 1), (has_left, -1)):

        @pl.when(beside)
        def _():
            greet((s, q, z + step))

    for near, step in ((has_next, 1), (has_prev, -1)):

        @pl.when(near)
        def _():
            greet((s + step, q, z))

        for side, move in ((has_high, 1), (has_low, -1)):

            @pl.when(both(near, side))
            def _():
                greet((s + step, q + move, z))

    for side, move in ((has_high, 1), (has_low, -1)):

        @pl.when(side)
        def _():
            greet((s, q + move, z))

    for load in loads[4:]:
        load.start()

    def peer(d):
        return lax.rem(z + d + Z, Z)

    def block(index):
        return pl.ds(pl.multiple_of(index * W, W), W)

    def gather(source, at, reach, after=None):
        arrive = []
        for d in range(1, Z):
            for sign in (1, -1):
                if d <= reach:
                    target, sends = z + sign * d, (z + d < Z) if sign > 0 else (z >= d)
                    src, dst = source, at(z)
                else:
                    target = z + sign
                    held = z - sign * (d - 1)
                    sends = both(z < Z - 1, z >= d - 1) if sign > 0 else both(z > 0, z <= Z - d)
                    src = dst = at(jnp.clip(held, 0, Z - 1))
                receives = (z >= d) if sign > 0 else (z + d < Z)
                target = jnp.clip(target, 0, Z - 1)
                earlier = None if after is None else after[len(arrive)][2]
                arrive.append((d, z - sign * d, links.copy(src, dst, (s, q, target), sends, receives, earlier)))
        return arrive

    def gather_start(arrive, distances):
        for d in distances:
            for distance, _, made in arrive:
                if distance == d:
                    made.start()

    def gather_wait(arrive, d, reach, use=None):
        for distance, owner, made in arrive:
            if distance == d:
                made.wait()
        for distance, owner, made in arrive:
            if distance == d + 1 and d >= reach:
                made.start()
        if use is not None:
            for distance, owner, made in arrive:
                if distance == d:
                    when(made.receives, functools.partial(use, owner))

    class Scatter:
        def __init__(self, at, landing, hop, after=None):
            self.at, self.landing, self.hop, self.far, self.near = at, landing, hop, {}, {}
            for sign in (1, -1):
                for D in range(Z - 1, 0, -1):
                    for f in range(F):
                        target, origin = z + sign * D, z - sign * D
                        sends = (z + D < Z) if sign > 0 else (z >= D)
                        src = at(jnp.clip(target, 0, Z - 1), f)
                        if D >= 3:
                            before = (z >= 1) if sign > 0 else (z < Z - 1)
                            further = (z + D <= Z) if sign > 0 else (z >= D - 1)
                            self.far[sign, D, f] = links.copy(
                                src,
                                hop.at[int(sign > 0), D - 3, f],
                                (s, q, jnp.clip(z + sign, 0, Z - 1)),
                                sends,
                                both(before, further),
                                after and after.far[sign, D, f],
                            )
                        else:
                            receives = (z >= D) if sign > 0 else (z + D < Z)
                            slot = 2 * (sign > 0) + D - 1
                            self.near[sign, D, f] = links.copy(
                                src,
                                landing.at[slot, f],
                                (s, q, jnp.clip(target, 0, Z - 1)),
                                sends,
                                receives,
                                after and after.near[sign, D, f],
                            )

        def copies(self):
            return [*self.far.values(), *self.near.values()]

        def start(self, f, distances):
            for D in distances:
                for sign in (1, -1):
                    made = self.far.get((sign, D, f)) or self.near[sign, D, f]
                    joined = self.far.get((sign, D + 1, f))
                    if joined is None:
                        made.start()
                    else:
                        when(both(made.sends, jnp.logical_not(joined.receives)), lambda: made.made().start())

        def join(self, f):
            for D in range(Z - 1, 2, -1):
                for sign in (1, -1):
                    arrived = self.far[sign, D, f]
                    onward = self.far.get((sign, D - 1, f)) or self.near[sign, D - 1, f]

                    @pl.when(arrived.receives)
                    def _():
                        arrived.made().wait_recv()
                        held = self.at(jnp.clip(z + sign * (D - 1), 0, Z - 1), f)
                        total = held[...].astype(f32) + self.hop[int(sign > 0), D - 3, f].astype(f32)
                        held[...] = total.astype(bf16)
                        onward.made().start()

        def total(self, own):
            for D in (1, 2):
                for sign in (1, -1):
                    for f in range(F):
                        if (sign, D, f) in self.near:
                            self.near[sign, D, f].wait()
            for D in (1, 2):
                for sign in (1, -1):
                    if (sign, D, 0) in self.near:
                        made = self.near[sign, D, 0]
                        term = self.landing[2 * (sign > 0) + D - 1].astype(f32)
                        own = own + jnp.where(made.receives, term, 0.0)
            return own

    q_own = {}
    for d in range(1, Z):
        for sign in (1, -1):
            target = jnp.clip(z + sign * d, 0, Z - 1)
            ends = (z + d < Z, z >= d)
            q_own[sign, d] = links.copy(qs.at[target], qr.at[z], (s, q, target), *ends[::sign])
    q_next = {
        d: links.copy((qr if d else qs).at[peer(-d), two], qn.at[peer(-d)], (prv, q, z), has_prev, has_next)
        for d in range(Z)
    }

    def q_pass_on(sign, d):
        made = q_own[sign, d]
        made.wait()

        @pl.when(made.receives)
        def _():
            q_next[(sign * d) % Z].start()

    def rows_out(src, dst, device, towards, after=None):
        sides = (has_high, has_low) if towards > 0 else (has_low, has_high)
        return links.copy(src, dst, device, *sides, after)

    q_rows = [
        rows_out(qp.at[own, R], qp.at[own, 0], (s, upper, z), 1),
        rows_out(qp.at[own, 1], qp.at[own, R + 1], (s, lower, z), -1),
    ]
    q_corner = [
        links.copy(qp.at[two, R], qp.at[halo, 0], (prv, upper, z), both(has_prev, has_high), both(has_next, has_low)),
        links.copy(qp.at[two, 1], qp.at[halo, R + 1], (prv, lower, z), both(has_prev, has_low), both(has_next, has_high)),
    ]
    x_rows = [
        rows_out(xp.at[:, R], xp.at[:, 0], (s, upper, z), 1),
        rows_out(xp.at[:, 1], xp.at[:, R + 1], (s, lower, z), -1),
    ]
    x_all = gather(act, lambda owner: xp.at[:, body, block(owner)], 2)
    g_out = Scatter(lambda owner, f: gs.at[owner, f], gr, g_hop)
    f_out = [links.copy(fs.at[t], fr.at[t], (nxt, q, z), has_next, has_prev) for t in range(2)]
    v_all = gather(vall.at[z], lambda owner: vall.at[owner], 2, x_all)
    sums = [
        {
            d: links.copy(st.at[k, 0], st.at[k, d], (s, q, peer(d)), True, True, q_own[-1, d] if k else None)
            for d in range(1, Z)
        }
        for k in range(2)
    ]
    xq_rows = [
        rows_out(xq.at[:, :, R], xq.at[:, :, 0], (s, upper, z), 1),
        rows_out(xq.at[:, :, 1], xq.at[:, :, R + 1], (s, lower, z), -1),
    ]
    v_next = links.copy(vall.at[z, two], vh, (prv, q, z), has_prev, has_next, q_corner[0])
    g_next = links.copy(gt, gh, (prv, q, z), has_prev, has_next, q_corner[1])
    squares_next = links.copy(sq, sh.at[Z], (prv, q, z), has_prev, has_next)
    sums_next = {
        d: links.copy(st.at[1, 0], sh.at[d], (prv, q, peer(d)), has_prev, has_next, q_next[d]) for d in range(Z)
    }

    def gi_out(frames, after):
        return [
            rows_out(gi.at[frames, R - 1], gd.at[frames], (s, upper, z), 1, after[0]),
            rows_out(gi.at[frames, 0], gu.at[frames], (s, lower, z), -1, after[1]),
        ]

    gi_rows, gi_corner = gi_out(own, q_rows), gi_out(halo, (None, None))
    b_out = Scatter(lambda owner, f: yb.at[f, :, block(owner)], rb, b_hop, g_out)
    y_own = {
        d: links.copy(yf.at[peer(d)], rf.at[z], (s, q, peer(d)), True, True, q_own[1, d]) for d in range(1, Z)
    }
    y_next = [
        links.copy(ys.at[t], yr.at[t], (nxt, q, z), has_next, has_prev, f_out[t]) for t in range(2)
    ]

    lane = lax.broadcasted_iota(jnp.int32, (8, C), 1)
    group = lax.broadcasted_iota(jnp.int32, (8, C), 0)
    segments = jnp.where(both(lane >= group * O, lane < group * O + O), 1.0, 0.0).astype(f32)

    def pack(value, offset=0):
        count = value.shape[0] // WW
        grouped = value.reshape(count, Z, W, value.shape[1])
        return jnp.concatenate(
            [grouped[:, m].reshape(count * W, value.shape[1])[:, offset : offset + O] for m in range(Z)], axis=1
        )

    def unpack(packed, m):
        return pad_to(packed[:, m * O : (m + 1) * O], 1, OP)

    segments_three = jnp.concatenate([segments] * 3, axis=1).astype(bf16)
    segments_down = jnp.concatenate([segments] * 3, axis=0).astype(bf16)

    def thirds(value, axis):
        high = value.astype(bf16).astype(f32)
        middle = (value - high).astype(bf16).astype(f32)
        return jnp.concatenate([high, middle, value - high - middle], axis=axis).astype(bf16)

    def segment_sums(value):
        return lax.dot_general(
            segments_three, thirds(value, 1), (((1,), (1,)), ((), ())), preferred_element_type=f32
        )

    def spread(tile):
        return lax.dot_general(
            thirds(tile, 0), segments_down, (((0,), (0,)), ((), ())), preferred_element_type=f32
        )

    def rhs_forward(w, taps):
        return jnp.concatenate(
            [
                jnp.concatenate([pad_to(w[i, j, l], 0, OP) for l in range(3) for i in taps], axis=0)
                for j in range(3)
            ],
            axis=1,
        )

    def rhs_backward(w, i):
        return jnp.concatenate(
            [jnp.concatenate([pad_to(w[2 - i, 2 - j, 2 - l], 0, OP) for l in range(3)], axis=1) for j in range(3)],
            axis=0,
        )

    def forward(lhs_of, w):
        parts = {}

        def run(f, taps):
            product = lax.dot_general(
                lhs_of(f), rhs_forward(w, taps), (((1,), (1,)), ((), ())), preferred_element_type=f32
            )
            joined = shift_sum(product, WW, len(taps) * OP)
            for n, i in enumerate(taps):
                parts.setdefault(f + 2 - i, []).append(joined[:, n * OP : n * OP + O])

        def finish(t):
            return functools.reduce(lambda a, b: a + b, parts[t])

        def ahead(t):
            if not parts:
                for f in range(F - 1, max(F - 3, -1), -1):
                    run(f, (0, 1))
            return finish(t)

        def rest(t):
            for f in range(F):
                if f + 2 - 2 == t:
                    run(f, (2,) if f >= F - 2 else (0, 1, 2))
            return finish(t)

        return ahead, rest

    def backward(qbuf, w, f, taps):
        lhs = jnp.concatenate(
            [
                pad_to(qbuf[f + i, pl.ds(j, R)].reshape(R * WW, qbuf.shape[3]), 1, OP)
                for i in taps
                for j in range(3)
            ],
            axis=1,
        )
        rhs = jnp.concatenate([rhs_backward(w, i) for i in taps], axis=0)
        return jnp.dot(lhs, rhs, preferred_element_type=f32)

    def fold_rows(pieces):
        return jnp.concatenate([p.reshape(p.shape[0] * W, O) for p in pieces], axis=1).astype(bf16)

    def unfold_rows(value, width):
        value = value.reshape(value.shape[0] * value.shape[1], W, fold * O).astype(f32)
        parts = [pad_to(value[:, :, k * O : (k + 1) * O], 2, width) for k in range(fold)]
        return jnp.stack(parts, axis=1).reshape(-1, R, W, width)

    loads[0].wait()
    folded = cotangent[...].astype(f32).reshape(F * R // fold, fold, W, C)
    for m in range(Z):
        qs[m] = fold_rows([folded[:, k, :, m * O : (m + 1) * O] for k in range(fold)]).reshape(qs.shape[1:])
    for load in loads[1:4]:
        load.wait()
    source = latent[...].reshape(rows, C).astype(f32)
    g_one, g_two = gain_one[...].reshape(1, C), gain_two[...].reshape(1, C)
    normed_one, _ = normalize(source, g_one)
    act[...] = silu(normed_one).astype(bf16).reshape(F, R, W, C)

    near = has_next.astype(jnp.int32) + has_prev.astype(jnp.int32)
    sides = has_high.astype(jnp.int32) + has_low.astype(jnp.int32)
    beside = has_right.astype(jnp.int32) + has_left.astype(jnp.int32)
    pl.semaphore_wait(barrier, beside + near + sides + near * sides)

    def announce(d):
        for k, known, teller in (
            (0, z + d - 1 < Z, has_left),
            (1, z >= d - 1, has_right),
        ):

            @pl.when(both(known, teller))
            def _():
                pl.semaphore_signal(
                    seen.at[k, d - 2],
                    inc=1,
                    device_id=(s, q, jnp.clip(z - 1 if k == 0 else z + 1, 0, Z - 1)),
                    device_id_type=MESH,
                )

    def await_seen(d):
        for k, known in ((0, z + d < Z), (1, z >= d)):

            @pl.when(known)
            def _():
                pl.semaphore_wait(seen.at[k, d - 2], 1)

    for d in range(1, Z):
        if d > 1:
            await_seen(d)
        if d < Z - 1:
            announce(d + 1)
        for sign in (1, -1):
            q_own[sign, d].start()
    qr[z] = qs[z]
    xp[:, body, block(z)] = act[...]
    q_next[0].start()

    def zero(ref, index):
        ref[index] = jnp.zeros_like(ref[index])

    full = slice(None)

    @pl.when(jnp.logical_not(has_next))
    def _():
        zero(qp, (halo,))
        zero(qq, (halo,))

    for missing, row in ((jnp.logical_not(has_low), 0), (jnp.logical_not(has_high), R + 1)):

        @pl.when(missing)
        def _():
            zero(qp, (full, row))
            zero(qq, (full, row))
            zero(xp, (full, row))
            zero(xq, (full, full, row))

    @pl.when(jnp.logical_not(has_prev))
    def _():
        zero(fr, (full,))
        zero(yr, (full,))

    for m in range(Z):
        gains[m] = jnp.broadcast_to(jnp.concatenate([g_two[:, m * O : (m + 1) * O]] * Z, axis=1), (8, C))

    load_two.wait()
    for i in range(3):
        for j in range(3):
            for l in range(3):
                w = w_two[i, j, l].astype(f32)
                w_gap[i, j, l] = jnp.concatenate(
                    [pad_to(w[:, m * O : (m + 1) * O], 1, OP) for m in range(Z)], axis=1
                ).astype(bf16)
    gather_start(x_all, (2, 1))
    for d in range(1, Z):
        for sign in (1, -1):
            q_pass_on(sign, d)
    for m in range(Z):
        qp[own, body, m * W : (m + 1) * W] = unfold_rows(qr[m], OP).astype(bf16)
    for made in q_rows + q_corner:
        made.start()
    for made in q_rows:
        made.wait()
    for f in range(F):
        early[f] = backward(qp, w_two, f, range(F - f))
    for d in range(Z):
        q_next[d].wait()

    @pl.when(has_next)
    def _():
        for m in range(Z):
            qp[halo, body, m * W : (m + 1) * W] = unfold_rows(qn[m], OP).astype(bf16)

    for made in q_corner:
        made.wait()
    for f in range(F):
        total = early[f] + backward(qp, w_two, f, range(F - f, 3))
        total = shift_sum(total, WW, C)
        if f == 0:
            gather_wait(x_all, 2, 2)
        for m in range(Z):
            gs[m, f] = pack(total, m * O).astype(bf16).reshape(R, W, C)
        g_out.start(f, range(Z - 1, 1, -1))
    for f in range(F):
        g_out.start(f, (1,))

    gather_wait(x_all, 1, 2)
    for d in range(3, Z):
        gather_wait(x_all, d, 2)
    for made in x_rows:
        made.start()
    load_one.wait()
    for made in x_rows:
        made.wait()

    def lhs_one(f):
        return jnp.concatenate([xp[f, pl.ds(j, R)].reshape(R * WW, C) for j in range(3)], axis=1)

    ahead, inner = forward(lhs_one, w_one)
    for t in (F + 1, F):
        fs[t - F] = pack(ahead(t)).astype(bf16).reshape(R, W, C)
        f_out[t - F].start()
    rest, inner = inner, []
    for t in range(F):
        g_out.join(t)
        inner.append(pack(rest(t)))
    for made in f_out:
        made.wait()
    for t in range(2):
        inner[t] = inner[t] + fr[t].reshape(R * W, C).astype(f32)
    inner = jnp.concatenate(inner, axis=0)
    vall[z] = inner.astype(bf16).reshape(F, R, W, C)
    st[0, 0] = segment_sums(inner * inner)
    for d in range(1, Z):
        sums[0][d].start()

    links.retire([*q_own.values(), *q_next.values(), *q_corner])
    v_next.start()
    grad_two = g_out.total(gs[z].astype(f32)).reshape(rows, C)
    gt[...] = grad_two[: 2 * R * W].astype(bf16).reshape(2, R, W, C)
    g_next.start()
    links.retire([made for _, _, made in x_all])
    gather_start(v_all, (2,))
    squares = st[0, 0]
    for d in range(1, Z):
        sums[0][d].wait()
        squares = squares + st[0, d]
    sq[...] = squares
    squares_next.start()
    inverse = lax.rsqrt(squares / C + epsilon)
    inverse_wide = spread(inverse)
    gain = gains[z][0:1]
    scaled = grad_two * silu_slope(inner * inverse_wide * gain) * gain
    st[1, 0] = segment_sums(inner * scaled)
    for d in range(1, Z):
        sums[1][d].start()
    for d in range(Z):
        sums_next[d].start()

    def activate(owner):
        value = vall[owner].reshape(rows, C).astype(f32)
        active = silu(value * inverse_wide * gains[owner][0:1])
        for m in range(Z):
            xq[owner, :, body, m * W : (m + 1) * W] = unpack(active, m).astype(bf16).reshape(F, R, W, OP)

    gather_start(v_all, (1,))
    activate(z)

    links.retire([*f_out, *q_rows, *g_out.copies()])
    means = st[1, 0]
    for d in range(1, Z):
        sums[1][d].wait()
        means = means + st[1, d]
    factor = spread(inverse * inverse * inverse * means / C)
    grad_inner = (inverse_wide * scaled - inner * factor).astype(bf16)
    gi[own] = grad_inner.reshape(F, R, W, C)
    for made in gi_rows:
        made.start()

    def place(ref, frames, band, count):
        value = ref.reshape(count, C).astype(f32)
        for m in range(Z):
            piece = unpack(value, m).astype(bf16)
            qq[frames, band, m * W : (m + 1) * W] = piece.reshape(
                qq.at[frames, band, m * W : (m + 1) * W].shape
            )

    place(gi[own], own, body, rows)
    gather_wait(v_all, 2, 2, activate)

    def place_rows(frames, count, among):
        for side, ref, row in ((has_low, gd, 0), (has_high, gu, R + 1)):

            @pl.when(side if among is None else both(side, among))
            def _():
                place(ref[frames], frames, row, count * W)

    for made in (v_next, g_next, squares_next):
        made.wait()
    for d in range(Z):
        sums_next[d].wait()

    @pl.when(has_next)
    def _():
        taken = slice(0, 2 * R * W)
        inverse = lax.rsqrt(sh[Z] / C + epsilon)
        mean = sh[0]
        for d in range(1, Z):
            mean = mean + sh[d]
        value = vh[...].reshape(2 * R * W, C).astype(f32)
        inverse_wide = spread(inverse)[taken]
        upstream = gh[...].reshape(2 * R * W, C).astype(f32)
        upstream = upstream * silu_slope(value * inverse_wide * gain) * gain
        factor = spread(inverse * inverse * inverse * mean / C)[taken]
        gi[halo] = (inverse_wide * upstream - value * factor).astype(bf16).reshape(2, R, W, C)
        place(gi[halo], halo, body, 2 * R * W)

    @pl.when(jnp.logical_not(has_next))
    def _():
        zero(gi, (halo,))

    for made in gi_corner:
        made.start()
    for made in gi_rows:
        made.wait()
    place_rows(own, F, None)
    for f in range(F):
        early[f] = backward(qq, w_one, f, range(F - f))
    for made in gi_corner:
        made.wait()
    place_rows(halo, 2, has_next)
    for f in range(F):
        total = early[f] + backward(qq, w_one, f, range(F - f, 3))
        yb[f] = shift_sum(total, WW, C).astype(bf16).reshape(R, WW, C)
        b_out.start(f, range(Z - 1, 2, -1))
        if f == 0:
            gather_wait(v_all, 1, 2, activate)
            for d in range(3, Z):
                gather_wait(v_all, d, 2, activate)
            for made in xq_rows:
                made.start()
    for d in (2, 1):
        for f in range(F):
            b_out.start(f, (d,))

    def lhs_two(f):
        return jnp.concatenate(
            [xq[m, f, pl.ds(j, R)].reshape(R * WW, OP) for j in range(3) for m in range(Z)], axis=1
        )

    for made in xq_rows:
        made.wait()
    ahead, branch = forward(lhs_two, w_gap)
    for t in (F + 1, F):
        ys[t - F] = pack(ahead(t)).astype(bf16).reshape(R, W, C)
        y_next[t - F].start()
    rest, branch = branch, []
    for t in range(F):
        b_out.join(t)
        branch.append(rest(t).reshape(R, Z, W, O))
    for made in y_next:
        made.wait()
    for t in range(F):
        for m in range(Z):
            term = branch[t][:, m].reshape(R // fold, fold, W, O)
            if t < 2:
                carried = yr[t].reshape(R * W, C).astype(f32)[:, m * O : (m + 1) * O]
                term = term + carried.reshape(R // fold, fold, W, O)
            yf[m, t] = fold_rows([term[:, k] for k in range(fold)]).reshape(R // fold, W, fold * O)
    for d in sorted(range(1, Z), key=lambda d: -abs(2 * d - Z)):
        y_own[d].start()
    rf[z] = yf[z]

    source = latent[...].reshape(rows, C).astype(f32)
    normed_one, inverse_one = normalize(source, g_one)
    slope_one = silu_slope(normed_one)
    upstream = cotangent[...].reshape(rows, C).astype(f32)
    grad_one = b_out.total(yb[:, :, block(z)].astype(f32)).reshape(rows, C)
    grad = norm_backward(source, inverse_one, g_one, grad_one * slope_one)
    latent_grad[...] = (upstream + grad).astype(bf16).reshape(F, R, W, C)
    for d in range(1, Z):
        y_own[d].wait()
    branch = jnp.concatenate([unfold_rows(rf[m], O).reshape(rows, O) for m in range(Z)], axis=1)
    out[...] = (source + branch).astype(bf16).reshape(F, R, W, C)
    links.drain()


def hand_over(first, second, first_out, second_out, sem):
    copies = [
        pltpu.make_async_copy(first, first_out, sem.at[0]),
        pltpu.make_async_copy(second, second_out, sem.at[1]),
    ]
    for made in copies:
        made.start()
    for made in copies:
        made.wait()


def local(sizes, latent, cotangent, gain_one, gain_two, kernel_one, kernel_two):
    S, Q, Z = sizes
    F, R, W, C = latent.shape
    O = kernel_one.shape[3]
    WW = W * Z
    OP = -(-O // 128) * 128
    rows = F * R * W
    taps = kernel_one.shape[:3]
    fold = fold_of(R, O)
    packed = (F, R, W, C)
    slots = (Z - 1) * (5 + 2 * F) + Z + 13
    shapes = [
        kernel_one.shape,
        kernel_two.shape,
        taps + (O, Z * OP),
        packed,
        (F, R + 2, WW, C),
        (Z, F, R // fold, W, fold * O),
        (Z, F, R // fold, W, fold * O),
        (Z, 2, R // fold, W, fold * O),
        (F + 2, R + 2, WW, OP),
        (Z,) + packed,
        (4,) + packed,
        (2, R, W, C),
        (2, R, W, C),
        (Z,) + packed,
        None,
        None,
        (Z, F, R + 2, WW, OP),
        (F + 2, R, W, C),
        (2, R, W, C),
        (F + 2, W, C),
        (F + 2, W, C),
        (F + 2, R + 2, WW, OP),
        (Z, F, R // fold, W, fold * O),
        (Z, F, R // fold, W, fold * O),
        (2, R, W, C),
        (2, R, W, C),
        (F, R, WW, C),
        (4,) + packed,
        (2, max(Z - 3, 1)) + packed,
        (2, max(Z - 3, 1)) + packed,
        (2, R, W, C),
        (2, R, W, C),
        None,
        None,
        None,
        packed,
        packed,
        None,
        None,
    ]
    scratch = [pltpu.VMEM(shape, bf16) if shape else None for shape in shapes]
    scratch[14] = pltpu.VMEM((2, Z, 8, rows), f32)
    scratch[15] = pltpu.VMEM((Z, 8, C), f32)
    scratch[32] = pltpu.VMEM((8, rows), f32)
    scratch[33] = pltpu.VMEM((Z + 1, 8, rows), f32)
    scratch[34] = pltpu.VMEM((F, R * WW, 3 * C), f32)
    scratch[37] = scratch[38] = pltpu.VMEM((C,), f32)
    hbm = pl.BlockSpec(memory_space=pltpu.HBM)
    results = pl.pallas_call(
        functools.partial(kernel, sizes),
        out_shape=[jax.ShapeDtypeStruct((F, R, W, C), bf16)] * 2,
        in_specs=[hbm] * 6,
        out_specs=[pl.BlockSpec(memory_space=pltpu.VMEM)] * 2,
        scratch_shapes=[
            *scratch,
            pltpu.SemaphoreType.DMA((slots,)),
            pltpu.SemaphoreType.DMA((slots,)),
            pltpu.SemaphoreType.DMA((6,)),
            pltpu.SemaphoreType.REGULAR((2, max(Z - 2, 1))),
        ],
        compiler_params=pltpu.CompilerParams(
            collective_id=0, has_side_effects=True, vmem_limit_bytes=28 * 1024 * 1024
        ),
    )(*[pltpu.with_memory_space_constraint(a, pltpu.HBM) for a in (latent, cotangent, gain_one, gain_two, kernel_one, kernel_two)])
    vmem = pl.BlockSpec(memory_space=pltpu.VMEM)
    return pl.pallas_call(
        hand_over,
        out_shape=[jax.ShapeDtypeStruct((F, R, W, C), bf16)] * 2,
        in_specs=[vmem] * 2,
        out_specs=[hbm] * 2,
        scratch_shapes=[pltpu.SemaphoreType.DMA((2,))],
    )(*[pltpu.with_memory_space_constraint(a, pltpu.VMEM) for a in results])

def solution(mesh):
    sizes = (mesh.shape["section"], mesh.shape["seq"], mesh.shape["exp"])
    spread = P("section", "seq", "exp", None)
    split = P(None, None, None, "exp", None)
    return jax.shard_map(
        functools.partial(local, sizes),
        mesh=mesh,
        in_specs=(spread, spread, P(), P(), split, split),
        out_specs=(spread, spread),
        check_vma=False,
    )
```

```python
import functools

import jax
import jax.numpy as jnp
from jax import lax
from jax.experimental import pallas as pl
from jax.experimental.pallas import tpu as pltpu
from jax.sharding import PartitionSpec as P

epsilon = 1e-06
MESH = pl.DeviceIdType.MESH
bf16, f32 = jnp.bfloat16, jnp.float32


def normalize(values, gain):
    inverse = lax.rsqrt(jnp.mean(values * values, axis=-1, keepdims=True) + epsilon)
    return values * inverse * gain, inverse


def norm_backward(values, inverse, gain, upstream):
    scaled = upstream * gain
    mean = jnp.mean(values * scaled, axis=-1, keepdims=True)
    return inverse * scaled - values * (inverse * inverse * inverse) * mean


def silu(normed):
    return normed / (1.0 + jnp.exp(-normed))


def silu_slope(normed):
    sigma = 1.0 / (1.0 + jnp.exp(-normed))
    return sigma * (1.0 + normed * (1.0 - sigma))


def shift_sum(taps, width, size):
    rows = taps.shape[0]
    column = lax.rem(lax.broadcasted_iota(jnp.int32, (rows, size), 0), width)
    low = pltpu.roll(taps[:, :size], 1, axis=0)
    high = pltpu.roll(taps[:, 2 * size :], rows - 1, axis=0)
    return (
        taps[:, size : 2 * size]
        + jnp.where(column == 0, 0.0, low)
        + jnp.where(column == width - 1, 0.0, high)
    )


def fold_of(rows, width):
    return next((n for n in (4, 2) if rows % n == 0 and n * width % 128 == 0), 1)


def pad_to(value, axis, size):
    shape = list(value.shape)
    if shape[axis] == size:
        return value
    shape[axis] = size - shape[axis]
    return jnp.concatenate([value, jnp.zeros(shape, value.dtype)], axis=axis)


class Links:
    def __init__(self, send, recv):
        self.send, self.recv, self.slots, self.open = send, recv, 0, []

    def copy(self, src, dst, device, sends=True, receives=True, after=None):
        slot = self.slots if after is None else after.slot
        self.slots += after is None
        made = Copy(self, slot, src, dst, device, sends, receives)
        self.open.append(made)
        return made

    def retire(self, copies):
        for made in copies:
            made.drain()
            self.open.remove(made)

    def drain(self):
        for made in self.open:
            made.drain()
        assert self.slots == self.send.shape[0], self.slots


class Copy:
    def __init__(self, links, slot, src, dst, device, sends, receives):
        self.made = lambda: pltpu.make_async_remote_copy(
            src_ref=src,
            dst_ref=dst,
            send_sem=links.send.at[slot],
            recv_sem=links.recv.at[slot],
            device_id=device,
            device_id_type=MESH,
        )
        self.slot, self.sends, self.receives = slot, sends, receives

    def start(self):
        when(self.sends, lambda: self.made().start())

    def wait(self):
        when(self.receives, lambda: self.made().wait_recv())

    def drain(self):
        when(self.sends, lambda: self.made().wait_send())


def when(condition, action):
    if condition is True:
        action()
    else:
        pl.when(condition)(action)


def kernel(sizes, latent_hbm, cotangent_hbm, gain_one_hbm, gain_two_hbm, kernel_one, kernel_two, out, latent_grad, *scratch):
    S, Q, Z = sizes
    (
        w_one, w_two, w_gap, act, xp, qs, qr, qn, qp, gs, gr, fs, fr, vall, st, gains,
        xq, gi, gh, gu, gd, qq, yf, rf, ys, yr, yb, rb, g_hop, b_hop, vh, gt, sq, sh, early,
        latent, cotangent, gain_one, gain_two, send, recv, w_sem, seen,
    ) = scratch
    F, R, W, C = latent_hbm.shape
    O = kernel_one.shape[3]
    WW = W * Z
    OP = -(-O // 128) * 128
    rows = F * R * W
    s, q, z = lax.axis_index("section"), lax.axis_index("seq"), lax.axis_index("exp")
    has_next, has_prev = s < S - 1, s > 0
    has_high, has_low = q < Q - 1, q > 0
    both = jnp.logical_and
    nxt, prv = jnp.minimum(s + 1, S - 1), jnp.maximum(s - 1, 0)
    upper, lower = jnp.minimum(q + 1, Q - 1), jnp.maximum(q - 1, 0)
    fold = fold_of(R, O)
    body, own, halo = pl.ds(1, R), pl.ds(0, F), pl.ds(F, 2)
    two = pl.ds(0, 2)
    links = Links(send, recv)

    barrier = pltpu.get_barrier_semaphore()
    loads = [
        pltpu.make_async_copy(src, dst, w_sem.at[k])
        for k, (src, dst) in enumerate(
            [
                (cotangent_hbm, cotangent),
                (latent_hbm, latent),
                (gain_one_hbm, gain_one),
                (gain_two_hbm, gain_two),
                (kernel_two, w_two),
                (kernel_one, w_one),
            ]
        )
    ]
    load_two, load_one = loads[4:]
    for load in loads[:4]:
        load.start()

    def greet(device):
        pl.semaphore_signal(barrier, inc=1, device_id=device, device_id_type=MESH)

    has_right, has_left = z < Z - 1, z > 0
    for beside, step in ((has_right, 1), (has_left, -1)):

        @pl.when(beside)
        def _():
            greet((s, q, z + step))

    for near, step in ((has_next, 1), (has_prev, -1)):

        @pl.when(near)
        def _():
            greet((s + step, q, z))

        for side, move in ((has_high, 1), (has_low, -1)):

            @pl.when(both(near, side))
            def _():
                greet((s + step, q + move, z))

    for side, move in ((has_high, 1), (has_low, -1)):

        @pl.when(side)
        def _():
            greet((s, q + move, z))

    for load in loads[4:]:
        load.start()

    def peer(d):
        return lax.rem(z + d + Z, Z)

    def block(index):
        return pl.ds(pl.multiple_of(index * W, W), W)

    def gather(source, at, reach, after=None):
        arrive = []
        for d in range(1, Z):
            for sign in (1, -1):
                if d <= reach:
                    target, sends = z + sign * d, (z + d < Z) if sign > 0 else (z >= d)
                    src, dst = source, at(z)
                else:
                    target = z + sign
                    held = z - sign * (d - 1)
                    sends = both(z < Z - 1, z >= d - 1) if sign > 0 else both(z > 0, z <= Z - d)
                    src = dst = at(jnp.clip(held, 0, Z - 1))
                receives = (z >= d) if sign > 0 else (z + d < Z)
                target = jnp.clip(target, 0, Z - 1)
                earlier = None if after is None else after[len(arrive)][2]
                arrive.append((d, z - sign * d, links.copy(src, dst, (s, q, target), sends, receives, earlier)))
        return arrive

    def gather_start(arrive, distances):
        for d in distances:
            for distance, _, made in arrive:
                if distance == d:
                    made.start()

    def gather_wait(arrive, d, reach, use=None):
        for distance, owner, made in arrive:
            if distance == d:
                made.wait()
        for distance, owner, made in arrive:
            if distance == d + 1 and d >= reach:
                made.start()
        if use is not None:
            for distance, owner, made in arrive:
                if distance == d:
                    when(made.receives, functools.partial(use, owner))

    class Scatter:
        def __init__(self, at, landing, hop, after=None):
            self.at, self.landing, self.hop, self.far, self.near = at, landing, hop, {}, {}
            for sign in (1, -1):
                for D in range(Z - 1, 0, -1):
                    for f in range(F):
                        target, origin = z + sign * D, z - sign * D
                        sends = (z + D < Z) if sign > 0 else (z >= D)
                        src = at(jnp.clip(target, 0, Z - 1), f)
                        if D >= 3:
                            before = (z >= 1) if sign > 0 else (z < Z - 1)
                            further = (z + D <= Z) if sign > 0 else (z >= D - 1)
                            self.far[sign, D, f] = links.copy(
                                src,
                                hop.at[int(sign > 0), D - 3, f],
                                (s, q, jnp.clip(z + sign, 0, Z - 1)),
                                sends,
                                both(before, further),
                                after and after.far[sign, D, f],
                            )
                        else:
                            receives = (z >= D) if sign > 0 else (z + D < Z)
                            slot = 2 * (sign > 0) + D - 1
                            self.near[sign, D, f] = links.copy(
                                src,
                                landing.at[slot, f],
                                (s, q, jnp.clip(target, 0, Z - 1)),
                                sends,
                                receives,
                                after and after.near[sign, D, f],
                            )

        def copies(self):
            return [*self.far.values(), *self.near.values()]

        def start(self, f, distances):
            for D in distances:
                for sign in (1, -1):
                    made = self.far.get((sign, D, f)) or self.near[sign, D, f]
                    joined = self.far.get((sign, D + 1, f))
                    if joined is None:
                        made.start()
                    else:
                        when(both(made.sends, jnp.logical_not(joined.receives)), lambda: made.made().start())

        def join(self, f):
            for D in range(Z - 1, 2, -1):
                for sign in (1, -1):
                    arrived = self.far[sign, D, f]
                    onward = self.far.get((sign, D - 1, f)) or self.near[sign, D - 1, f]

                    @pl.when(arrived.receives)
                    def _():
                        arrived.made().wait_recv()
                        held = self.at(jnp.clip(z + sign * (D - 1), 0, Z - 1), f)
                        total = held[...].astype(f32) + self.hop[int(sign > 0), D - 3, f].astype(f32)
                        held[...] = total.astype(bf16)
                        onward.made().start()

        def total(self, own):
            for D in (1, 2):
                for sign in (1, -1):
                    for f in range(F):
                        if (sign, D, f) in self.near:
                            self.near[sign, D, f].wait()
            for D in (1, 2):
                for sign in (1, -1):
                    if (sign, D, 0) in self.near:
                        made = self.near[sign, D, 0]
                        term = self.landing[2 * (sign > 0) + D - 1].astype(f32)
                        own = own + jnp.where(made.receives, term, 0.0)
            return own

    q_own = {}
    for d in range(1, Z):
        for sign in (1, -1):
            target = jnp.clip(z + sign * d, 0, Z - 1)
            ends = (z + d < Z, z >= d)
            q_own[sign, d] = links.copy(qs.at[target], qr.at[z], (s, q, target), *ends[::sign])
    q_next = {
        d: links.copy((qr if d else qs).at[peer(-d), two], qn.at[peer(-d)], (prv, q, z), has_prev, has_next)
        for d in range(Z)
    }

    def q_pass_on(sign, d):
        made = q_own[sign, d]
        made.wait()

        @pl.when(made.receives)
        def _():
            q_next[(sign * d) % Z].start()

    def rows_out(src, dst, device, towards, after=None):
        sides = (has_high, has_low) if towards > 0 else (has_low, has_high)
        return links.copy(src, dst, device, *sides, after)

    q_rows = [
        rows_out(qp.at[own, R], qp.at[own, 0], (s, upper, z), 1),
        rows_out(qp.at[own, 1], qp.at[own, R + 1], (s, lower, z), -1),
    ]
    q_corner = [
        links.copy(qp.at[two, R], qp.at[halo, 0], (prv, upper, z), both(has_prev, has_high), both(has_next, has_low)),
        links.copy(qp.at[two, 1], qp.at[halo, R + 1], (prv, lower, z), both(has_prev, has_low), both(has_next, has_high)),
    ]
    x_rows = [
        rows_out(xp.at[:, R], xp.at[:, 0], (s, upper, z), 1),
        rows_out(xp.at[:, 1], xp.at[:, R + 1], (s, lower, z), -1),
    ]
    x_all = gather(act, lambda owner: xp.at[:, body, block(owner)], 2)
    g_out = Scatter(lambda owner, f: gs.at[owner, f], gr, g_hop)
    f_out = [links.copy(fs.at[t], fr.at[t], (nxt, q, z), has_next, has_prev) for t in range(2)]
    v_all = gather(vall.at[z], lambda owner: vall.at[owner], 2, x_all)
    sums = [
        {
            d: links.copy(st.at[k, 0], st.at[k, d], (s, q, peer(d)), True, True, q_own[-1, d] if k else None)
            for d in range(1, Z)
        }
        for k in range(2)
    ]
    xq_rows = [
        rows_out(xq.at[:, :, R], xq.at[:, :, 0], (s, upper, z), 1),
        rows_out(xq.at[:, :, 1], xq.at[:, :, R + 1], (s, lower, z), -1),
    ]
    v_next = links.copy(vall.at[z, two], vh, (prv, q, z), has_prev, has_next, q_corner[0])
    g_next = links.copy(gt, gh, (prv, q, z), has_prev, has_next, q_corner[1])
    squares_next = links.copy(sq, sh.at[Z], (prv, q, z), has_prev, has_next)
    sums_next = {
        d: links.copy(st.at[1, 0], sh.at[d], (prv, q, peer(d)), has_prev, has_next, q_next[d]) for d in range(Z)
    }

    def gi_out(frames, after):
        return [
            rows_out(gi.at[frames, R - 1], gd.at[frames], (s, upper, z), 1, after[0]),
            rows_out(gi.at[frames, 0], gu.at[frames], (s, lower, z), -1, after[1]),
        ]

    gi_rows, gi_corner = gi_out(own, q_rows), gi_out(halo, (None, None))
    b_out = Scatter(lambda owner, f: yb.at[f, :, block(owner)], rb, b_hop, g_out)
    y_own = {
        d: links.copy(yf.at[peer(d)], rf.at[z], (s, q, peer(d)), True, True, q_own[1, d]) for d in range(1, Z)
    }
    y_next = [
        links.copy(ys.at[t], yr.at[t], (nxt, q, z), has_next, has_prev, f_out[t]) for t in range(2)
    ]

    lane = lax.broadcasted_iota(jnp.int32, (8, C), 1)
    group = lax.broadcasted_iota(jnp.int32, (8, C), 0)
    segments = jnp.where(both(lane >= group * O, lane < group * O + O), 1.0, 0.0).astype(f32)

    def pack(value, offset=0):
        count = value.shape[0] // WW
        grouped = value.reshape(count, Z, W, value.shape[1])
        return jnp.concatenate(
            [grouped[:, m].reshape(count * W, value.shape[1])[:, offset : offset + O] for m in range(Z)], axis=1
        )

    def unpack(packed, m):
        return pad_to(packed[:, m * O : (m + 1) * O], 1, OP)

    segments_three = jnp.concatenate([segments] * 3, axis=1).astype(bf16)
    segments_down = jnp.concatenate([segments] * 3, axis=0).astype(bf16)

    def thirds(value, axis):
        high = value.astype(bf16).astype(f32)
        middle = (value - high).astype(bf16).astype(f32)
        return jnp.concatenate([high, middle, value - high - middle], axis=axis).astype(bf16)

    def segment_sums(value):
        return lax.dot_general(
            segments_three, thirds(value, 1), (((1,), (1,)), ((), ())), preferred_element_type=f32
        )

    def spread(tile):
        return lax.dot_general(
            thirds(tile, 0), segments_down, (((0,), (0,)), ((), ())), preferred_element_type=f32
        )

    def rhs_forward(w, taps):
        return jnp.concatenate(
            [
                jnp.concatenate([pad_to(w[i, j, l], 0, OP) for l in range(3) for i in taps], axis=0)
                for j in range(3)
            ],
            axis=1,
        )

    def rhs_backward(w, i):
        return jnp.concatenate(
            [jnp.concatenate([pad_to(w[2 - i, 2 - j, 2 - l], 0, OP) for l in range(3)], axis=1) for j in range(3)],
            axis=0,
        )

    def forward(lhs_of, w):
        parts = {}

        def run(f, taps):
            product = lax.dot_general(
                lhs_of(f), rhs_forward(w, taps), (((1,), (1,)), ((), ())), preferred_element_type=f32
            )
            joined = shift_sum(product, WW, len(taps) * OP)
            for n, i in enumerate(taps):
                parts.setdefault(f + 2 - i, []).append(joined[:, n * OP : n * OP + O])

        def finish(t):
            return functools.reduce(lambda a, b: a + b, parts[t])

        def ahead(t):
            run(t - 2, (0, 1))
            return finish(t)

        def rest(t):
            for f in range(F):
                if f + 2 - 2 == t:
                    run(f, (2,) if f >= F - 2 else (0, 1, 2))
            return finish(t)

        return ahead, rest

    def backward(qbuf, w, f, taps):
        lhs = jnp.concatenate(
            [
                pad_to(qbuf[f + i, pl.ds(j, R)].reshape(R * WW, qbuf.shape[3]), 1, OP)
                for i in taps
                for j in range(3)
            ],
            axis=1,
        )
        rhs = jnp.concatenate([rhs_backward(w, i) for i in taps], axis=0)
        return jnp.dot(lhs, rhs, preferred_element_type=f32)

    def fold_rows(pieces):
        return jnp.concatenate([p.reshape(p.shape[0] * W, O) for p in pieces], axis=1).astype(bf16)

    def unfold_rows(value, width):
        value = value.reshape(value.shape[0] * value.shape[1], W, fold * O).astype(f32)
        parts = [pad_to(value[:, :, k * O : (k + 1) * O], 2, width) for k in range(fold)]
        return jnp.stack(parts, axis=1).reshape(-1, R, W, width)

    loads[0].wait()
    folded = cotangent[...].astype(f32).reshape(F * R // fold, fold, W, C)
    for m in range(Z):
        qs[m] = fold_rows([folded[:, k, :, m * O : (m + 1) * O] for k in range(fold)]).reshape(qs.shape[1:])
    for load in loads[1:4]:
        load.wait()
    source = latent[...].reshape(rows, C).astype(f32)
    g_one, g_two = gain_one[...].reshape(1, C), gain_two[...].reshape(1, C)
    normed_one, _ = normalize(source, g_one)
    act[...] = silu(normed_one).astype(bf16).reshape(F, R, W, C)

    near = has_next.astype(jnp.int32) + has_prev.astype(jnp.int32)
    sides = has_high.astype(jnp.int32) + has_low.astype(jnp.int32)
    beside = has_right.astype(jnp.int32) + has_left.astype(jnp.int32)
    pl.semaphore_wait(barrier, beside + near + sides + near * sides)

    def announce(d):
        for k, known, teller in (
            (0, z + d - 1 < Z, has_left),
            (1, z >= d - 1, has_right),
        ):

            @pl.when(both(known, teller))
            def _():
                pl.semaphore_signal(
                    seen.at[k, d - 2],
                    inc=1,
                    device_id=(s, q, jnp.clip(z - 1 if k == 0 else z + 1, 0, Z - 1)),
                    device_id_type=MESH,
                )

    def await_seen(d):
        for k, known in ((0, z + d < Z), (1, z >= d)):

            @pl.when(known)
            def _():
                pl.semaphore_wait(seen.at[k, d - 2], 1)

    for d in range(1, Z):
        if d > 1:
            await_seen(d)
        if d < Z - 1:
            announce(d + 1)
        for sign in (1, -1):
            q_own[sign, d].start()
    qr[z] = qs[z]
    xp[:, body, block(z)] = act[...]
    q_next[0].start()

    def zero(ref, index):
        ref[index] = jnp.zeros_like(ref[index])

    full = slice(None)

    @pl.when(jnp.logical_not(has_next))
    def _():
        zero(qp, (halo,))
        zero(qq, (halo,))

    for missing, row in ((jnp.logical_not(has_low), 0), (jnp.logical_not(has_high), R + 1)):

        @pl.when(missing)
        def _():
            zero(qp, (full, row))
            zero(qq, (full, row))
            zero(xp, (full, row))
            zero(xq, (full, full, row))

    @pl.when(jnp.logical_not(has_prev))
    def _():
        zero(fr, (full,))
        zero(yr, (full,))

    for m in range(Z):
        gains[m] = jnp.broadcast_to(jnp.concatenate([g_two[:, m * O : (m + 1) * O]] * Z, axis=1), (8, C))

    load_two.wait()
    for i in range(3):
        for j in range(3):
            for l in range(3):
                w = w_two[i, j, l].astype(f32)
                w_gap[i, j, l] = jnp.concatenate(
                    [pad_to(w[:, m * O : (m + 1) * O], 1, OP) for m in range(Z)], axis=1
                ).astype(bf16)
    gather_start(x_all, (2, 1))
    for d in range(1, Z):
        for sign in (1, -1):
            q_pass_on(sign, d)
    for m in range(Z):
        qp[own, body, m * W : (m + 1) * W] = unfold_rows(qr[m], OP).astype(bf16)
    for made in q_rows + q_corner:
        made.start()
    for made in q_rows:
        made.wait()
    for f in range(F):
        early[f] = backward(qp, w_two, f, range(F - f))
    for d in range(Z):
        q_next[d].wait()

    @pl.when(has_next)
    def _():
        for m in range(Z):
            qp[halo, body, m * W : (m + 1) * W] = unfold_rows(qn[m], OP).astype(bf16)

    for made in q_corner:
        made.wait()
    for f in range(F):
        total = early[f] + backward(qp, w_two, f, range(F - f, 3))
        total = shift_sum(total, WW, C)
        if f == 0:
            gather_wait(x_all, 2, 2)
        for m in range(Z):
            gs[m, f] = pack(total, m * O).astype(bf16).reshape(R, W, C)
        g_out.start(f, range(Z - 1, 1, -1))
    for f in range(F):
        g_out.start(f, (1,))

    gather_wait(x_all, 1, 2)
    for d in range(3, Z):
        gather_wait(x_all, d, 2)
    for made in x_rows:
        made.start()
    load_one.wait()
    for made in x_rows:
        made.wait()

    def lhs_one(f):
        return jnp.concatenate([xp[f, pl.ds(j, R)].reshape(R * WW, C) for j in range(3)], axis=1)

    ahead, inner = forward(lhs_one, w_one)
    for t in (F + 1, F):
        fs[t - F] = pack(ahead(t)).astype(bf16).reshape(R, W, C)
        f_out[t - F].start()
    rest, inner = inner, []
    for t in range(F):
        g_out.join(t)
        inner.append(pack(rest(t)))
    for made in f_out:
        made.wait()
    for t in range(2):
        inner[t] = inner[t] + fr[t].reshape(R * W, C).astype(f32)
    inner = jnp.concatenate(inner, axis=0)
    vall[z] = inner.astype(bf16).reshape(F, R, W, C)
    st[0, 0] = segment_sums(inner * inner)
    for d in range(1, Z):
        sums[0][d].start()

    links.retire([*q_own.values(), *q_next.values(), *q_corner])
    v_next.start()
    grad_two = g_out.total(gs[z].astype(f32)).reshape(rows, C)
    gt[...] = grad_two[: 2 * R * W].astype(bf16).reshape(2, R, W, C)
    g_next.start()
    links.retire([made for _, _, made in x_all])
    gather_start(v_all, (2,))
    squares = st[0, 0]
    for d in range(1, Z):
        sums[0][d].wait()
        squares = squares + st[0, d]
    sq[...] = squares
    squares_next.start()
    inverse = lax.rsqrt(squares / C + epsilon)
    inverse_wide = spread(inverse)
    gain = gains[z][0:1]
    scaled = grad_two * silu_slope(inner * inverse_wide * gain) * gain
    st[1, 0] = segment_sums(inner * scaled)
    for d in range(1, Z):
        sums[1][d].start()
    for d in range(Z):
        sums_next[d].start()

    def activate(owner):
        value = vall[owner].reshape(rows, C).astype(f32)
        active = silu(value * inverse_wide * gains[owner][0:1])
        for m in range(Z):
            xq[owner, :, body, m * W : (m + 1) * W] = unpack(active, m).astype(bf16).reshape(F, R, W, OP)

    gather_start(v_all, (1,))
    activate(z)

    links.retire([*f_out, *q_rows, *g_out.copies()])
    means = st[1, 0]
    for d in range(1, Z):
        sums[1][d].wait()
        means = means + st[1, d]
    factor = spread(inverse * inverse * inverse * means / C)
    grad_inner = (inverse_wide * scaled - inner * factor).astype(bf16)
    gi[own] = grad_inner.reshape(F, R, W, C)
    for made in gi_rows:
        made.start()

    def place(ref, frames, band, count):
        value = ref.reshape(count, C).astype(f32)
        for m in range(Z):
            piece = unpack(value, m).astype(bf16)
            qq[frames, band, m * W : (m + 1) * W] = piece.reshape(
                qq.at[frames, band, m * W : (m + 1) * W].shape
            )

    place(gi[own], own, body, rows)
    gather_wait(v_all, 2, 2, activate)

    def place_rows(frames, count, among):
        for side, ref, row in ((has_low, gd, 0), (has_high, gu, R + 1)):

            @pl.when(side if among is None else both(side, among))
            def _():
                place(ref[frames], frames, row, count * W)

    for made in (v_next, g_next, squares_next):
        made.wait()
    for d in range(Z):
        sums_next[d].wait()

    @pl.when(has_next)
    def _():
        taken = slice(0, 2 * R * W)
        inverse = lax.rsqrt(sh[Z] / C + epsilon)
        mean = sh[0]
        for d in range(1, Z):
            mean = mean + sh[d]
        value = vh[...].reshape(2 * R * W, C).astype(f32)
        inverse_wide = spread(inverse)[taken]
        upstream = gh[...].reshape(2 * R * W, C).astype(f32)
        upstream = upstream * silu_slope(value * inverse_wide * gain) * gain
        factor = spread(inverse * inverse * inverse * mean / C)[taken]
        gi[halo] = (inverse_wide * upstream - value * factor).astype(bf16).reshape(2, R, W, C)
        place(gi[halo], halo, body, 2 * R * W)

    @pl.when(jnp.logical_not(has_next))
    def _():
        zero(gi, (halo,))

    for made in gi_corner:
        made.start()
    for made in gi_rows:
        made.wait()
    place_rows(own, F, None)
    for f in range(F):
        early[f] = backward(qq, w_one, f, range(F - f))
    for made in gi_corner:
        made.wait()
    place_rows(halo, 2, has_next)
    for f in range(F):
        total = early[f] + backward(qq, w_one, f, range(F - f, 3))
        yb[f] = shift_sum(total, WW, C).astype(bf16).reshape(R, WW, C)
        b_out.start(f, range(Z - 1, 2, -1))
        if f == 0:
            gather_wait(v_all, 1, 2, activate)
            for d in range(3, Z):
                gather_wait(v_all, d, 2, activate)
            for made in xq_rows:
                made.start()
    for d in (2, 1):
        for f in range(F):
            b_out.start(f, (d,))

    def lhs_two(f):
        return jnp.concatenate(
            [xq[m, f, pl.ds(j, R)].reshape(R * WW, OP) for j in range(3) for m in range(Z)], axis=1
        )

    for made in xq_rows:
        made.wait()
    ahead, branch = forward(lhs_two, w_gap)
    for t in (F + 1, F):
        ys[t - F] = pack(ahead(t)).astype(bf16).reshape(R, W, C)
        y_next[t - F].start()
    rest, branch = branch, []
    for t in range(F):
        b_out.join(t)
        branch.append(rest(t).reshape(R, Z, W, O))
    for made in y_next:
        made.wait()
    for t in range(F):
        for m in range(Z):
            term = branch[t][:, m].reshape(R // fold, fold, W, O)
            if t < 2:
                carried = yr[t].reshape(R * W, C).astype(f32)[:, m * O : (m + 1) * O]
                term = term + carried.reshape(R // fold, fold, W, O)
            yf[m, t] = fold_rows([term[:, k] for k in range(fold)]).reshape(R // fold, W, fold * O)
    for d in sorted(range(1, Z), key=lambda d: -abs(2 * d - Z)):
        y_own[d].start()
    rf[z] = yf[z]

    source = latent[...].reshape(rows, C).astype(f32)
    normed_one, inverse_one = normalize(source, g_one)
    slope_one = silu_slope(normed_one)
    upstream = cotangent[...].reshape(rows, C).astype(f32)
    grad_one = b_out.total(yb[:, :, block(z)].astype(f32)).reshape(rows, C)
    grad = norm_backward(source, inverse_one, g_one, grad_one * slope_one)
    latent_grad[...] = (upstream + grad).astype(bf16).reshape(F, R, W, C)
    for d in range(1, Z):
        y_own[d].wait()
    branch = jnp.concatenate([unfold_rows(rf[m], O).reshape(rows, O) for m in range(Z)], axis=1)
    out[...] = (source + branch).astype(bf16).reshape(F, R, W, C)
    links.drain()


def hand_over(first, second, first_out, second_out, sem):
    copies = [
        pltpu.make_async_copy(first, first_out, sem.at[0]),
        pltpu.make_async_copy(second, second_out, sem.at[1]),
    ]
    for made in copies:
        made.start()
    for made in copies:
        made.wait()


def local(sizes, latent, cotangent, gain_one, gain_two, kernel_one, kernel_two):
    S, Q, Z = sizes
    F, R, W, C = latent.shape
    O = kernel_one.shape[3]
    WW = W * Z
    OP = -(-O // 128) * 128
    rows = F * R * W
    taps = kernel_one.shape[:3]
    fold = fold_of(R, O)
    packed = (F, R, W, C)
    slots = (Z - 1) * (5 + 2 * F) + Z + 13
    shapes = [
        kernel_one.shape,
        kernel_two.shape,
        taps + (O, Z * OP),
        packed,
        (F, R + 2, WW, C),
        (Z, F, R // fold, W, fold * O),
        (Z, F, R // fold, W, fold * O),
        (Z, 2, R // fold, W, fold * O),
        (F + 2, R + 2, WW, OP),
        (Z,) + packed,
        (4,) + packed,
        (2, R, W, C),
        (2, R, W, C),
        (Z,) + packed,
        None,
        None,
        (Z, F, R + 2, WW, OP),
        (F + 2, R, W, C),
        (2, R, W, C),
        (F + 2, W, C),
        (F + 2, W, C),
        (F + 2, R + 2, WW, OP),
        (Z, F, R // fold, W, fold * O),
        (Z, F, R // fold, W, fold * O),
        (2, R, W, C),
        (2, R, W, C),
        (F, R, WW, C),
        (4,) + packed,
        (2, max(Z - 3, 1)) + packed,
        (2, max(Z - 3, 1)) + packed,
        (2, R, W, C),
        (2, R, W, C),
        None,
        None,
        None,
        packed,
        packed,
        None,
        None,
    ]
    scratch = [pltpu.VMEM(shape, bf16) if shape else None for shape in shapes]
    scratch[14] = pltpu.VMEM((2, Z, 8, rows), f32)
    scratch[15] = pltpu.VMEM((Z, 8, C), f32)
    scratch[32] = pltpu.VMEM((8, rows), f32)
    scratch[33] = pltpu.VMEM((Z + 1, 8, rows), f32)
    scratch[34] = pltpu.VMEM((F, R * WW, 3 * C), f32)
    scratch[37] = scratch[38] = pltpu.VMEM((C,), f32)
    hbm = pl.BlockSpec(memory_space=pltpu.HBM)
    results = pl.pallas_call(
        functools.partial(kernel, sizes),
        out_shape=[jax.ShapeDtypeStruct((F, R, W, C), bf16)] * 2,
        in_specs=[hbm] * 6,
        out_specs=[pl.BlockSpec(memory_space=pltpu.VMEM)] * 2,
        scratch_shapes=[
            *scratch,
            pltpu.SemaphoreType.DMA((slots,)),
            pltpu.SemaphoreType.DMA((slots,)),
            pltpu.SemaphoreType.DMA((6,)),
            pltpu.SemaphoreType.REGULAR((2, max(Z - 2, 1))),
        ],
        compiler_params=pltpu.CompilerParams(
            collective_id=0, has_side_effects=True, vmem_limit_bytes=28 * 1024 * 1024
        ),
    )(*[pltpu.with_memory_space_constraint(a, pltpu.HBM) for a in (latent, cotangent, gain_one, gain_two, kernel_one, kernel_two)])
    vmem = pl.BlockSpec(memory_space=pltpu.VMEM)
    return pl.pallas_call(
        hand_over,
        out_shape=[jax.ShapeDtypeStruct((F, R, W, C), bf16)] * 2,
        in_specs=[vmem] * 2,
        out_specs=[hbm] * 2,
        scratch_shapes=[pltpu.SemaphoreType.DMA((2,))],
    )(*[pltpu.with_memory_space_constraint(a, pltpu.VMEM) for a in results])

def solution(mesh):
    sizes = (mesh.shape["section"], mesh.shape["seq"], mesh.shape["exp"])
    spread = P("section", "seq", "exp", None)
    split = P(None, None, None, "exp", None)
    return jax.shard_map(
        functools.partial(local, sizes),
        mesh=mesh,
        in_specs=(spread, spread, P(), P(), split, split),
        out_specs=(spread, spread),
        check_vma=False,
    )
```
